8 devices in a mesh: replica: 1 (over z), model: 8 (over y, x, core).
Axes of the slice: x: 2, y: 2, z: 1, core: 2. Of those that a mesh axis runs over, the one named last changes fastest.
Arguments:
- x: bfloat16 [128, 8192], P('replica')
- cache_len: int32 [128], P('replica')
- w_query: bfloat16 [2, 8192, 8192], P(None, None, 'model')
- w_key: bfloat16 [2, 8192, 128], replicated
- w_value: bfloat16 [2, 8192, 128], replicated
- w_out: bfloat16 [2, 8192, 8192], P(None, 'model')
- k_cache: bfloat16 [2, 128, 2048, 128], P(None, ('replica', 'model'))
- v_cache: bfloat16 [2, 128, 2048, 128], P(None, ('replica', 'model'))
Outputs:
- output 1: bfloat16 [128, 8192], P('replica')
- output 2: bfloat16 [2, 128, 2048, 128], P(None, ('replica', 'model'))
- output 3: bfloat16 [2, 128, 2048, 128], P(None, ('replica', 'model'))
All inputs are finite; a program needn't handle non-finite values.
Results may differ from the reference program's by a relative error of at most 0.00536.
Values are sent between devices in bfloat16 or wider.
A program may use at most 1 GiB of HBM per device.

```python
import jax
import jax.numpy as jnp
from jax import lax

LAYERS = 2
BATCH = 128
D_MODEL = 8192
NUM_HEADS = 64
HEAD_DIM = 128
SEQ_LEN = 2048

SEQ_BITS = SEQ_LEN.bit_length() - 1
Q_WIDTH = NUM_HEADS * HEAD_DIM


def setup_inputs(seed: int = 0, part: int = 0) -> dict:
    root_key = jax.random.key(seed)
    shared = jax.random.split(root_key, 4)
    part_keys = jax.random.split(jax.random.fold_in(root_key, part), 6)
    x = jax.random.normal(part_keys[0], (BATCH, D_MODEL), jnp.float32).astype(jnp.bfloat16)
    raw_len = jax.random.randint(part_keys[1], (BATCH,), 0, SEQ_LEN)
    shift_by = jax.random.randint(part_keys[2], (BATCH,), 0, SEQ_BITS + 1)
    row_order = jax.random.permutation(part_keys[3], BATCH)
    cache_len = jnp.right_shift(raw_len, shift_by)
    cache_len = cache_len.at[row_order[0]].set(SEQ_LEN - 1).at[row_order[1]].set(0)
    w_query = (1.5 * D_MODEL ** -0.5) * jax.random.normal(shared[0], (LAYERS, D_MODEL, Q_WIDTH), jnp.float32)
    w_key = (1.5 * D_MODEL ** -0.5) * jax.random.normal(shared[1], (LAYERS, D_MODEL, HEAD_DIM), jnp.float32)
    w_value = (D_MODEL ** -0.5) * jax.random.normal(shared[2], (LAYERS, D_MODEL, HEAD_DIM), jnp.float32)
    w_out = (2.0 * Q_WIDTH ** -0.5) * jax.random.normal(shared[3], (LAYERS, Q_WIDTH, D_MODEL), jnp.float32)
    k_cache = 1.5 * jax.random.normal(part_keys[4], (LAYERS, BATCH, SEQ_LEN, HEAD_DIM), jnp.float32)
    v_cache = jax.random.normal(part_keys[5], (LAYERS, BATCH, SEQ_LEN, HEAD_DIM), jnp.float32)
    return {
        "x": x,
        "cache_len": cache_len,
        "w_query": w_query.astype(jnp.bfloat16),
        "w_key": w_key.astype(jnp.bfloat16),
        "w_value": w_value.astype(jnp.bfloat16),
        "w_out": w_out.astype(jnp.bfloat16),
        "k_cache": k_cache.astype(jnp.bfloat16),
        "v_cache": v_cache.astype(jnp.bfloat16),
    }


def attend_layer(hidden, cache_len, query_w, key_w, value_w, out_w, k_layer, v_layer):
    query = jnp.dot(hidden, query_w, preferred_element_type=jnp.float32).astype(jnp.bfloat16)
    query = query.reshape(BATCH, NUM_HEADS, HEAD_DIM)
    k_new = jnp.dot(hidden, key_w, preferred_element_type=jnp.float32).astype(jnp.bfloat16)
    v_new = jnp.dot(hidden, value_w, preferred_element_type=jnp.float32).astype(jnp.bfloat16)
    write_here = jnp.arange(SEQ_LEN)[None, :, None] == cache_len[:, None, None]
    k_layer = jnp.where(write_here, k_new[:, None, :], k_layer)
    v_layer = jnp.where(write_here, v_new[:, None, :], v_layer)

    def one_row(row_items):
        q_row, k_row, v_row, row_len = row_items
        scores = jnp.dot(q_row, k_row.T, preferred_element_type=jnp.float32) * (HEAD_DIM ** -0.5)
        visible = jnp.arange(SEQ_LEN)[None, :] <= row_len
        scores = jnp.where(visible, scores, -jnp.inf)
        weights = jax.nn.softmax(scores, axis=-1).astype(jnp.bfloat16)
        context = jnp.dot(weights, v_row, preferred_element_type=jnp.float32)
        return context.astype(jnp.bfloat16)

    context = lax.map(one_row, (query, k_layer, v_layer, cache_len))
    update = jnp.dot(context.reshape(BATCH, Q_WIDTH), out_w, preferred_element_type=jnp.float32)
    hidden = (hidden.astype(jnp.float32) + update).astype(jnp.bfloat16)
    return hidden, k_layer, v_layer


def reference(x, cache_len, w_query, w_key, w_value, w_out, k_cache, v_cache):
    def layer_step(hidden, params):
        query_w, key_w, value_w, out_w, k_layer, v_layer = params
        hidden, k_layer, v_layer = attend_layer(hidden, cache_len, query_w, key_w, value_w, out_w, k_layer, v_layer)
        return hidden, (k_layer, v_layer)

    out, (k_all, v_all) = lax.scan(layer_step, x, (w_query, w_key, w_value, w_out, k_cache, v_cache))
    return out, k_all, v_all
```

```python
import functools

import jax
import jax.numpy as jnp
from jax import lax
from jax.experimental import pallas as pl
from jax.experimental.pallas import tpu as pltpu
from jax.sharding import PartitionSpec as P

MESH = pl.DeviceIdType.MESH
BF16 = jnp.bfloat16
F32 = jnp.float32
VMEM_LIMIT = 62 * 1024 * 1024

DEVICES = 8
ROWS = 128
MY_ROWS = 16
D_MODEL = 8192
HEAD_DIM = 128
MY_HEADS = 8
NUM_HEADS = 64
MY_COLS = 1024
SEQ = 2048
TILE = 256
TILES = MY_COLS // TILE

GROUPS = 2
PIECE = MY_COLS // GROUPS
HALF = ROWS // 2


def dot(a, b):
    return jnp.dot(a, b, preferred_element_type=F32)


def places():
    me = lax.axis_index("model")
    core = lax.rem(me, 2)
    x = lax.rem(lax.div(me, 2), 2)
    y = lax.div(me, 4)
    flip = 1 - 2 * core
    xn = me + 2 - 4 * x
    yn = me + 4 - 8 * y
    diag = xn + 4 - 8 * y
    return me, flip, xn, yn, diag


class Copies:
    def __init__(self, send_sems, recv_sems):
        self.send_sems, self.recv_sems, self.started = send_sems, recv_sems, []

    def start(self, src, dst, device):
        i = len(self.started)
        copy = pltpu.make_async_remote_copy(
            src_ref=src,
            dst_ref=dst,
            send_sem=self.send_sems.at[i],
            recv_sem=self.recv_sems.at[i],
            device_id={"model": device},
            device_id_type=MESH,
        )
        copy.start()
        self.started.append(copy)
        return copy

    def finish(self):
        for copy in self.started:
            copy.wait_send()


class Loads:
    def __init__(self, sems):
        self.sems, self.count = sems, 0

    def start(self, src, dst):
        copy = pltpu.make_async_copy(src, dst, self.sems.at[self.count])
        copy.start()
        self.count += 1
        return copy


def meet_all(me):
    barrier = pltpu.get_barrier_semaphore()
    for k in range(1, DEVICES):
        pl.semaphore_signal(barrier, inc=1, device_id={"model": lax.rem(me + k, DEVICES)}, device_id_type=MESH)
    pl.semaphore_wait(barrier, DEVICES - 1)


def send_query_tile(copies, me, j, q_send, q_out):
    started = []
    for k in range(1, DEVICES):
        to = lax.rem(me + k, DEVICES)
        started.append(copies.start(q_send.at[j, to], q_out.at[j, me], to))
    return started


def new_rows(h_rows, w):
    return dot(h_rows, w)


def query_kernel(x_hbm, wq_hbm, wk_hbm, wv_hbm, q_out, kn_out, vn_out,
                 x_buf, wq_buf, wk_buf, wv_buf, q_send, load_sems, send_sems, recv_sems):
    me, _, _, _, _ = places()
    loads = Loads(load_sems)
    x_load = loads.start(x_hbm, x_buf)
    wq_loads = [loads.start(wq_hbm.at[0, :, pl.ds(j * TILE, TILE)], wq_buf.at[j]) for j in range(TILES)]
    wk_load = loads.start(wk_hbm.at[0], wk_buf)
    wv_load = loads.start(wv_hbm.at[0], wv_buf)
    meet_all(me)
    copies = Copies(send_sems, recv_sems)
    x_load.wait()
    arrivals = []
    for j in range(TILES):
        wq_loads[j].wait()
        q_send[j] = dot(x_buf[...], wq_buf[j]).astype(BF16).reshape(DEVICES, MY_ROWS, TILE)
        arrivals += send_query_tile(copies, me, j, q_send, q_out)
        q_out[j, me] = q_send[j, me]
    x_rows = x_buf[pl.ds(pl.multiple_of(me * MY_ROWS, MY_ROWS), MY_ROWS), :]
    wk_load.wait()
    kn_out[...] = dot(x_rows, wk_buf[...]).astype(BF16)
    wv_load.wait()
    vn_out[...] = dot(x_rows, wv_buf[...]).astype(BF16)
    for copy in arrivals:
        copy.wait_recv()
    copies.finish()


def query_call(x, w_query, w_key, w_value):
    any_spec = pl.BlockSpec(memory_space=pl.ANY)
    vmem_spec = pl.BlockSpec(memory_space=pltpu.VMEM)
    sends = TILES * (DEVICES - 1)
    return pl.pallas_call(
        query_kernel,
        name="query",
        out_shape=(
            jax.ShapeDtypeStruct((TILES, DEVICES, MY_ROWS, TILE), BF16),
            jax.ShapeDtypeStruct((MY_ROWS, HEAD_DIM), BF16),
            jax.ShapeDtypeStruct((MY_ROWS, HEAD_DIM), BF16),
        ),
        in_specs=[any_spec] * 4,
        out_specs=(vmem_spec,) * 3,
        scratch_shapes=[
            pltpu.VMEM((ROWS, D_MODEL), BF16),
            pltpu.VMEM((TILES, D_MODEL, TILE), BF16),
            pltpu.VMEM((D_MODEL, HEAD_DIM), BF16),
            pltpu.VMEM((D_MODEL, HEAD_DIM), BF16),
            pltpu.VMEM((TILES, DEVICES, MY_ROWS, TILE), BF16),
            pltpu.SemaphoreType.DMA((TILES + 3,)),
            pltpu.SemaphoreType.DMA((sends,)),
            pltpu.SemaphoreType.DMA((sends,)),
        ],
        compiler_params=pltpu.CompilerParams(
            collective_id=0, has_side_effects=True, vmem_limit_bytes=VMEM_LIMIT
        ),
    )(x, w_query, w_key, w_value)


def attend_kernel(layer, has_prev, *refs):
    if has_prev:
        len_ref, q_ref, kn_ref, vn_ref, k_hbm, v_hbm, _, _ = refs[:8]
        rest = refs[8:]
    else:
        len_ref, q_ref, kn_ref, vn_ref, k_hbm, v_hbm = refs[:6]
        rest = refs[6:]
    ctx_ref, k_out, v_out, k_buf, v_buf, q_buf, kn_buf, vn_buf, in_sems, out_sems = rest
    me = lax.axis_index("model")

    def load(which, b):
        hbm, buf = ((k_hbm, k_buf), (v_hbm, v_buf))[which]
        return pltpu.make_async_copy(hbm.at[layer, b], buf.at[b], in_sems.at[which, b])

    def save(which, b):
        hbm, buf = ((k_out, k_buf), (v_out, v_buf))[which]
        return pltpu.make_async_copy(buf.at[b], hbm.at[layer, b], out_sems.at[which, b])

    @pl.loop(0, MY_ROWS)
    def _(b):
        load(0, b).start()
        load(1, b).start()

    kn_buf[...] = kn_ref[...].astype(F32)
    vn_buf[...] = vn_ref[...].astype(F32)
    for j in range(TILES):
        for src in range(DEVICES):
            block = q_ref[j, src].astype(F32)
            for h in range(TILE // HEAD_DIM):
                head = src * MY_HEADS + j * (TILE // HEAD_DIM) + h
                q_buf[:, head, :] = block[:, h * HEAD_DIM:(h + 1) * HEAD_DIM]

    scale = HEAD_DIM ** -0.5

    @pl.loop(0, MY_ROWS)
    def _(b):
        pos = len_ref[me * MY_ROWS + b]
        base = pl.multiple_of((pos // 16) * 16, 16)
        here = lax.broadcasted_iota(jnp.int32, (16, HEAD_DIM), 0) == pos - base

        def patch(buf, new):
            tile = buf[b, pl.ds(base, 16), :].astype(F32)
            row = jnp.broadcast_to(new[pl.ds(b, 1), :], (16, HEAD_DIM))
            buf[b, pl.ds(base, 16), :] = jnp.where(here, row, tile).astype(BF16)

        def attend(n):
            q = q_buf[b].astype(BF16)
            k = k_buf[b, 0:n, :]
            s = lax.dot_general(q, k, (((1,), (1,)), ((), ())), preferred_element_type=F32) * scale
            t = lax.broadcasted_iota(jnp.int32, (NUM_HEADS, n), 1)
            s = jnp.where(t <= pos, s, -jnp.inf)
            e = jnp.exp(s - jnp.max(s, axis=1, keepdims=True))
            p = (e * (1.0 / jnp.sum(e, axis=1, keepdims=True))).astype(BF16)
            c = dot(p, v_buf[b, 0:n, :])
            ctx_ref[:, b] = c.reshape(DEVICES, MY_HEADS, HEAD_DIM).astype(BF16)

        load(0, b).wait()
        patch(k_buf, kn_buf)
        load(1, b).wait()
        patch(v_buf, vn_buf)

        @pl.when(pos < 256)
        def _():
            attend(256)

        @pl.when(jnp.logical_and(pos >= 256, pos < 1024))
        def _():
            attend(1024)

        @pl.when(pos >= 1024)
        def _():
            attend(2048)

        save(0, b).start()
        save(1, b).start()

    @pl.loop(0, MY_ROWS)
    def _(b):
        save(0, b).wait()
        save(1, b).wait()


def attend_call(layer, cache_len, q, kn, vn, k_cache, v_cache, prev):
    any_spec = pl.BlockSpec(memory_space=pl.ANY)
    vmem_spec = pl.BlockSpec(memory_space=pltpu.VMEM)
    return pl.pallas_call(
        functools.partial(attend_kernel, layer, bool(prev)),
        name="attend",
        out_shape=(
            jax.ShapeDtypeStruct((DEVICES, MY_ROWS, MY_HEADS, HEAD_DIM), BF16),
            jax.ShapeDtypeStruct(k_cache.shape, BF16),
            jax.ShapeDtypeStruct(v_cache.shape, BF16),
        ),
        in_specs=[pl.BlockSpec(memory_space=pltpu.SMEM)] + [vmem_spec] * 3 + [any_spec] * (2 + len(prev)),
        out_specs=(vmem_spec, any_spec, any_spec),
        scratch_shapes=[
            pltpu.VMEM((MY_ROWS, SEQ, HEAD_DIM), BF16),
            pltpu.VMEM((MY_ROWS, SEQ, HEAD_DIM), BF16),
            pltpu.VMEM((MY_ROWS, NUM_HEADS, HEAD_DIM), F32),
            pltpu.VMEM((MY_ROWS, HEAD_DIM), F32),
            pltpu.VMEM((MY_ROWS, HEAD_DIM), F32),
            pltpu.SemaphoreType.DMA((2, MY_ROWS)),
            pltpu.SemaphoreType.DMA((2, MY_ROWS)),
        ],
        input_output_aliases={6: 1, 7: 2} if prev else {},
        compiler_params=pltpu.CompilerParams(vmem_limit_bytes=VMEM_LIMIT),
    )(cache_len, q, kn, vn, k_cache, v_cache, *prev)


SELF, XN, YN, DIAG = range(4)


def combine_kernel(layer, last, *refs):
    if last:
        (ctx_in, res_hbm, wo_hbm, out_hbm,
         ctx_buf, lhs, res_buf, wo_buf, send_d2d, recv_d2d, acc, rx_diag, ry_diag, rx_dir, ry_dir, rx_fwd, ry_fwd, h_buf,
         load_sems, send_sems, recv_sems) = refs
    else:
        (ctx_in, res_hbm, wo_hbm, wq_hbm, wk_hbm, wv_hbm, own_out, q_out, kn_out, vn_out,
         ctx_buf, lhs, res_buf, wo_buf, send_d2d, recv_d2d, acc, rx_diag, ry_diag, rx_dir, ry_dir, rx_fwd, ry_fwd, h_buf,
         wq_buf, wk_buf, wv_buf, q_acc, q_send,
         load_sems, send_sems, recv_sems) = refs
    me, flip, xn, yn, diag = places()
    partner = me + flip
    chip_mate = {SELF: me, XN: xn, YN: yn, DIAG: diag}
    owner = lambda r, c: chip_mate[r] + c * flip
    column = lambda r, c, g: pl.multiple_of(owner(r, c) * MY_COLS + g * PIECE, PIECE)
    loads = Loads(load_sems)
    copies = Copies(send_sems, recv_sems)
    order = (DIAG, XN, YN, SELF)
    steps = [(g, r) for g in range(GROUPS) for r in order]
    top, bottom = pl.ds(0, HALF), pl.ds(HALF, HALF)

    own_load = loads.start(ctx_in.at[me], ctx_buf.at[me])
    wo_loads = {}
    for g, r in steps:
        for c in (1, 0):
            wo_loads[g, r, c] = loads.start(wo_hbm.at[layer, :, pl.ds(column(r, c, g), PIECE)], wo_buf.at[g, r, c])
    if last:
        res_load = loads.start(res_hbm, res_buf)
    else:
        res_load = loads.start(res_hbm.at[:, pl.ds(pl.multiple_of(me * MY_COLS, MY_COLS), MY_COLS)], res_buf)
        wq_loads = {}
        for r in (SELF, XN, YN, DIAG):
            for c in (0, 1):
                for g in range(GROUPS):
                    wq_loads[r, c, g] = loads.start(
                        wq_hbm.at[layer + 1, pl.ds(column(r, c, g), PIECE), :], wq_buf.at[r, c, g])
        wk_load = loads.start(wk_hbm.at[layer + 1], wk_buf)
        wv_load = loads.start(wv_hbm.at[layer + 1], wv_buf)

    meet_all(me)

    arrivals = []
    for k in range(1, DEVICES):
        to = lax.rem(me + k, DEVICES)
        arrivals.append(copies.start(ctx_in.at[to], ctx_buf.at[me], to))
    own_load.wait()
    for copy in arrivals:
        copy.wait_recv()
    for src in range(DEVICES):
        rows = ctx_buf[src].astype(F32).reshape(MY_ROWS, MY_COLS).astype(BF16)
        lhs[src * MY_ROWS:(src + 1) * MY_ROWS, :] = rows

    d2d = {}
    first, direct, forward = {}, {}, {}

    def settle(g, r):
        d2d[g, r].wait_recv()
        acc[g, r] += recv_d2d[g, r]
        if r == DIAG:
            first[g, 0] = copies.start(acc.at[g, r, top], rx_diag.at[g], xn)
            first[g, 1] = copies.start(acc.at[g, r, bottom], ry_diag.at[g], yn)

    def send_direct(g):
        direct[g, 0] = copies.start(acc.at[g, XN, top], rx_dir.at[g], xn)
        direct[g, 1] = copies.start(acc.at[g, YN, bottom], ry_dir.at[g], yn)

    pending = None
    for g, r in steps:
        wo_loads[g, r, 1].wait()
        send_d2d[g, r] = dot(lhs[...], wo_buf[g, r, 1])
        d2d[g, r] = copies.start(send_d2d.at[g, r], recv_d2d.at[g, r], partner)
        wo_loads[g, r, 0].wait()
        acc[g, r] = dot(lhs[...], wo_buf[g, r, 0])
        if pending is not None:
            settle(*pending)
            if pending == (0, YN):
                send_direct(0)
        pending = (g, r)
    settle(*pending)
    if GROUPS == 1:
        pass

    for g in range(GROUPS):
        first[g, 0].wait_recv()
        acc[g, YN, top] += rx_diag[g]
        forward[g, 1] = copies.start(acc.at[g, YN, top], ry_fwd.at[g], yn)
        first[g, 1].wait_recv()
        acc[g, XN, bottom] += ry_diag[g]
        forward[g, 0] = copies.start(acc.at[g, XN, bottom], rx_fwd.at[g], xn)
        if g + 1 < GROUPS:
            send_direct(g + 1)

    res_load.wait()
    gather = {}

    def finish_piece(g):
        cols = slice(g * PIECE, (g + 1) * PIECE)
        direct[g, 0].wait_recv()
        forward[g, 1].wait_recv()
        total = acc[g, SELF, top] + rx_dir[g] + ry_fwd[g]
        h_buf[SELF, 0, g, top] = (res_buf[top, cols].astype(F32) + total).astype(BF16)
        direct[g, 1].wait_recv()
        forward[g, 0].wait_recv()
        total = acc[g, SELF, bottom] + ry_dir[g] + rx_fwd[g]
        h_buf[SELF, 0, g, bottom] = (res_buf[bottom, cols].astype(F32) + total).astype(BF16)
        mine = h_buf.at[SELF, 0, g]
        gather[XN, 0, g] = [copies.start(mine, h_buf.at[XN, 0, g], xn)]
        gather[YN, 0, g] = [copies.start(mine, h_buf.at[YN, 0, g], yn)]
        gather[SELF, 1, g] = [copies.start(mine, h_buf.at[SELF, 1, g], partner)]
        if not last:
            own_out[:, cols] = h_buf[SELF, 0, g]

    def arrive(r, c, g):
        for copy in gather[r, c, g]:
            copy.wait_recv()

    stores = []
    if last:
        def use(r, c, g):
            stores.append(loads.start(h_buf.at[r, c, g], out_hbm.at[:, pl.ds(column(r, c, g), PIECE)]))
    else:
        q_acc[...] = jnp.zeros_like(q_acc)

        def use(r, c, g):
            wq_loads[r, c, g].wait()
            q_acc[...] += dot(h_buf[r, c, g], wq_buf[r, c, g])

    for g in range(GROUPS):
        finish_piece(g)
    for g in range(GROUPS):
        use(SELF, 0, g)
    for g in range(GROUPS):
        arrive(SELF, 1, g)
        use(SELF, 1, g)
    for g in range(GROUPS):
        arrive(XN, 0, g)
        down = [copies.start(h_buf.at[XN, 0, g, top], h_buf.at[DIAG, 0, g, top], yn)]
        gather[XN, 1, g] = [copies.start(h_buf.at[XN, 0, g], h_buf.at[XN, 1, g], partner)]
        arrive(YN, 0, g)
        down += [copies.start(h_buf.at[YN, 0, g, bottom], h_buf.at[DIAG, 0, g, bottom], xn)]
        gather[DIAG, 0, g] = down
        gather[YN, 1, g] = [copies.start(h_buf.at[YN, 0, g], h_buf.at[YN, 1, g], partner)]
        use(XN, 0, g)
        use(YN, 0, g)
        arrive(XN, 1, g)
        use(XN, 1, g)
        arrive(YN, 1, g)
        use(YN, 1, g)
    for g in range(GROUPS):
        arrive(DIAG, 0, g)
        gather[DIAG, 1, g] = [copies.start(h_buf.at[DIAG, 0, g], h_buf.at[DIAG, 1, g], partner)]
        use(DIAG, 0, g)
    for g in range(GROUPS):
        arrive(DIAG, 1, g)
        use(DIAG, 1, g)

    if last:
        for store in stores:
            store.wait()
    else:
        arrivals = []
        for j in range(TILES):
            q_send[j] = q_acc[:, j * TILE:(j + 1) * TILE].astype(BF16).reshape(DEVICES, MY_ROWS, TILE)
            arrivals += send_query_tile(copies, me, j, q_send, q_out)
            q_out[j, me] = q_send[j, me]
        wk_load.wait()
        wv_load.wait()
        mine = pl.ds(pl.multiple_of(me * MY_ROWS, MY_ROWS), MY_ROWS)
        kn = jnp.zeros((MY_ROWS, HEAD_DIM), F32)
        vn = jnp.zeros((MY_ROWS, HEAD_DIM), F32)
        for r in (SELF, XN, YN, DIAG):
            for c in (0, 1):
                for g in range(GROUPS):
                    rows = h_buf[r, c, g, mine, :]
                    depth = pl.ds(column(r, c, g), PIECE)
                    kn += dot(rows, wk_buf[depth, :])
                    vn += dot(rows, wv_buf[depth, :])
        kn_out[...] = kn.astype(BF16)
        vn_out[...] = vn.astype(BF16)
        for copy in arrivals:
            copy.wait_recv()
    copies.finish()


def combine_call(layer, last, ctx, residual, w_out, more):
    any_spec = pl.BlockSpec(memory_space=pl.ANY)
    vmem_spec = pl.BlockSpec(memory_space=pltpu.VMEM)
    sends = (DEVICES - 1) + GROUPS * (4 + 6 + 9)
    loads = 1 + 8 * GROUPS + 1 + 8 * GROUPS
    scratch = [
        pltpu.VMEM((DEVICES, MY_ROWS, MY_HEADS, HEAD_DIM), BF16),
        pltpu.VMEM((ROWS, MY_COLS), BF16),
        pltpu.VMEM((ROWS, MY_COLS), BF16),
        pltpu.VMEM((GROUPS, 4, 2, MY_COLS, PIECE), BF16),
        pltpu.VMEM((GROUPS, 4, ROWS, PIECE), F32),
        pltpu.VMEM((GROUPS, 4, ROWS, PIECE), F32),
        pltpu.VMEM((GROUPS, 4, ROWS, PIECE), F32),
    ] + [pltpu.VMEM((GROUPS, HALF, PIECE), F32)] * 6 + [
        pltpu.VMEM((4, 2, GROUPS, ROWS, PIECE), BF16),
    ]
    if last:
        out_shape = jax.ShapeDtypeStruct((ROWS, D_MODEL), BF16)
        out_specs = any_spec
    else:
        out_shape = (
            jax.ShapeDtypeStruct((ROWS, MY_COLS), BF16),
            jax.ShapeDtypeStruct((TILES, DEVICES, MY_ROWS, TILE), BF16),
            jax.ShapeDtypeStruct((MY_ROWS, HEAD_DIM), BF16),
            jax.ShapeDtypeStruct((MY_ROWS, HEAD_DIM), BF16),
        )
        out_specs = (vmem_spec,) * 4
        sends += TILES * (DEVICES - 1)
        loads += 2
        scratch += [
            pltpu.VMEM((4, 2, GROUPS, PIECE, MY_COLS), BF16),
            pltpu.VMEM((D_MODEL, HEAD_DIM), BF16),
            pltpu.VMEM((D_MODEL, HEAD_DIM), BF16),
            pltpu.VMEM((ROWS, MY_COLS), F32),
            pltpu.VMEM((TILES, DEVICES, MY_ROWS, TILE), BF16),
        ]
    scratch += [
        pltpu.SemaphoreType.DMA((loads,)),
        pltpu.SemaphoreType.DMA((sends,)),
        pltpu.SemaphoreType.DMA((sends,)),
    ]
    return pl.pallas_call(
        functools.partial(combine_kernel, layer, last),
        name="combine_last" if last else "combine",
        out_shape=out_shape,
        in_specs=[vmem_spec] + [any_spec] * (2 + len(more)),
        out_specs=out_specs,
        scratch_shapes=scratch,
        compiler_params=pltpu.CompilerParams(
            collective_id=2 if last else 1, has_side_effects=True, vmem_limit_bytes=VMEM_LIMIT
        ),
    )(ctx, residual, w_out, *more)


def solution(mesh):
    cache_spec = P(None, ("replica", "model"), None, None)

    def device_step(x, cache_len, w_query, w_key, w_value, w_out, k_cache, v_cache):
        q, kn, vn = query_call(x, w_query, w_key, w_value)
        ctx, k_all, v_all = attend_call(0, cache_len, q, kn, vn, k_cache, v_cache, ())
        own, q, kn, vn = combine_call(0, False, ctx, x, w_out, (w_query, w_key, w_value))
        ctx, k_all, v_all = attend_call(1, cache_len, q, kn, vn, k_cache, v_cache, (k_all, v_all))
        out = combine_call(1, True, ctx, own, w_out, ())
        return out, k_all, v_all

    return jax.shard_map(
        device_step,
        mesh=mesh,
        in_specs=(P("replica", None), P("replica"), P(None, None, "model"), P(), P(), P(None, "model", None), cache_spec, cache_spec),
        out_specs=(P("replica", None), cache_spec, cache_spec),
        check_vma=False,
    )
```

```python
import functools

import jax
import jax.numpy as jnp
from jax import lax
from jax.experimental import pallas as pl
from jax.experimental.pallas import tpu as pltpu
from jax.sharding import PartitionSpec as P

MESH = pl.DeviceIdType.MESH
BF16 = jnp.bfloat16
F32 = jnp.float32
MIB = 1024 * 1024

DEVICES = 8
ROWS = 128
MY_ROWS = 16
D_MODEL = 8192
HEAD_DIM = 128
MY_HEADS = 8
NUM_HEADS = 64
MY_COLS = 1024
SEQ = 2048
TILE = 256
TILES = MY_COLS // TILE

HALF_COLS = 512
GROUPS = 2
PIECE = MY_COLS // GROUPS
HALF = ROWS // 2
SLOTS = 8 * GROUPS
TOGETHER = 2
SPANS = (256, 1024, 2048)


def dot(a, b):
    return jnp.dot(a, b, preferred_element_type=F32)


def places():
    me = lax.axis_index("model")
    core = lax.rem(me, 2)
    x = lax.rem(lax.div(me, 2), 2)
    y = lax.div(me, 4)
    flip = 1 - 2 * core
    xn = me + 2 - 4 * x
    yn = me + 4 - 8 * y
    diag = xn + 4 - 8 * y
    return me, flip, xn, yn, diag


class Copies:
    def __init__(self, send_sems, recv_sems):
        self.send_sems, self.recv_sems, self.started = send_sems, recv_sems, []

    def start(self, src, dst, device):
        i = len(self.started)
        copy = pltpu.make_async_remote_copy(
            src_ref=src,
            dst_ref=dst,
            send_sem=self.send_sems.at[i],
            recv_sem=self.recv_sems.at[i],
            device_id={"model": device},
            device_id_type=MESH,
        )
        copy.start()
        self.started.append(copy)
        return copy

    def finish(self):
        for copy in self.started:
            copy.wait_send()


class Loads:
    def __init__(self, sems):
        self.sems, self.count = sems, 0

    def start(self, src, dst):
        copy = pltpu.make_async_copy(src, dst, self.sems.at[self.count])
        copy.start()
        self.count += 1
        return copy


def meet_all(me):
    barrier = pltpu.get_barrier_semaphore()
    for k in range(1, DEVICES):
        pl.semaphore_signal(barrier, inc=1, device_id={"model": lax.rem(me + k, DEVICES)}, device_id_type=MESH)
    pl.semaphore_wait(barrier, DEVICES - 1)


def send_query_tile(copies, me, j, q_send, q_out):
    started = []
    for k in range(1, DEVICES):
        to = lax.rem(me + k, DEVICES)
        started.append(copies.start(q_send.at[j, to], q_out.at[j, me], to))
    return started


def new_rows(h_rows, w):
    return dot(h_rows, w)


def load_cache(loads, layer, k_hbm, v_hbm, kv_pre):
    return [loads.start(hbm.at[layer], kv_pre.at[i]) for i, hbm in enumerate((k_hbm, v_hbm))]


def in_vmem(*arrays):
    return [pltpu.with_memory_space_constraint(a, pltpu.VMEM) for a in arrays]


def in_hbm(*arrays):
    return [pltpu.with_memory_space_constraint(a, pltpu.HBM) for a in arrays]


QUERY_SHAPES = (
    pltpu.VMEM((TILES, DEVICES, MY_ROWS, TILE), BF16),
    pltpu.VMEM((MY_ROWS, HEAD_DIM), BF16),
    pltpu.VMEM((MY_ROWS, HEAD_DIM), BF16),
    pltpu.VMEM((2, MY_ROWS, SEQ, HEAD_DIM), BF16),
)


def query_kernel(x_hbm, wq_hbm, wk_hbm, wv_hbm, k_hbm, v_hbm, q_out, kn_out, vn_out, kv_pre,
                 x_buf, wq_buf, wk_buf, wv_buf, q_send, load_sems, send_sems, recv_sems):
    me, _, _, _, _ = places()
    loads = Loads(load_sems)
    x_load = loads.start(x_hbm, x_buf)
    wq_loads = [loads.start(wq_hbm.at[0, :, pl.ds(j * TILE, TILE)], wq_buf.at[j]) for j in range(TILES)]
    wk_load = loads.start(wk_hbm.at[0], wk_buf)
    wv_load = loads.start(wv_hbm.at[0], wv_buf)
    cache_loads = load_cache(loads, 0, k_hbm, v_hbm, kv_pre)
    meet_all(me)
    copies = Copies(send_sems, recv_sems)
    x_load.wait()
    arrivals = []
    for j in range(TILES):
        wq_loads[j].wait()
        q_send[j] = dot(x_buf[...], wq_buf[j]).astype(BF16).reshape(DEVICES, MY_ROWS, TILE)
        arrivals += send_query_tile(copies, me, j, q_send, q_out)
        q_out[j, me] = q_send[j, me]
    x_rows = x_buf[pl.ds(pl.multiple_of(me * MY_ROWS, MY_ROWS), MY_ROWS), :]
    wk_load.wait()
    kn_out[...] = dot(x_rows, wk_buf[...]).astype(BF16)
    wv_load.wait()
    vn_out[...] = dot(x_rows, wv_buf[...]).astype(BF16)
    for copy in arrivals:
        copy.wait_recv()
    copies.finish()
    for load in cache_loads:
        load.wait()


def query_call(x, w_query, w_key, w_value, k_cache, v_cache):
    any_spec = pl.BlockSpec(memory_space=pl.ANY)
    vmem_spec = pl.BlockSpec(memory_space=pltpu.VMEM)
    sends = TILES * (DEVICES - 1)
    return pl.pallas_call(
        query_kernel,
        name="query",
        out_shape=QUERY_SHAPES,
        in_specs=[any_spec] * 6,
        out_specs=(vmem_spec,) * len(QUERY_SHAPES),
        scratch_shapes=[
            pltpu.VMEM((ROWS, D_MODEL), BF16),
            pltpu.VMEM((TILES, D_MODEL, TILE), BF16),
            pltpu.VMEM((D_MODEL, HEAD_DIM), BF16),
            pltpu.VMEM((D_MODEL, HEAD_DIM), BF16),
            pltpu.VMEM((TILES, DEVICES, MY_ROWS, TILE), BF16),
            pltpu.SemaphoreType.DMA((TILES + 5,)),
            pltpu.SemaphoreType.DMA((sends,)),
            pltpu.SemaphoreType.DMA((sends,)),
        ],
        compiler_params=pltpu.CompilerParams(
            collective_id=0, has_side_effects=True, vmem_limit_bytes=26 * MIB
        ),
    )(*in_hbm(x, w_query, w_key, w_value, k_cache, v_cache))


def attend_kernel(layer, has_prev, len_ref, q_ref, kn_ref, vn_ref, *refs):
    k_out, v_out, ctx_ref, kv_buf, q_buf, kn_buf, vn_buf, out_sems = refs[-8:]
    k_buf, v_buf = kv_buf.at[0], kv_buf.at[1]
    me = lax.axis_index("model")

    def save(which, b):
        hbm, buf = ((k_out, k_buf), (v_out, v_buf))[which]
        return pltpu.make_async_copy(buf.at[b], hbm.at[layer, b], out_sems.at[which, b])

    kn_buf[...] = kn_ref[...].astype(F32)
    vn_buf[...] = vn_ref[...].astype(F32)
    for j in range(TILES):
        for src in range(DEVICES):
            block = q_ref[j, src].astype(F32)
            for h in range(TILE // HEAD_DIM):
                head = src * MY_HEADS + j * (TILE // HEAD_DIM) + h
                q_buf[:, head, :] = block[:, h * HEAD_DIM:(h + 1) * HEAD_DIM]

    scale = HEAD_DIM ** -0.5

    @pl.loop(0, MY_ROWS)
    def _(b):
        pos = len_ref[me * MY_ROWS + b]
        base = pl.multiple_of((pos // 16) * 16, 16)
        here = lax.broadcasted_iota(jnp.int32, (16, HEAD_DIM), 0) == pos - base
        for buf, new in ((k_buf, kn_buf), (v_buf, vn_buf)):
            tile = buf[b, pl.ds(base, 16), :].astype(F32)
            row = jnp.broadcast_to(new[pl.ds(b, 1), :], (16, HEAD_DIM))
            buf[b, pl.ds(base, 16), :] = jnp.where(here, row, tile).astype(BF16)

    @pl.loop(0, MY_ROWS)
    def _(b):
        save(0, b).start()
        save(1, b).start()

    def attend(b, pos, n):
        q = q_buf[b].astype(BF16)
        k = k_buf[b, 0:n, :]
        s = lax.dot_general(q, k, (((1,), (1,)), ((), ())), preferred_element_type=F32) * scale
        t = lax.broadcasted_iota(jnp.int32, (NUM_HEADS, n), 1)
        s = jnp.where(t <= pos, s, -jnp.inf)
        e = jnp.exp(s - jnp.max(s, axis=1, keepdims=True))
        p = (e * (1.0 / jnp.sum(e, axis=1, keepdims=True))).astype(BF16)
        c = dot(p, v_buf[b, 0:n, :])
        return c.reshape(DEVICES, MY_HEADS, HEAD_DIM).astype(BF16)

    @pl.loop(0, MY_ROWS // TOGETHER)
    def _(i):
        rows = [i * TOGETHER + k for k in range(TOGETHER)]
        pos = [len_ref[me * MY_ROWS + b] for b in rows]
        longest = functools.reduce(jnp.maximum, pos)
        low = 0
        for n in SPANS:
            @pl.when(jnp.logical_and(longest >= low, longest < n))
            def _(n=n):
                done = [attend(b, p, n) for b, p in zip(rows, pos)]
                for b, c in zip(rows, done):
                    ctx_ref[:, b] = c
            low = n

    @pl.loop(0, MY_ROWS)
    def _(b):
        save(0, b).wait()
        save(1, b).wait()


def attend_call(layer, cache_len, q, kn, vn, kv_pre, prev):
    any_spec = pl.BlockSpec(memory_space=pl.ANY)
    vmem_spec = pl.BlockSpec(memory_space=pltpu.VMEM)
    whole = jax.ShapeDtypeStruct((2,) + kv_pre.shape[1:], BF16)
    k_all, v_all, ctx, _ = pl.pallas_call(
        functools.partial(attend_kernel, layer, bool(prev)),
        name="attend",
        out_shape=(
            whole,
            whole,
            pltpu.VMEM((DEVICES, MY_ROWS, MY_HEADS, HEAD_DIM), BF16),
            pltpu.VMEM(kv_pre.shape, BF16),
        ),
        in_specs=[pl.BlockSpec(memory_space=pltpu.SMEM)] + [vmem_spec] * 4 + [any_spec] * len(prev),
        out_specs=(any_spec, any_spec, vmem_spec, vmem_spec),
        scratch_shapes=[
            pltpu.VMEM((MY_ROWS, NUM_HEADS, HEAD_DIM), F32),
            pltpu.VMEM((MY_ROWS, HEAD_DIM), F32),
            pltpu.VMEM((MY_ROWS, HEAD_DIM), F32),
            pltpu.SemaphoreType.DMA((2, MY_ROWS)),
        ],
        input_output_aliases={4: 3} | ({5: 0, 6: 1} if prev else {}),
        compiler_params=pltpu.CompilerParams(vmem_limit_bytes=16 * MIB),
    )(cache_len, *in_vmem(q, kn, vn, kv_pre), *prev)
    return ctx, k_all, v_all


SELF, XN, YN, DIAG = range(4)


def combine_kernel(layer, last, *refs):
    if last:
        (ctx_in, res_hbm, wo_hbm, out_ref,
         ctx_buf, lhs, res_buf, w_buf, send_d2d, recv_d2d, acc, rx_diag, ry_diag, rx_dir, ry_dir, rx_fwd, ry_fwd, h_buf,
         load_sems, send_sems, recv_sems) = refs
    else:
        (ctx_in, res_hbm, wo_hbm, wq_hbm, wk_hbm, wv_hbm, k_hbm, v_hbm, own_out, q_out, kn_out, vn_out, kv_pre,
         ctx_buf, lhs, res_buf, w_buf, send_d2d, recv_d2d, acc, rx_diag, ry_diag, rx_dir, ry_dir, rx_fwd, ry_fwd, h_buf,
         wk_buf, wv_buf, q_acc, q_send,
         load_sems, send_sems, recv_sems) = refs
    me, flip, xn, yn, diag = places()
    partner = me + flip
    chip_mate = {SELF: me, XN: xn, YN: yn, DIAG: diag}
    owner = lambda r, c: chip_mate[r] + c * flip
    column = lambda r, c, g: pl.multiple_of(owner(r, c) * MY_COLS + g * PIECE, PIECE)
    loads = Loads(load_sems)
    copies = Copies(send_sems, recv_sems)
    order = (DIAG, XN, YN, SELF)
    steps = [(g, r) for g in range(GROUPS) for r in order]
    top, bottom = pl.ds(0, HALF), pl.ds(HALF, HALF)

    own_load = loads.start(ctx_in.at[me], ctx_buf.at[me])
    wo_loads, wo_slot = {}, {}
    for g, r in steps:
        for c in (1, 0):
            slot = wo_slot[g, r, c] = len(wo_slot)
            wo_loads[g, r, c] = loads.start(wo_hbm.at[layer, :, pl.ds(column(r, c, g), PIECE)], w_buf.at[slot])
    if last:
        res_load = loads.start(res_hbm, res_buf)
    else:
        res_load = loads.start(res_hbm.at[:, pl.ds(pl.multiple_of(me * MY_COLS, MY_COLS), MY_COLS)], res_buf)
        wk_load = loads.start(wk_hbm.at[layer + 1], wk_buf)
        wv_load = loads.start(wv_hbm.at[layer + 1], wv_buf)
    wq_order = [(r, c, g) for r in (SELF, XN, YN, DIAG) for c in (0, 1) for g in range(GROUPS)]
    wq_loads, wq_slot = {}, {}

    def refill(slot):
        if last:
            return
        r, c, g = wq_order[len(wq_slot)]
        wq_slot[r, c, g] = slot
        rows = pl.ds(column(r, c, g), PIECE)
        wq_loads[r, c, g] = [
            loads.start(wq_hbm.at[layer + 1, rows, pl.ds(n * HALF_COLS, HALF_COLS)],
                        w_buf.at[slot, pl.ds(n * PIECE, PIECE), :])
            for n in range(MY_COLS // HALF_COLS)
        ]

    meet_all(me)

    arrivals = []
    for k in range(1, DEVICES):
        to = lax.rem(me + k, DEVICES)
        arrivals.append(copies.start(ctx_in.at[to], ctx_buf.at[me], to))
    own_load.wait()
    for copy in arrivals:
        copy.wait_recv()
    for src in range(DEVICES):
        rows = ctx_buf[src].astype(F32).reshape(MY_ROWS, MY_COLS).astype(BF16)
        lhs[src * MY_ROWS:(src + 1) * MY_ROWS, :] = rows

    d2d = {}
    first, direct, forward = {}, {}, {}

    def settle(g, r):
        d2d[g, r].wait_recv()
        acc[g, r] += recv_d2d[g, r]
        if r == DIAG:
            first[g, 0] = copies.start(acc.at[g, r, top], rx_diag.at[g], xn)
            first[g, 1] = copies.start(acc.at[g, r, bottom], ry_diag.at[g], yn)

    def send_direct(g):
        direct[g, 0] = copies.start(acc.at[g, XN, top], rx_dir.at[g], xn)
        direct[g, 1] = copies.start(acc.at[g, YN, bottom], ry_dir.at[g], yn)

    pending = None
    for g, r in steps:
        for c, target in ((1, send_d2d), (0, acc)):
            wo_loads[g, r, c].wait()
            target[g, r] = dot(lhs[...], w_buf[wo_slot[g, r, c]])
            refill(wo_slot[g, r, c])
            if c == 1:
                d2d[g, r] = copies.start(send_d2d.at[g, r], recv_d2d.at[g, r], partner)
        if pending is not None:
            settle(*pending)
            if pending == (0, YN):
                send_direct(0)
        pending = (g, r)
    settle(*pending)
    if not last:
        cache_loads = load_cache(loads, layer + 1, k_hbm, v_hbm, kv_pre)

    for g in range(GROUPS):
        first[g, 0].wait_recv()
        acc[g, YN, top] += rx_diag[g]
        forward[g, 1] = copies.start(acc.at[g, YN, top], ry_fwd.at[g], yn)
        first[g, 1].wait_recv()
        acc[g, XN, bottom] += ry_diag[g]
        forward[g, 0] = copies.start(acc.at[g, XN, bottom], rx_fwd.at[g], xn)
        if g + 1 < GROUPS:
            send_direct(g + 1)

    res_load.wait()
    gather = {}
    own_stores = []

    def finish_piece(g):
        cols = slice(g * PIECE, (g + 1) * PIECE)
        direct[g, 0].wait_recv()
        forward[g, 1].wait_recv()
        total = acc[g, SELF, top] + rx_dir[g] + ry_fwd[g]
        h_buf[SELF, 0, g, top] = (res_buf[top, cols].astype(F32) + total).astype(BF16)
        direct[g, 1].wait_recv()
        forward[g, 0].wait_recv()
        total = acc[g, SELF, bottom] + ry_dir[g] + rx_fwd[g]
        h_buf[SELF, 0, g, bottom] = (res_buf[bottom, cols].astype(F32) + total).astype(BF16)
        mine = h_buf.at[SELF, 0, g]
        gather[XN, 0, g] = [copies.start(mine, h_buf.at[XN, 0, g], xn)]
        gather[YN, 0, g] = [copies.start(mine, h_buf.at[YN, 0, g], yn)]
        gather[SELF, 1, g] = [copies.start(mine, h_buf.at[SELF, 1, g], partner)]
        if not last:
            own_stores.append(loads.start(mine, own_out.at[:, pl.ds(g * PIECE, PIECE)]))

    def arrive(r, c, g):
        for copy in gather[r, c, g]:
            copy.wait_recv()

    if last:
        def use(r, c, g):
            out_ref[:, pl.ds(column(r, c, g), PIECE)] = h_buf[r, c, g]
    else:
        q_acc[...] = jnp.zeros_like(q_acc)

        def use(r, c, g):
            for n, load in enumerate(wq_loads[r, c, g]):
                load.wait()
                w = w_buf[wq_slot[r, c, g], n * PIECE:(n + 1) * PIECE, :]
                q_acc[:, n * HALF_COLS:(n + 1) * HALF_COLS] += dot(h_buf[r, c, g], w)

    for g in range(GROUPS):
        finish_piece(g)
    for g in range(GROUPS):
        use(SELF, 0, g)
    for g in range(GROUPS):
        arrive(SELF, 1, g)
        use(SELF, 1, g)
    for g in range(GROUPS):
        arrive(XN, 0, g)
        down = [copies.start(h_buf.at[XN, 0, g, top], h_buf.at[DIAG, 0, g, top], yn)]
        gather[XN, 1, g] = [copies.start(h_buf.at[XN, 0, g], h_buf.at[XN, 1, g], partner)]
        arrive(YN, 0, g)
        down += [copies.start(h_buf.at[YN, 0, g, bottom], h_buf.at[DIAG, 0, g, bottom], xn)]
        gather[DIAG, 0, g] = down
        gather[YN, 1, g] = [copies.start(h_buf.at[YN, 0, g], h_buf.at[YN, 1, g], partner)]
        use(XN, 0, g)
        use(YN, 0, g)
        arrive(XN, 1, g)
        use(XN, 1, g)
        arrive(YN, 1, g)
        use(YN, 1, g)
    for g in range(GROUPS):
        arrive(DIAG, 0, g)
        gather[DIAG, 1, g] = [copies.start(h_buf.at[DIAG, 0, g], h_buf.at[DIAG, 1, g], partner)]
        use(DIAG, 0, g)
    for g in range(GROUPS):
        arrive(DIAG, 1, g)
        use(DIAG, 1, g)

    if not last:
        arrivals = []
        for j in range(TILES):
            q_send[j] = q_acc[:, j * TILE:(j + 1) * TILE].astype(BF16).reshape(DEVICES, MY_ROWS, TILE)
            arrivals += send_query_tile(copies, me, j, q_send, q_out)
            q_out[j, me] = q_send[j, me]
        wk_load.wait()
        wv_load.wait()
        mine = pl.ds(pl.multiple_of(me * MY_ROWS, MY_ROWS), MY_ROWS)
        kn = jnp.zeros((MY_ROWS, HEAD_DIM), F32)
        vn = jnp.zeros((MY_ROWS, HEAD_DIM), F32)
        for r in (SELF, XN, YN, DIAG):
            for c in (0, 1):
                for g in range(GROUPS):
                    rows = h_buf[r, c, g, mine, :]
                    depth = pl.ds(column(r, c, g), PIECE)
                    kn += dot(rows, wk_buf[depth, :])
                    vn += dot(rows, wv_buf[depth, :])
        kn_out[...] = kn.astype(BF16)
        vn_out[...] = vn.astype(BF16)
        for copy in arrivals:
            copy.wait_recv()
        for load in cache_loads + own_stores:
            load.wait()
    copies.finish()


def combine_call(layer, last, ctx, residual, w_out, more):
    any_spec = pl.BlockSpec(memory_space=pl.ANY)
    vmem_spec = pl.BlockSpec(memory_space=pltpu.VMEM)
    sends = (DEVICES - 1) + GROUPS * (4 + 6 + 9)
    loads = 1 + SLOTS + 1
    scratch = [
        pltpu.VMEM((DEVICES, MY_ROWS, MY_HEADS, HEAD_DIM), BF16),
        pltpu.VMEM((ROWS, MY_COLS), BF16),
        pltpu.VMEM((ROWS, MY_COLS), BF16),
        pltpu.VMEM((SLOTS, MY_COLS, PIECE), BF16),
        pltpu.VMEM((GROUPS, 4, ROWS, PIECE), F32),
        pltpu.VMEM((GROUPS, 4, ROWS, PIECE), F32),
        pltpu.VMEM((GROUPS, 4, ROWS, PIECE), F32),
    ] + [pltpu.VMEM((GROUPS, HALF, PIECE), F32)] * 6 + [
        pltpu.VMEM((4, 2, GROUPS, ROWS, PIECE), BF16),
    ]
    if last:
        out_shape = pltpu.VMEM((ROWS, D_MODEL), BF16)
        out_specs = vmem_spec
    else:
        out_shape = (jax.ShapeDtypeStruct((ROWS, MY_COLS), BF16),) + QUERY_SHAPES
        out_specs = (any_spec,) + (vmem_spec,) * len(QUERY_SHAPES)
        sends += TILES * (DEVICES - 1)
        loads += 4 + 2 * SLOTS + GROUPS
        scratch += [
            pltpu.VMEM((D_MODEL, HEAD_DIM), BF16),
            pltpu.VMEM((D_MODEL, HEAD_DIM), BF16),
            pltpu.VMEM((ROWS, MY_COLS), F32),
            pltpu.VMEM((TILES, DEVICES, MY_ROWS, TILE), BF16),
        ]
    scratch += [
        pltpu.SemaphoreType.DMA((loads,)),
        pltpu.SemaphoreType.DMA((sends,)),
        pltpu.SemaphoreType.DMA((sends,)),
    ]
    return pl.pallas_call(
        functools.partial(combine_kernel, layer, last),
        name="combine_last" if last else "combine",
        out_shape=out_shape,
        in_specs=[vmem_spec] + [any_spec] * (2 + len(more)),
        out_specs=out_specs,
        scratch_shapes=scratch,
        compiler_params=pltpu.CompilerParams(
            collective_id=2 if last else 1, has_side_effects=True, vmem_limit_bytes=40 * MIB
        ),
    )(*in_vmem(ctx), *in_hbm(residual, w_out, *more))


def solution(mesh):
    cache_spec = P(None, ("replica", "model"), None, None)

    def device_step(x, cache_len, w_query, w_key, w_value, w_out, k_cache, v_cache):
        q, kn, vn, kv_pre = query_call(x, w_query, w_key, w_value, k_cache, v_cache)
        ctx, k_all, v_all = attend_call(0, cache_len, q, kn, vn, kv_pre, ())
        own, q, kn, vn, kv_pre = combine_call(
            0, False, ctx, x, w_out, (w_query, w_key, w_value, k_cache, v_cache))
        ctx, k_all, v_all = attend_call(1, cache_len, q, kn, vn, kv_pre, (k_all, v_all))
        out = combine_call(1, True, ctx, own, w_out, ())
        return out, k_all, v_all

    return jax.shard_map(
        device_step,
        mesh=mesh,
        in_specs=(P("replica", None), P("replica"), P(None, None, "model"), P(), P(), P(None, "model", None), cache_spec, cache_spec),
        out_specs=(P("replica", None), cache_spec, cache_spec),
        check_vma=False,
    )
```

```python
import functools

import jax
import jax.numpy as jnp
from jax import lax
from jax.experimental import pallas as pl
from jax.experimental.pallas import tpu as pltpu
from jax.sharding import PartitionSpec as P

MESH = pl.DeviceIdType.MESH
BF16 = jnp.bfloat16
F32 = jnp.float32
MIB = 1024 * 1024

DEVICES = 8
ROWS = 128
MY_ROWS = 16
D_MODEL = 8192
HEAD_DIM = 128
MY_HEADS = 8
NUM_HEADS = 64
MY_COLS = 1024
SEQ = 2048
TILE = 256
TILES = MY_COLS // TILE

HALF_COLS = 512
GROUPS = 2
PIECE = MY_COLS // GROUPS
HALF = ROWS // 2
SLOTS = 8 * GROUPS
TOGETHER = 8
SPANS = (256, 512, 1024, 2048)


def dot(a, b):
    return jnp.dot(a, b, preferred_element_type=F32)


def places():
    me = lax.axis_index("model")
    core = lax.rem(me, 2)
    x = lax.rem(lax.div(me, 2), 2)
    y = lax.div(me, 4)
    flip = 1 - 2 * core
    xn = me + 2 - 4 * x
    yn = me + 4 - 8 * y
    diag = xn + 4 - 8 * y
    return me, flip, xn, yn, diag


def await_all(ref, sem):
    pltpu.make_async_copy(ref, ref, sem).wait()


class Copies:
    def __init__(self, send_sems, recv_sems):
        self.send_sems, self.recv_sems, self.receives = send_sems, recv_sems, 0

    def new_receive(self):
        self.receives += 1
        return self.recv_sems.at[self.receives - 1]

    def start(self, src, dst, device, kind, recv_sem=None):
        copy = pltpu.make_async_remote_copy(
            src_ref=src,
            dst_ref=dst,
            send_sem=self.send_sems.at[kind],
            recv_sem=self.new_receive() if recv_sem is None else recv_sem,
            device_id={"model": device},
            device_id_type=MESH,
        )
        copy.start()
        return copy


def meet_all(me):
    barrier = pltpu.get_barrier_semaphore()
    for k in range(1, DEVICES):
        pl.semaphore_signal(barrier, inc=1, device_id={"model": lax.rem(me + k, DEVICES)}, device_id_type=MESH)
    pl.semaphore_wait(barrier, DEVICES - 1)


def send_query_tile(copies, me, j, q_send, q_out, kind, recv_sem):
    for k in range(1, DEVICES):
        to = lax.rem(me + k, DEVICES)
        copies.start(q_send.at[j, to], q_out.at[j, me], to, kind, recv_sem)
    q_out[j, me] = q_send[j, me]


def load_cache(layer, k_hbm, v_hbm, kv_pre, sem):
    for i, hbm in enumerate((k_hbm, v_hbm)):
        pltpu.make_async_copy(hbm.at[layer], kv_pre.at[i], sem).start()


def load_kv_weights(layer, wk_hbm, wv_hbm, wkv_buf, sem):
    for i, hbm in enumerate((wk_hbm, wv_hbm)):
        pltpu.make_async_copy(hbm.at[layer], wkv_buf.at[i], sem).start()


def in_vmem(*arrays):
    return [pltpu.with_memory_space_constraint(a, pltpu.VMEM) for a in arrays]


def in_hbm(*arrays):
    return [pltpu.with_memory_space_constraint(a, pltpu.HBM) for a in arrays]


QUERY_SHAPES = (
    pltpu.VMEM((TILES, DEVICES, MY_ROWS, TILE), BF16),
    pltpu.VMEM((MY_ROWS, HEAD_DIM), BF16),
    pltpu.VMEM((MY_ROWS, HEAD_DIM), BF16),
    pltpu.VMEM((2, MY_ROWS, SEQ, HEAD_DIM), BF16),
)


def query_kernel(x_hbm, wq_hbm, wk_hbm, wv_hbm, k_hbm, v_hbm, q_out, kn_out, vn_out, kv_pre,
                 x_buf, wq_buf, wkv_buf, q_send, load_sems, send_sems, recv_sems):
    me, _, _, _, _ = places()
    wkv_sem, cache_sem = load_sems.at[TILES + 1], load_sems.at[TILES + 2]
    x_load = pltpu.make_async_copy(x_hbm, x_buf, load_sems.at[TILES])
    x_load.start()
    wq_loads = [pltpu.make_async_copy(wq_hbm.at[0, :, pl.ds(j * TILE, TILE)], wq_buf.at[j], load_sems.at[j])
                for j in range(TILES)]
    for load in wq_loads:
        load.start()
    load_kv_weights(0, wk_hbm, wv_hbm, wkv_buf, wkv_sem)
    load_cache(0, k_hbm, v_hbm, kv_pre, cache_sem)
    meet_all(me)
    copies = Copies(send_sems, recv_sems)
    q_sem = copies.new_receive()
    x_load.wait()
    for j in range(TILES):
        wq_loads[j].wait()
        q_send[j] = dot(x_buf[...], wq_buf[j]).astype(BF16).reshape(DEVICES, MY_ROWS, TILE)
        send_query_tile(copies, me, j, q_send, q_out, 0, q_sem)
    x_rows = x_buf[pl.ds(pl.multiple_of(me * MY_ROWS, MY_ROWS), MY_ROWS), :]
    await_all(wkv_buf, wkv_sem)
    kn_out[...] = dot(x_rows, wkv_buf[0]).astype(BF16)
    vn_out[...] = dot(x_rows, wkv_buf[1]).astype(BF16)
    others = pl.ds(0, DEVICES - 1)
    await_all(q_out.at[:, others], q_sem)
    await_all(q_send.at[:, others], send_sems.at[0])
    await_all(kv_pre, cache_sem)


def query_call(x, w_query, w_key, w_value, k_cache, v_cache):
    any_spec = pl.BlockSpec(memory_space=pl.ANY)
    vmem_spec = pl.BlockSpec(memory_space=pltpu.VMEM)
    return pl.pallas_call(
        query_kernel,
        name="query",
        out_shape=QUERY_SHAPES,
        in_specs=[any_spec] * 6,
        out_specs=(vmem_spec,) * len(QUERY_SHAPES),
        scratch_shapes=[
            pltpu.VMEM((ROWS, D_MODEL), BF16),
            pltpu.VMEM((TILES, D_MODEL, TILE), BF16),
            pltpu.VMEM((2, D_MODEL, HEAD_DIM), BF16),
            pltpu.VMEM((TILES, DEVICES, MY_ROWS, TILE), BF16),
            pltpu.SemaphoreType.DMA((TILES + 3,)),
            pltpu.SemaphoreType.DMA((1,)),
            pltpu.SemaphoreType.DMA((1,)),
        ],
        compiler_params=pltpu.CompilerParams(
            collective_id=0, has_side_effects=True, vmem_limit_bytes=26 * MIB
        ),
    )(*in_hbm(x, w_query, w_key, w_value, k_cache, v_cache))


def attend_kernel(layer, has_prev, len_ref, q_ref, kn_ref, vn_ref, *refs):
    k_out, v_out, ctx_ref, kv_buf, q_buf, kn_buf, vn_buf, out_sems = refs[-8:]
    k_buf, v_buf = kv_buf.at[0], kv_buf.at[1]
    me = lax.axis_index("model")

    def save(which, b):
        hbm, buf = ((k_out, k_buf), (v_out, v_buf))[which]
        return pltpu.make_async_copy(buf.at[b], hbm.at[layer, b], out_sems.at[which])

    kn_buf[...] = kn_ref[...].astype(F32)
    vn_buf[...] = vn_ref[...].astype(F32)

    @pl.loop(0, MY_ROWS)
    def _(b):
        pos = len_ref[me * MY_ROWS + b]
        base = pl.multiple_of((pos // 16) * 16, 16)
        here = lax.broadcasted_iota(jnp.int32, (16, HEAD_DIM), 0) == pos - base
        for buf, new in ((k_buf, kn_buf), (v_buf, vn_buf)):
            tile = buf[b, pl.ds(base, 16), :].astype(F32)
            row = jnp.broadcast_to(new[pl.ds(b, 1), :], (16, HEAD_DIM))
            buf[b, pl.ds(base, 16), :] = jnp.where(here, row, tile).astype(BF16)

        @pl.when(b >= 1)
        def _():
            save(0, b - 1).start()
            save(1, b - 1).start()

    save(0, MY_ROWS - 1).start()
    save(1, MY_ROWS - 1).start()

    for j in range(TILES):
        for src in range(DEVICES):
            block = q_ref[j, src].astype(F32)
            for h in range(TILE // HEAD_DIM):
                head = src * MY_HEADS + j * (TILE // HEAD_DIM) + h
                q_buf[:, head, :] = block[:, h * HEAD_DIM:(h + 1) * HEAD_DIM]

    scale = HEAD_DIM ** -0.5

    def attend(rows, n):
        t = lax.broadcasted_iota(jnp.int32, (NUM_HEADS, n), 1)
        s = [lax.dot_general(q_buf[b].astype(BF16), k_buf[b, 0:n, :], (((1,), (1,)), ((), ())),
                             preferred_element_type=F32) for b in rows]
        s = [jnp.where(t <= len_ref[me * MY_ROWS + b], v * scale, -jnp.inf) for v, b in zip(s, rows)]
        peak = [jnp.max(v, axis=1, keepdims=True) for v in s]
        e = [jnp.exp(v - u) for v, u in zip(s, peak)]
        share = [1.0 / jnp.sum(v, axis=1, keepdims=True) for v in e]
        p = [(v * u).astype(BF16) for v, u in zip(e, share)]
        c = [dot(v, v_buf[b, 0:n, :]) for v, b in zip(p, rows)]
        for v, b in zip(c, rows):
            ctx_ref[:, b] = v.reshape(DEVICES, MY_HEADS, HEAD_DIM).astype(BF16)

    @pl.loop(0, MY_ROWS // TOGETHER)
    def _(i):
        attend([i * TOGETHER + k for k in range(TOGETHER)], SPANS[0])

    @pl.loop(0, MY_ROWS)
    def _(b):
        pos = len_ref[me * MY_ROWS + b]
        for low, n in zip(SPANS, SPANS[1:]):
            @pl.when(jnp.logical_and(pos >= low, pos < n))
            def _(n=n):
                attend([b], n)

    for which, hbm in enumerate((k_out, v_out)):
        await_all(hbm.at[layer], out_sems.at[which])


def attend_call(layer, cache_len, q, kn, vn, kv_pre, prev):
    any_spec = pl.BlockSpec(memory_space=pl.ANY)
    vmem_spec = pl.BlockSpec(memory_space=pltpu.VMEM)
    whole = jax.ShapeDtypeStruct((2,) + kv_pre.shape[1:], BF16)
    k_all, v_all, ctx, _ = pl.pallas_call(
        functools.partial(attend_kernel, layer, bool(prev)),
        name="attend",
        out_shape=(
            whole,
            whole,
            pltpu.VMEM((DEVICES, MY_ROWS, MY_HEADS, HEAD_DIM), BF16),
            pltpu.VMEM(kv_pre.shape, BF16),
        ),
        in_specs=[pl.BlockSpec(memory_space=pltpu.SMEM)] + [vmem_spec] * 4 + [any_spec] * len(prev),
        out_specs=(any_spec, any_spec, vmem_spec, vmem_spec),
        scratch_shapes=[
            pltpu.VMEM((MY_ROWS, NUM_HEADS, HEAD_DIM), F32),
            pltpu.VMEM((MY_ROWS, HEAD_DIM), F32),
            pltpu.VMEM((MY_ROWS, HEAD_DIM), F32),
            pltpu.SemaphoreType.DMA((2,)),
        ],
        input_output_aliases={4: 3} | ({5: 0, 6: 1} if prev else {}),
        compiler_params=pltpu.CompilerParams(vmem_limit_bytes=16 * MIB),
    )(cache_len, *in_vmem(q, kn, vn, kv_pre), *prev)
    return ctx, k_all, v_all


SELF, XN, YN, DIAG = range(4)
CONTEXT, CORE, SUMS, WHOLE, HALVES, QUERY = range(6)


def combine_kernel(layer, last, *refs):
    if last:
        (ctx_in, res_buf, wo_hbm, out_ref,
         ctx_buf, lhs, w_buf, send_d2d, recv_d2d, acc, rx_diag, ry_diag, rx_dir, ry_dir, rx_fwd, ry_fwd, h_buf,
         load_sems, send_sems, recv_sems) = refs
    else:
        (ctx_in, res_hbm, wo_hbm, wq_hbm, wk_hbm, wv_hbm, k_hbm, v_hbm, own_out, q_out, kn_out, vn_out, kv_pre,
         ctx_buf, lhs, res_buf, w_buf, send_d2d, recv_d2d, acc, rx_diag, ry_diag, rx_dir, ry_dir, rx_fwd, ry_fwd, h_buf,
         wkv_buf, q_acc, q_send,
         load_sems, send_sems, recv_sems) = refs
    me, flip, xn, yn, diag = places()
    partner = me + flip
    chip_mate = {SELF: me, XN: xn, YN: yn, DIAG: diag}
    owner = lambda r, c: chip_mate[r] + c * flip
    column = lambda r, c, g: pl.multiple_of(owner(r, c) * MY_COLS + g * PIECE, PIECE)
    copies = Copies(send_sems, recv_sems)
    order = (DIAG, XN, YN, SELF)
    steps = [(g, r) for g in range(GROUPS) for r in order]
    top, bottom = pl.ds(0, HALF), pl.ds(HALF, HALF)

    wo_slot, wo_loads = {}, []
    for g, r in steps:
        for c in (1, 0):
            slot = wo_slot[g, r, c] = len(wo_slot)
            wo_loads.append(pltpu.make_async_copy(
                wo_hbm.at[layer, :, pl.ds(column(r, c, g), PIECE)], w_buf.at[slot], load_sems.at[slot]))
            wo_loads[-1].start()
    if not last:
        res_sem, wkv_sem, cache_sem = [load_sems.at[SLOTS + i] for i in range(3)]
        res_load = pltpu.make_async_copy(
            res_hbm.at[:, pl.ds(pl.multiple_of(me * MY_COLS, MY_COLS), MY_COLS)], res_buf, res_sem)
        res_load.start()
        load_kv_weights(layer + 1, wk_hbm, wv_hbm, wkv_buf, wkv_sem)
    wq_order = [(r, c, g) for r in (SELF, XN, YN, DIAG) for c in (0, 1) for g in range(GROUPS)]
    wq_slot = {}

    def refill(slot):
        if last:
            return
        r, c, g = wq_order[len(wq_slot)]
        wq_slot[r, c, g] = slot
        rows = pl.ds(column(r, c, g), PIECE)
        for n in range(MY_COLS // HALF_COLS):
            pltpu.make_async_copy(
                wq_hbm.at[layer + 1, rows, pl.ds(n * HALF_COLS, HALF_COLS)],
                w_buf.at[slot, pl.ds(n * PIECE, PIECE), :], load_sems.at[slot]).start()

    meet_all(me)

    ctx_sem = copies.new_receive()
    for k in range(1, DEVICES):
        to = lax.rem(me + k, DEVICES)
        copies.start(ctx_in.at[to], ctx_buf.at[me], to, CONTEXT, ctx_sem)
    ctx_buf[me] = ctx_in[me]
    await_all(ctx_buf.at[pl.ds(0, DEVICES - 1)], ctx_sem)
    for src in range(DEVICES):
        rows = ctx_buf[src].astype(F32).reshape(MY_ROWS, MY_COLS).astype(BF16)
        lhs[src * MY_ROWS:(src + 1) * MY_ROWS, :] = rows

    d2d = {}
    first, direct, forward = {}, {}, {}

    def settle(g, r):
        d2d[g, r].wait_recv()
        acc[g, r] += recv_d2d[g, r]
        if r == DIAG:
            first[g, 0] = copies.start(acc.at[g, r, top], rx_diag.at[g], xn, SUMS)
            first[g, 1] = copies.start(acc.at[g, r, bottom], ry_diag.at[g], yn, SUMS)

    def send_direct(g):
        direct[g, 0] = copies.start(acc.at[g, XN, top], rx_dir.at[g], xn, SUMS)
        direct[g, 1] = copies.start(acc.at[g, YN, bottom], ry_dir.at[g], yn, SUMS)

    pending = None
    for g, r in steps:
        for c, target in ((1, send_d2d), (0, acc)):
            wo_loads[wo_slot[g, r, c]].wait()
            target[g, r] = dot(lhs[...], w_buf[wo_slot[g, r, c]])
            refill(wo_slot[g, r, c])
            if c == 1:
                d2d[g, r] = copies.start(send_d2d.at[g, r], recv_d2d.at[g, r], partner, CORE)
        if pending is not None:
            settle(*pending)
            if pending == (0, YN):
                send_direct(0)
        pending = (g, r)
    settle(*pending)
    if not last:
        load_cache(layer + 1, k_hbm, v_hbm, kv_pre, cache_sem)

    for g in range(GROUPS):
        first[g, 0].wait_recv()
        acc[g, YN, top] += rx_diag[g]
        forward[g, 1] = copies.start(acc.at[g, YN, top], ry_fwd.at[g], yn, SUMS)
        first[g, 1].wait_recv()
        acc[g, XN, bottom] += ry_diag[g]
        forward[g, 0] = copies.start(acc.at[g, XN, bottom], rx_fwd.at[g], xn, SUMS)
        if g + 1 < GROUPS:
            send_direct(g + 1)

    if not last:
        res_load.wait()
    gather = {}

    def finish_piece(g):
        cols = slice(g * PIECE, (g + 1) * PIECE)
        direct[g, 0].wait_recv()
        forward[g, 1].wait_recv()
        total = acc[g, SELF, top] + rx_dir[g] + ry_fwd[g]
        h_buf[SELF, 0, g, top] = (res_buf[top, cols].astype(F32) + total).astype(BF16)
        direct[g, 1].wait_recv()
        forward[g, 0].wait_recv()
        total = acc[g, SELF, bottom] + ry_dir[g] + rx_fwd[g]
        h_buf[SELF, 0, g, bottom] = (res_buf[bottom, cols].astype(F32) + total).astype(BF16)
        mine = h_buf.at[SELF, 0, g]
        gather[XN, 0, g] = copies.start(mine, h_buf.at[XN, 0, g], xn, WHOLE)
        gather[YN, 0, g] = copies.start(mine, h_buf.at[YN, 0, g], yn, WHOLE)
        gather[SELF, 1, g] = copies.start(mine, h_buf.at[SELF, 1, g], partner, WHOLE)
        if not last:
            own_out[:, cols] = h_buf[SELF, 0, g]

    def arrive(r, c, g):
        gather[r, c, g].wait_recv()

    if last:
        def use(r, c, g):
            out_ref[:, pl.ds(column(r, c, g), PIECE)] = h_buf[r, c, g]
    else:
        q_acc[...] = jnp.zeros_like(q_acc)

        def use(r, c, g):
            slot = wq_slot[r, c, g]
            await_all(w_buf.at[slot], load_sems.at[slot])
            for n in range(MY_COLS // HALF_COLS):
                w = w_buf[slot, n * PIECE:(n + 1) * PIECE, :]
                q_acc[:, n * HALF_COLS:(n + 1) * HALF_COLS] += dot(h_buf[r, c, g], w)

    for g in range(GROUPS):
        finish_piece(g)
    for g in range(GROUPS):
        use(SELF, 0, g)
    for g in range(GROUPS):
        arrive(SELF, 1, g)
        use(SELF, 1, g)
    diag_sems = {}
    for g in range(GROUPS):
        diag_sem = diag_sems[g] = copies.new_receive()
        arrive(XN, 0, g)
        copies.start(h_buf.at[XN, 0, g, top], h_buf.at[DIAG, 0, g, top], yn, HALVES, diag_sem)
        gather[XN, 1, g] = copies.start(h_buf.at[XN, 0, g], h_buf.at[XN, 1, g], partner, WHOLE)
        arrive(YN, 0, g)
        copies.start(h_buf.at[YN, 0, g, bottom], h_buf.at[DIAG, 0, g, bottom], xn, HALVES, diag_sem)
        gather[YN, 1, g] = copies.start(h_buf.at[YN, 0, g], h_buf.at[YN, 1, g], partner, WHOLE)
        use(XN, 0, g)
        use(YN, 0, g)
        arrive(XN, 1, g)
        use(XN, 1, g)
        arrive(YN, 1, g)
        use(YN, 1, g)
    for g in range(GROUPS):
        await_all(h_buf.at[DIAG, 0, g], diag_sems[g])
        gather[DIAG, 1, g] = copies.start(h_buf.at[DIAG, 0, g], h_buf.at[DIAG, 1, g], partner, WHOLE)
        use(DIAG, 0, g)
    for g in range(GROUPS):
        arrive(DIAG, 1, g)
        use(DIAG, 1, g)

    if not last:
        q_sem = copies.new_receive()
        for j in range(TILES):
            q_send[j] = q_acc[:, j * TILE:(j + 1) * TILE].astype(BF16).reshape(DEVICES, MY_ROWS, TILE)
            send_query_tile(copies, me, j, q_send, q_out, QUERY, q_sem)
        await_all(wkv_buf, wkv_sem)
        mine = pl.ds(pl.multiple_of(me * MY_ROWS, MY_ROWS), MY_ROWS)
        kn = jnp.zeros((MY_ROWS, HEAD_DIM), F32)
        vn = jnp.zeros((MY_ROWS, HEAD_DIM), F32)
        for r in (SELF, XN, YN, DIAG):
            for c in (0, 1):
                for g in range(GROUPS):
                    rows = h_buf[r, c, g, mine, :]
                    depth = pl.ds(column(r, c, g), PIECE)
                    kn += dot(rows, wkv_buf[0, depth, :])
                    vn += dot(rows, wkv_buf[1, depth, :])
        kn_out[...] = kn.astype(BF16)
        vn_out[...] = vn.astype(BF16)
        others = pl.ds(0, DEVICES - 1)
        await_all(q_out.at[:, others], q_sem)
        await_all(q_send.at[:, others], send_sems.at[QUERY])
        await_all(kv_pre, cache_sem)
    await_all(ctx_in.at[pl.ds(0, DEVICES - 1)], send_sems.at[CONTEXT])
    await_all(send_d2d, send_sems.at[CORE])
    await_all(acc.at[:, pl.ds(0, 3)], send_sems.at[SUMS])
    await_all(h_buf.at[pl.ds(0, 3)], send_sems.at[WHOLE])
    await_all(h_buf.at[0, 0], send_sems.at[HALVES])


def combine_call(layer, last, ctx, residual, w_out, more):
    any_spec = pl.BlockSpec(memory_space=pl.ANY)
    vmem_spec = pl.BlockSpec(memory_space=pltpu.VMEM)
    receives = (1 if last else 2) + GROUPS * (4 + 6 + 7)
    scratch = [
        pltpu.VMEM((DEVICES, MY_ROWS, MY_HEADS, HEAD_DIM), BF16),
        pltpu.VMEM((ROWS, MY_COLS), BF16),
        pltpu.VMEM((SLOTS, MY_COLS, PIECE), BF16),
        pltpu.VMEM((GROUPS, 4, ROWS, PIECE), F32),
        pltpu.VMEM((GROUPS, 4, ROWS, PIECE), F32),
        pltpu.VMEM((GROUPS, 4, ROWS, PIECE), F32),
    ] + [pltpu.VMEM((GROUPS, HALF, PIECE), F32)] * 6 + [
        pltpu.VMEM((4, 2, GROUPS, ROWS, PIECE), BF16),
    ]
    if last:
        out_shape = pltpu.VMEM((ROWS, D_MODEL), BF16)
        out_specs = vmem_spec
    else:
        out_shape = (pltpu.VMEM((ROWS, MY_COLS), BF16),) + QUERY_SHAPES
        out_specs = (vmem_spec,) * len(out_shape)
        scratch.insert(2, pltpu.VMEM((ROWS, MY_COLS), BF16))
        scratch += [
            pltpu.VMEM((2, D_MODEL, HEAD_DIM), BF16),
            pltpu.VMEM((ROWS, MY_COLS), F32),
            pltpu.VMEM((TILES, DEVICES, MY_ROWS, TILE), BF16),
        ]
    scratch += [
        pltpu.SemaphoreType.DMA((SLOTS + (0 if last else 3),)),
        pltpu.SemaphoreType.DMA((5 if last else 6,)),
        pltpu.SemaphoreType.DMA((receives,)),
    ]
    return pl.pallas_call(
        functools.partial(combine_kernel, layer, last),
        name="combine_last" if last else "combine",
        out_shape=out_shape,
        in_specs=[vmem_spec, vmem_spec if last else any_spec] + [any_spec] * (1 + len(more)),
        out_specs=out_specs,
        scratch_shapes=scratch,
        compiler_params=pltpu.CompilerParams(
            collective_id=2 if last else 1, has_side_effects=True, vmem_limit_bytes=40 * MIB
        ),
    )(*in_vmem(ctx), *(in_vmem if last else in_hbm)(residual), *in_hbm(w_out, *more))


def solution(mesh):
    cache_spec = P(None, ("replica", "model"), None, None)

    def device_step(x, cache_len, w_query, w_key, w_value, w_out, k_cache, v_cache):
        q, kn, vn, kv_pre = query_call(x, w_query, w_key, w_value, k_cache, v_cache)
        ctx, k_all, v_all = attend_call(0, cache_len, q, kn, vn, kv_pre, ())
        own, q, kn, vn, kv_pre = combine_call(
            0, False, ctx, x, w_out, (w_query, w_key, w_value, k_cache, v_cache))
        ctx, k_all, v_all = attend_call(1, cache_len, q, kn, vn, kv_pre, (k_all, v_all))
        out = combine_call(1, True, ctx, own, w_out, ())
        return out, k_all, v_all

    return jax.shard_map(
        device_step,
        mesh=mesh,
        in_specs=(P("replica", None), P("replica"), P(None, None, "model"), P(), P(), P(None, "model", None), cache_spec, cache_spec),
        out_specs=(P("replica", None), cache_spec, cache_spec),
        check_vma=False,
    )
```

```python
import functools

import jax
import jax.numpy as jnp
from jax import lax
from jax.experimental import pallas as pl
from jax.experimental.pallas import tpu as pltpu
from jax.sharding import PartitionSpec as P

MESH = pl.DeviceIdType.MESH
BF16 = jnp.bfloat16
F32 = jnp.float32
MIB = 1024 * 1024

DEVICES = 8
ROWS = 128
MY_ROWS = 16
D_MODEL = 8192
HEAD_DIM = 128
MY_HEADS = 8
NUM_HEADS = 64
MY_COLS = 1024
SEQ = 2048
TILE = 256
TILES = MY_COLS // TILE

HALF_COLS = 512
GROUPS = 2
PIECE = MY_COLS // GROUPS
HALF = ROWS // 2
SLOTS = 8 * GROUPS
LATE_ROWS = 4
TOGETHER = 8
SPANS = (256, 512, 1024, 2048)


def dot(a, b):
    return jnp.dot(a, b, preferred_element_type=F32)


def places():
    me = lax.axis_index("model")
    core = lax.rem(me, 2)
    x = lax.rem(lax.div(me, 2), 2)
    y = lax.div(me, 4)
    flip = 1 - 2 * core
    xn = me + 2 - 4 * x
    yn = me + 4 - 8 * y
    diag = xn + 4 - 8 * y
    return me, flip, xn, yn, diag


def await_all(ref, sem):
    pltpu.make_async_copy(ref, ref, sem).wait()


class Copies:
    def __init__(self, send_sems, recv_sems):
        self.send_sems, self.recv_sems, self.receives = send_sems, recv_sems, 0

    def new_receive(self):
        self.receives += 1
        return self.recv_sems.at[self.receives - 1]

    def start(self, src, dst, device, kind, recv_sem=None):
        copy = pltpu.make_async_remote_copy(
            src_ref=src,
            dst_ref=dst,
            send_sem=self.send_sems.at[kind],
            recv_sem=self.new_receive() if recv_sem is None else recv_sem,
            device_id={"model": device},
            device_id_type=MESH,
        )
        copy.start()
        return copy


def meet_all(me):
    barrier = pltpu.get_barrier_semaphore()
    for k in range(1, DEVICES):
        pl.semaphore_signal(barrier, inc=1, device_id={"model": lax.rem(me + k, DEVICES)}, device_id_type=MESH)
    pl.semaphore_wait(barrier, DEVICES - 1)


def others():
    me, flip, xn, yn, diag = places()
    return [diag, diag + flip, xn, yn, xn + flip, yn + flip, me + flip]


def send_query_tile(copies, me, j, q_send, q_out, kind, recv_sem):
    for to in others():
        copies.start(q_send.at[j, to], q_out.at[j, me], to, kind, recv_sem)
    q_out[j, me] = q_send[j, me]


def load_cache(layer, rows, k_hbm, v_hbm, kv, sem):
    for i, hbm in enumerate((k_hbm, v_hbm)):
        pltpu.make_async_copy(hbm.at[layer, rows], kv.at[i, rows], sem).start()


def load_kv_weights(layer, core, wk_hbm, wv_hbm, wkv_buf, sem):
    for i, hbm in enumerate((wk_hbm, wv_hbm)):
        @pl.when(core == i)
        def _():
            pltpu.make_async_copy(hbm.at[layer], wkv_buf, sem).start()


def share_new_rows(copies, core, partner, made, kv_send, kv_out, kind):
    kv_send[...] = made.reshape(2, MY_ROWS, HEAD_DIM).astype(BF16)
    copy = copies.start(kv_send.at[1 - core], kv_out.at[core], partner, kind)
    kv_out[core] = kv_send[core]
    return copy


def in_vmem(*arrays):
    return [pltpu.with_memory_space_constraint(a, pltpu.VMEM) for a in arrays]


def in_hbm(*arrays):
    return [pltpu.with_memory_space_constraint(a, pltpu.HBM) for a in arrays]


QUERY_SHAPES = (
    pltpu.VMEM((TILES, DEVICES, MY_ROWS, TILE), BF16),
    pltpu.VMEM((2, MY_ROWS, HEAD_DIM), BF16),
    pltpu.VMEM((2, MY_ROWS, SEQ, HEAD_DIM), BF16),
)


def query_kernel(x_hbm, wq_hbm, wk_hbm, wv_hbm, k_hbm, v_hbm, q_out, kv_out, kv_pre,
                 x_buf, wq_buf, wkv_buf, q_send, kv_send, load_sems, send_sems, recv_sems):
    me, flip, _, _, _ = places()
    core = lax.rem(me, 2)
    wkv_sem, cache_sem = load_sems.at[TILES + 1], load_sems.at[TILES + 2]
    x_load = pltpu.make_async_copy(x_hbm, x_buf, load_sems.at[TILES])
    x_load.start()
    wq_loads = [pltpu.make_async_copy(wq_hbm.at[0, :, pl.ds(j * TILE, TILE)], wq_buf.at[j], load_sems.at[j])
                for j in range(TILES)]
    for load in wq_loads:
        load.start()
    load_kv_weights(0, core, wk_hbm, wv_hbm, wkv_buf, wkv_sem)
    early = pl.ds(0, MY_ROWS - LATE_ROWS)
    load_cache(0, early, k_hbm, v_hbm, kv_pre, cache_sem)
    meet_all(me)
    copies = Copies(send_sems, recv_sems)
    q_sem = copies.new_receive()
    x_load.wait()
    for j in range(TILES):
        wq_loads[j].wait()
        q_send[j] = dot(x_buf[...], wq_buf[j]).astype(BF16).reshape(DEVICES, MY_ROWS, TILE)
        send_query_tile(copies, me, j, q_send, q_out, 0, q_sem)
    chip_rows = pl.ds(pl.multiple_of((me - core) * MY_ROWS, 2 * MY_ROWS), 2 * MY_ROWS)
    await_all(wkv_buf, wkv_sem)
    shared = share_new_rows(copies, core, me + flip, dot(x_buf[chip_rows, :], wkv_buf[...]), kv_send, kv_out, 1)
    seven = pl.ds(0, DEVICES - 1)
    await_all(q_out.at[:, seven], q_sem)
    shared.wait()
    await_all(q_send.at[:, seven], send_sems.at[0])
    await_all(kv_pre.at[:, early], cache_sem)


def query_call(x, w_query, w_key, w_value, k_cache, v_cache):
    any_spec = pl.BlockSpec(memory_space=pl.ANY)
    vmem_spec = pl.BlockSpec(memory_space=pltpu.VMEM)
    return pl.pallas_call(
        query_kernel,
        name="query",
        out_shape=QUERY_SHAPES,
        in_specs=[any_spec] * 6,
        out_specs=(vmem_spec,) * len(QUERY_SHAPES),
        scratch_shapes=[
            pltpu.VMEM((ROWS, D_MODEL), BF16),
            pltpu.VMEM((TILES, D_MODEL, TILE), BF16),
            pltpu.VMEM((D_MODEL, HEAD_DIM), BF16),
            pltpu.VMEM((TILES, DEVICES, MY_ROWS, TILE), BF16),
            pltpu.VMEM((2, MY_ROWS, HEAD_DIM), BF16),
            pltpu.SemaphoreType.DMA((TILES + 3,)),
            pltpu.SemaphoreType.DMA((2,)),
            pltpu.SemaphoreType.DMA((2,)),
        ],
        compiler_params=pltpu.CompilerParams(
            collective_id=0, has_side_effects=True, vmem_limit_bytes=26 * MIB
        ),
    )(*in_hbm(x, w_query, w_key, w_value, k_cache, v_cache))


def attend_kernel(layer, late_rows, len_hbm, q_ref, new_ref, *refs):
    k_hbm, v_hbm = refs[1:3]
    k_out, v_out, ctx_ref, kv_buf, len_ref, q_buf, new_buf, sems = refs[-8:]
    k_buf, v_buf = kv_buf.at[0], kv_buf.at[1]
    me = lax.axis_index("model")
    out_sems, len_sem, late_sem = (sems.at[0], sems.at[1]), sems.at[2], sems.at[3]
    len_load = pltpu.make_async_copy(len_hbm, len_ref, len_sem)
    len_load.start()
    late = pl.ds(MY_ROWS - late_rows, late_rows)
    if late_rows:
        load_cache(layer, late, k_hbm, v_hbm, kv_buf, late_sem)

    def save(which, b):
        hbm, buf = ((k_out, k_buf), (v_out, v_buf))[which]
        return pltpu.make_async_copy(buf.at[b], hbm.at[layer, b], out_sems[which])

    new_buf[...] = new_ref[...].astype(F32)
    for j in range(TILES):
        for src in range(DEVICES):
            block = q_ref[j, src].astype(F32)
            for h in range(TILE // HEAD_DIM):
                head = src * MY_HEADS + j * (TILE // HEAD_DIM) + h
                q_buf[:, head, :] = block[:, h * HEAD_DIM:(h + 1) * HEAD_DIM]

    def write_tokens(first, last):
        @pl.loop(first, last)
        def _(b):
            pos = len_ref[me * MY_ROWS + b]
            base = pl.multiple_of((pos // 16) * 16, 16)
            here = lax.broadcasted_iota(jnp.int32, (16, HEAD_DIM), 0) == pos - base
            for i, buf in enumerate((k_buf, v_buf)):
                tile = buf[b, pl.ds(base, 16), :].astype(F32)
                row = jnp.broadcast_to(new_buf[i, pl.ds(b, 1), :], (16, HEAD_DIM))
                buf[b, pl.ds(base, 16), :] = jnp.where(here, row, tile).astype(BF16)

            @pl.when(b > first)
            def _():
                save(0, b - 1).start()
                save(1, b - 1).start()

        save(0, last - 1).start()
        save(1, last - 1).start()

    len_load.wait()
    write_tokens(0, MY_ROWS - late_rows)
    if late_rows:
        await_all(kv_buf.at[:, late], late_sem)
        write_tokens(MY_ROWS - late_rows, MY_ROWS)

    scale = HEAD_DIM ** -0.5

    def attend(rows, n):
        t = lax.broadcasted_iota(jnp.int32, (NUM_HEADS, n), 1)
        s = [lax.dot_general(q_buf[b].astype(BF16), k_buf[b, 0:n, :], (((1,), (1,)), ((), ())),
                             preferred_element_type=F32) for b in rows]
        s = [jnp.where(t <= len_ref[me * MY_ROWS + b], v * scale, -jnp.inf) for v, b in zip(s, rows)]
        peak = [jnp.max(v, axis=1, keepdims=True) for v in s]
        e = [jnp.exp(v - u) for v, u in zip(s, peak)]
        share = [1.0 / jnp.sum(v, axis=1, keepdims=True) for v in e]
        p = [(v * u).astype(BF16) for v, u in zip(e, share)]
        c = [dot(v, v_buf[b, 0:n, :]) for v, b in zip(p, rows)]
        for v, b in zip(c, rows):
            ctx_ref[:, b] = v.reshape(DEVICES, MY_HEADS, HEAD_DIM).astype(BF16)

    @pl.loop(0, MY_ROWS // TOGETHER)
    def _(i):
        attend([i * TOGETHER + k for k in range(TOGETHER)], SPANS[0])

    @pl.loop(0, MY_ROWS)
    def _(b):
        pos = len_ref[me * MY_ROWS + b]
        for low, n in zip(SPANS, SPANS[1:]):
            @pl.when(jnp.logical_and(pos >= low, pos < n))
            def _(n=n):
                attend([b], n)

    for which, hbm in enumerate((k_out, v_out)):
        await_all(hbm.at[layer], out_sems[which])


def attend_call(layer, late_rows, cache_len, q, kv_new, kv_pre, k_cache, v_cache, prev):
    any_spec = pl.BlockSpec(memory_space=pl.ANY)
    vmem_spec = pl.BlockSpec(memory_space=pltpu.VMEM)
    k_all, v_all, ctx, _ = pl.pallas_call(
        functools.partial(attend_kernel, layer, late_rows),
        name="attend",
        out_shape=(
            jax.ShapeDtypeStruct(k_cache.shape, BF16),
            jax.ShapeDtypeStruct(v_cache.shape, BF16),
            pltpu.VMEM((DEVICES, MY_ROWS, MY_HEADS, HEAD_DIM), BF16),
            pltpu.VMEM(kv_pre.shape, BF16),
        ),
        in_specs=[any_spec] + [vmem_spec] * 3 + [any_spec] * (2 + len(prev)),
        out_specs=(any_spec, any_spec, vmem_spec, vmem_spec),
        scratch_shapes=[
            pltpu.SMEM((ROWS,), jnp.int32),
            pltpu.VMEM((MY_ROWS, NUM_HEADS, HEAD_DIM), F32),
            pltpu.VMEM((2, MY_ROWS, HEAD_DIM), F32),
            pltpu.SemaphoreType.DMA((4,)),
        ],
        input_output_aliases={3: 3} | ({6: 0, 7: 1} if prev else {}),
        compiler_params=pltpu.CompilerParams(vmem_limit_bytes=16 * MIB),
    )(*in_hbm(cache_len), *in_vmem(q, kv_new, kv_pre), *in_hbm(k_cache, v_cache), *prev)
    return ctx, k_all, v_all


SELF, XN, YN, DIAG = range(4)
CONTEXT, CORE, SUMS, WHOLE, HALVES, QUERY, NEW_ROWS = range(7)


def combine_kernel(layer, last, *refs):
    if last:
        (ctx_in, res_buf, wo_hbm, out_ref,
         ctx_buf, lhs, w_buf, send_d2d, recv_d2d, acc, rx_diag, ry_diag, rx_dir, ry_dir, rx_fwd, ry_fwd, h_buf,
         load_sems, send_sems, recv_sems) = refs
    else:
        (ctx_in, res_hbm, wo_hbm, wq_hbm, wk_hbm, wv_hbm, k_hbm, v_hbm, own_out, q_out, kv_out, kv_pre,
         ctx_buf, lhs, res_buf, w_buf, send_d2d, recv_d2d, acc, rx_diag, ry_diag, rx_dir, ry_dir, rx_fwd, ry_fwd, h_buf,
         wkv_buf, q_acc, q_send, kv_send,
         load_sems, send_sems, recv_sems) = refs
    me, flip, xn, yn, diag = places()
    partner, core = me + flip, lax.rem(me, 2)
    chip_mate = {SELF: me, XN: xn, YN: yn, DIAG: diag}
    owner = lambda r, c: chip_mate[r] + c * flip
    column = lambda r, c, g: pl.multiple_of(owner(r, c) * MY_COLS + g * PIECE, PIECE)
    copies = Copies(send_sems, recv_sems)
    order = (DIAG, XN, YN, SELF)
    steps = [(g, r) for g in range(GROUPS) for r in order]
    top, bottom = pl.ds(0, HALF), pl.ds(HALF, HALF)

    wo_slot, wo_loads = {}, []
    for g, r in steps:
        for c in (1, 0):
            slot = wo_slot[g, r, c] = len(wo_slot)
            wo_loads.append(pltpu.make_async_copy(
                wo_hbm.at[layer, :, pl.ds(column(r, c, g), PIECE)], w_buf.at[slot], load_sems.at[slot]))
            wo_loads[-1].start()
    if not last:
        res_sem, wkv_sem, cache_sem = [load_sems.at[SLOTS + i] for i in range(3)]
        res_load = pltpu.make_async_copy(
            res_hbm.at[:, pl.ds(pl.multiple_of(me * MY_COLS, MY_COLS), MY_COLS)], res_buf, res_sem)
        res_load.start()
        load_kv_weights(layer + 1, core, wk_hbm, wv_hbm, wkv_buf, wkv_sem)
    wq_order = [(r, c, g) for r in (SELF, XN, YN, DIAG) for c in (0, 1) for g in range(GROUPS)]
    wq_slot = {}

    def refill(slot):
        if last:
            return
        r, c, g = wq_order[len(wq_slot)]
        wq_slot[r, c, g] = slot
        rows = pl.ds(column(r, c, g), PIECE)
        for n in range(MY_COLS // HALF_COLS):
            pltpu.make_async_copy(
                wq_hbm.at[layer + 1, rows, pl.ds(n * HALF_COLS, HALF_COLS)],
                w_buf.at[slot, pl.ds(n * PIECE, PIECE), :], load_sems.at[slot]).start()

    meet_all(me)

    ctx_sem = copies.new_receive()
    for to in others():
        copies.start(ctx_in.at[to], ctx_buf.at[me], to, CONTEXT, ctx_sem)
    ctx_buf[me] = ctx_in[me]
    await_all(ctx_buf.at[pl.ds(0, DEVICES - 1)], ctx_sem)
    for src in range(DEVICES):
        rows = ctx_buf[src].astype(F32).reshape(MY_ROWS, MY_COLS).astype(BF16)
        lhs[src * MY_ROWS:(src + 1) * MY_ROWS, :] = rows

    d2d = {}
    first, direct, forward = {}, {}, {}

    def settle(g, r):
        d2d[g, r].wait_recv()
        acc[g, r] += recv_d2d[g, r]
        if r == DIAG:
            first[g, 0] = copies.start(acc.at[g, r, top], rx_diag.at[g], xn, SUMS)
            first[g, 1] = copies.start(acc.at[g, r, bottom], ry_diag.at[g], yn, SUMS)

    def send_direct(g):
        direct[g, 0] = copies.start(acc.at[g, XN, top], rx_dir.at[g], xn, SUMS)
        direct[g, 1] = copies.start(acc.at[g, YN, bottom], ry_dir.at[g], yn, SUMS)

    pending = None
    for g, r in steps:
        for c, target in ((1, send_d2d), (0, acc)):
            wo_loads[wo_slot[g, r, c]].wait()
            target[g, r] = dot(lhs[...], w_buf[wo_slot[g, r, c]])
            refill(wo_slot[g, r, c])
            if c == 1:
                d2d[g, r] = copies.start(send_d2d.at[g, r], recv_d2d.at[g, r], partner, CORE)
        if pending is not None:
            settle(*pending)
            if pending == (0, YN):
                send_direct(0)
        pending = (g, r)
    settle(*pending)
    if not last:
        load_cache(layer + 1, pl.ds(0, MY_ROWS), k_hbm, v_hbm, kv_pre, cache_sem)

    for g in range(GROUPS):
        first[g, 0].wait_recv()
        acc[g, YN, top] += rx_diag[g]
        forward[g, 1] = copies.start(acc.at[g, YN, top], ry_fwd.at[g], yn, SUMS)
        first[g, 1].wait_recv()
        acc[g, XN, bottom] += ry_diag[g]
        forward[g, 0] = copies.start(acc.at[g, XN, bottom], rx_fwd.at[g], xn, SUMS)
        if g + 1 < GROUPS:
            send_direct(g + 1)

    if not last:
        res_load.wait()
    gather = {}

    def finish_piece(g):
        cols = slice(g * PIECE, (g + 1) * PIECE)
        direct[g, 0].wait_recv()
        forward[g, 1].wait_recv()
        total = acc[g, SELF, top] + rx_dir[g] + ry_fwd[g]
        h_buf[SELF, 0, g, top] = (res_buf[top, cols].astype(F32) + total).astype(BF16)
        direct[g, 1].wait_recv()
        forward[g, 0].wait_recv()
        total = acc[g, SELF, bottom] + ry_dir[g] + rx_fwd[g]
        h_buf[SELF, 0, g, bottom] = (res_buf[bottom, cols].astype(F32) + total).astype(BF16)
        mine = h_buf.at[SELF, 0, g]
        gather[XN, 0, g] = copies.start(mine, h_buf.at[XN, 0, g], xn, WHOLE)
        gather[YN, 0, g] = copies.start(mine, h_buf.at[YN, 0, g], yn, WHOLE)
        gather[SELF, 1, g] = copies.start(mine, h_buf.at[SELF, 1, g], partner, WHOLE)
        if not last:
            own_out[:, cols] = h_buf[SELF, 0, g]

    def arrive(r, c, g):
        gather[r, c, g].wait_recv()

    if last:
        def use(r, c, g):
            out_ref[:, pl.ds(column(r, c, g), PIECE)] = h_buf[r, c, g]
    else:
        q_acc[...] = jnp.zeros_like(q_acc)

        def use(r, c, g):
            slot = wq_slot[r, c, g]
            await_all(w_buf.at[slot], load_sems.at[slot])
            for n in range(MY_COLS // HALF_COLS):
                w = w_buf[slot, n * PIECE:(n + 1) * PIECE, :]
                q_acc[:, n * HALF_COLS:(n + 1) * HALF_COLS] += dot(h_buf[r, c, g], w)

    for g in range(GROUPS):
        finish_piece(g)
    for g in range(GROUPS):
        use(SELF, 0, g)
    for g in range(GROUPS):
        arrive(SELF, 1, g)
        use(SELF, 1, g)
    diag_sems = {}
    for g in range(GROUPS):
        diag_sem = diag_sems[g] = copies.new_receive()
        arrive(XN, 0, g)
        copies.start(h_buf.at[XN, 0, g, top], h_buf.at[DIAG, 0, g, top], yn, HALVES, diag_sem)
        gather[XN, 1, g] = copies.start(h_buf.at[XN, 0, g], h_buf.at[XN, 1, g], partner, WHOLE)
        arrive(YN, 0, g)
        copies.start(h_buf.at[YN, 0, g, bottom], h_buf.at[DIAG, 0, g, bottom], xn, HALVES, diag_sem)
        gather[YN, 1, g] = copies.start(h_buf.at[YN, 0, g], h_buf.at[YN, 1, g], partner, WHOLE)
        use(XN, 0, g)
        use(YN, 0, g)
        arrive(XN, 1, g)
        use(XN, 1, g)
        arrive(YN, 1, g)
        use(YN, 1, g)
    for g in range(GROUPS):
        await_all(h_buf.at[DIAG, 0, g], diag_sems[g])
        gather[DIAG, 1, g] = copies.start(h_buf.at[DIAG, 0, g], h_buf.at[DIAG, 1, g], partner, WHOLE)
        use(DIAG, 0, g)
    for g in range(GROUPS):
        arrive(DIAG, 1, g)
        use(DIAG, 1, g)

    if not last:
        q_sem = copies.new_receive()
        for j in range(TILES):
            q_send[j] = q_acc[:, j * TILE:(j + 1) * TILE].astype(BF16).reshape(DEVICES, MY_ROWS, TILE)
            q_out[j, me] = q_send[j, me]
        for to in others():
            copies.start(q_send.at[:, to], q_out.at[:, me], to, QUERY, q_sem)
        await_all(wkv_buf, wkv_sem)
        chip_rows = pl.ds(pl.multiple_of((me - core) * MY_ROWS, 2 * MY_ROWS), 2 * MY_ROWS)
        made = jnp.zeros((2 * MY_ROWS, HEAD_DIM), F32)
        for r in (SELF, XN, YN, DIAG):
            for c in (0, 1):
                for g in range(GROUPS):
                    made += dot(h_buf[r, c, g, chip_rows, :], wkv_buf[pl.ds(column(r, c, g), PIECE), :])
        shared = share_new_rows(copies, core, partner, made, kv_send, kv_out, NEW_ROWS)
        seven = pl.ds(0, DEVICES - 1)
        await_all(q_out.at[:, seven], q_sem)
        shared.wait()
        await_all(q_send.at[:, seven], send_sems.at[QUERY])
        await_all(kv_pre, cache_sem)
    await_all(ctx_in.at[pl.ds(0, DEVICES - 1)], send_sems.at[CONTEXT])
    await_all(send_d2d, send_sems.at[CORE])
    await_all(acc.at[:, pl.ds(0, 3)], send_sems.at[SUMS])
    await_all(h_buf.at[pl.ds(0, 3)], send_sems.at[WHOLE])
    await_all(h_buf.at[0, 0], send_sems.at[HALVES])


def combine_call(layer, last, ctx, residual, w_out, more):
    any_spec = pl.BlockSpec(memory_space=pl.ANY)
    vmem_spec = pl.BlockSpec(memory_space=pltpu.VMEM)
    receives = (1 if last else 3) + GROUPS * (4 + 6 + 7)
    scratch = [
        pltpu.VMEM((DEVICES, MY_ROWS, MY_HEADS, HEAD_DIM), BF16),
        pltpu.VMEM((ROWS, MY_COLS), BF16),
        pltpu.VMEM((SLOTS, MY_COLS, PIECE), BF16),
        pltpu.VMEM((GROUPS, 4, ROWS, PIECE), F32),
        pltpu.VMEM((GROUPS, 4, ROWS, PIECE), F32),
        pltpu.VMEM((GROUPS, 4, ROWS, PIECE), F32),
    ] + [pltpu.VMEM((GROUPS, HALF, PIECE), F32)] * 6 + [
        pltpu.VMEM((4, 2, GROUPS, ROWS, PIECE), BF16),
    ]
    if last:
        out_shape = pltpu.VMEM((ROWS, D_MODEL), BF16)
        out_specs = vmem_spec
    else:
        out_shape = (pltpu.VMEM((ROWS, MY_COLS), BF16),) + QUERY_SHAPES
        out_specs = (vmem_spec,) * len(out_shape)
        scratch.insert(2, pltpu.VMEM((ROWS, MY_COLS), BF16))
        scratch += [
            pltpu.VMEM((D_MODEL, HEAD_DIM), BF16),
            pltpu.VMEM((ROWS, MY_COLS), F32),
            pltpu.VMEM((TILES, DEVICES, MY_ROWS, TILE), BF16),
            pltpu.VMEM((2, MY_ROWS, HEAD_DIM), BF16),
        ]
    scratch += [
        pltpu.SemaphoreType.DMA((SLOTS + (0 if last else 3),)),
        pltpu.SemaphoreType.DMA((5 if last else 7,)),
        pltpu.SemaphoreType.DMA((receives,)),
    ]
    return pl.pallas_call(
        functools.partial(combine_kernel, layer, last),
        name="combine_last" if last else "combine",
        out_shape=out_shape,
        in_specs=[vmem_spec, vmem_spec if last else any_spec] + [any_spec] * (1 + len(more)),
        out_specs=out_specs,
        scratch_shapes=scratch,
        compiler_params=pltpu.CompilerParams(
            collective_id=2 if last else 1, has_side_effects=True, vmem_limit_bytes=40 * MIB
        ),
    )(*in_vmem(ctx), *(in_vmem if last else in_hbm)(residual), *in_hbm(w_out, *more))


def solution(mesh):
    cache_spec = P(None, ("replica", "model"), None, None)

    def device_step(x, cache_len, w_query, w_key, w_value, w_out, k_cache, v_cache):
        caches = (k_cache, v_cache)
        q, kv_new, kv_pre = query_call(x, w_query, w_key, w_value, *caches)
        ctx, k_all, v_all = attend_call(0, LATE_ROWS, cache_len, q, kv_new, kv_pre, *caches, ())
        own, q, kv_new, kv_pre = combine_call(0, False, ctx, x, w_out, (w_query, w_key, w_value, *caches))
        ctx, k_all, v_all = attend_call(1, 0, cache_len, q, kv_new, kv_pre, *caches, (k_all, v_all))
        out = combine_call(1, True, ctx, own, w_out, ())
        return out, k_all, v_all

    return jax.shard_map(
        device_step,
        mesh=mesh,
        in_specs=(P("replica", None), P("replica"), P(None, None, "model"), P(), P(), P(None, "model", None), cache_spec, cache_spec),
        out_specs=(P("replica", None), cache_spec, cache_spec),
        check_vma=False,
    )
```

```python
import functools

import jax
import jax.numpy as jnp
from jax import lax
from jax.experimental import pallas as pl
from jax.experimental.pallas import tpu as pltpu
from jax.sharding import PartitionSpec as P

MESH = pl.DeviceIdType.MESH
BF16 = jnp.bfloat16
F32 = jnp.float32
MIB = 1024 * 1024

DEVICES = 8
ROWS = 128
MY_ROWS = 16
D_MODEL = 8192
HEAD_DIM = 128
MY_HEADS = 8
NUM_HEADS = 64
MY_COLS = 1024
SEQ = 2048
QUERY_TILE = 512
QUERY_DEPTH = 2048

GROUPS = 2
GROUP_SEQS = MY_ROWS // GROUPS
GROUP_ROWS = ROWS // GROUPS
HALF = GROUP_ROWS // 2
LATE_ROWS = 4
TOGETHER = 8
SPANS = (256, 512, 1024, 2048)


def dot(a, b):
    return jnp.dot(a, b, preferred_element_type=F32)


def places():
    me = lax.axis_index("model")
    core = lax.rem(me, 2)
    x = lax.rem(lax.div(me, 2), 2)
    y = lax.div(me, 4)
    flip = 1 - 2 * core
    xn = me + 2 - 4 * x
    yn = me + 4 - 8 * y
    diag = xn + 4 - 8 * y
    return me, flip, xn, yn, diag


def await_all(ref, sem):
    pltpu.make_async_copy(ref, ref, sem).wait()


class Copies:
    def __init__(self, send_sems, recv_sems):
        self.send_sems, self.recv_sems, self.receives = send_sems, recv_sems, 0

    def new_receive(self):
        self.receives += 1
        return self.recv_sems.at[self.receives - 1]

    def start(self, src, dst, device, kind, recv_sem=None):
        copy = pltpu.make_async_remote_copy(
            src_ref=src,
            dst_ref=dst,
            send_sem=self.send_sems.at[kind],
            recv_sem=self.new_receive() if recv_sem is None else recv_sem,
            device_id={"model": device},
            device_id_type=MESH,
        )
        copy.start()
        return copy


def meet_all(me):
    barrier = pltpu.get_barrier_semaphore()
    for k in range(1, DEVICES):
        pl.semaphore_signal(barrier, inc=1, device_id={"model": lax.rem(me + k, DEVICES)}, device_id_type=MESH)
    pl.semaphore_wait(barrier, DEVICES - 1)


def others():
    me, flip, xn, yn, diag = places()
    return [diag, diag + flip, xn, yn, xn + flip, yn + flip, me + flip]


def load_cache(layer, rows, k_hbm, v_hbm, kv, sem):
    for i, hbm in enumerate((k_hbm, v_hbm)):
        pltpu.make_async_copy(hbm.at[layer, rows], kv.at[i, rows], sem).start()


def load_kv_weights(layer, core, wk_hbm, wv_hbm, wkv_buf, sem):
    for i, hbm in enumerate((wk_hbm, wv_hbm)):
        @pl.when(core == i)
        def _():
            pltpu.make_async_copy(hbm.at[layer], wkv_buf, sem).start()


def share_new_rows(copies, core, partner, made, kv_send, kv_out, kind):
    kv_send[...] = made.reshape(2, MY_ROWS, HEAD_DIM).astype(BF16)
    copy = copies.start(kv_send.at[1 - core], kv_out.at[core], partner, kind)
    kv_out[core] = kv_send[core]
    return copy


def in_vmem(*arrays):
    return [pltpu.with_memory_space_constraint(a, pltpu.VMEM) for a in arrays]


def in_hbm(*arrays):
    return [pltpu.with_memory_space_constraint(a, pltpu.HBM) for a in arrays]


QUERY_SHAPES = (
    pltpu.VMEM((DEVICES, MY_ROWS, MY_COLS), BF16),
    pltpu.VMEM((2, MY_ROWS, HEAD_DIM), BF16),
    pltpu.VMEM((2, MY_ROWS, SEQ, HEAD_DIM), BF16),
)


def query_kernel(x_hbm, wq_hbm, wk_hbm, wv_hbm, k_hbm, v_hbm, q_out, kv_out, kv_pre,
                 x_buf, wq_buf, wkv_buf, q_send, kv_send, load_sems, send_sems, recv_sems):
    me, flip, _, _, _ = places()
    core = lax.rem(me, 2)
    columns = [pl.ds(j * QUERY_TILE, QUERY_TILE) for j in range(MY_COLS // QUERY_TILE)]
    depths = [pl.ds(k * QUERY_DEPTH, QUERY_DEPTH) for k in range(D_MODEL // QUERY_DEPTH)]
    x_sem, wkv_sem, cache_sem = [load_sems.at[i] for i in range(3)]
    x_load = pltpu.make_async_copy(x_hbm, x_buf, x_sem)
    x_load.start()
    wq_loads = []
    for cols in columns:
        for depth in depths:
            sem = load_sems.at[3 + len(wq_loads)]
            wq_loads.append(pltpu.make_async_copy(wq_hbm.at[0, depth, cols], wq_buf.at[depth, cols], sem))
            wq_loads[-1].start()
    load_kv_weights(0, core, wk_hbm, wv_hbm, wkv_buf, wkv_sem)
    early = pl.ds(0, MY_ROWS - LATE_ROWS)
    load_cache(0, early, k_hbm, v_hbm, kv_pre, cache_sem)
    meet_all(me)
    copies = Copies(send_sems, recv_sems)
    q_sem = copies.new_receive()
    x_load.wait()
    for j, cols in enumerate(columns):
        q = None
        for k, depth in enumerate(depths):
            wq_loads[j * len(depths) + k].wait()
            part = dot(x_buf[:, depth], wq_buf[depth, cols])
            q = part if q is None else q + part
        q_send[:, :, cols] = q.astype(BF16).reshape(DEVICES, MY_ROWS, QUERY_TILE)
        for to in others():
            copies.start(q_send.at[to, :, cols], q_out.at[me, :, cols], to, 0, q_sem)
    q_out[me] = q_send[me]
    chip_rows = pl.ds(pl.multiple_of((me - core) * MY_ROWS, 2 * MY_ROWS), 2 * MY_ROWS)
    await_all(wkv_buf, wkv_sem)
    shared = share_new_rows(copies, core, me + flip, dot(x_buf[chip_rows, :], wkv_buf[...]), kv_send, kv_out, 1)
    seven = pl.ds(0, DEVICES - 1)
    await_all(q_out.at[seven], q_sem)
    shared.wait()
    await_all(q_send.at[seven], send_sems.at[0])
    await_all(kv_pre.at[:, early], cache_sem)


def query_call(x, w_query, w_key, w_value, k_cache, v_cache):
    any_spec = pl.BlockSpec(memory_space=pl.ANY)
    vmem_spec = pl.BlockSpec(memory_space=pltpu.VMEM)
    return pl.pallas_call(
        query_kernel,
        name="query",
        out_shape=QUERY_SHAPES,
        in_specs=[any_spec] * 6,
        out_specs=(vmem_spec,) * len(QUERY_SHAPES),
        scratch_shapes=[
            pltpu.VMEM((ROWS, D_MODEL), BF16),
            pltpu.VMEM((D_MODEL, MY_COLS), BF16),
            pltpu.VMEM((D_MODEL, HEAD_DIM), BF16),
            pltpu.VMEM((DEVICES, MY_ROWS, MY_COLS), BF16),
            pltpu.VMEM((2, MY_ROWS, HEAD_DIM), BF16),
            pltpu.SemaphoreType.DMA((3 + (MY_COLS // QUERY_TILE) * (D_MODEL // QUERY_DEPTH),)),
            pltpu.SemaphoreType.DMA((2,)),
            pltpu.SemaphoreType.DMA((2,)),
        ],
        compiler_params=pltpu.CompilerParams(
            collective_id=0, has_side_effects=True, vmem_limit_bytes=26 * MIB
        ),
    )(*in_hbm(x, w_query, w_key, w_value, k_cache, v_cache))


def attend_kernel(layer, late_rows, len_hbm, q_ref, new_ref, *refs):
    k_hbm, v_hbm = refs[1:3]
    k_out, v_out, ctx_ref, kv_buf, len_ref, q_buf, new_buf, sems = refs[-8:]
    k_buf, v_buf = kv_buf.at[0], kv_buf.at[1]
    me = lax.axis_index("model")
    out_sems, len_sem, late_sem = (sems.at[0], sems.at[1]), sems.at[2], sems.at[3]
    len_load = pltpu.make_async_copy(len_hbm, len_ref, len_sem)
    len_load.start()
    late = pl.ds(MY_ROWS - late_rows, late_rows)
    if late_rows:
        load_cache(layer, late, k_hbm, v_hbm, kv_buf, late_sem)

    def save(which, b):
        hbm, buf = ((k_out, k_buf), (v_out, v_buf))[which]
        return pltpu.make_async_copy(buf.at[b], hbm.at[layer, b], out_sems[which])

    new_buf[...] = new_ref[...].astype(F32)
    for src in range(DEVICES):
        block = q_ref[src].astype(F32)
        for h in range(MY_HEADS):
            q_buf[:, src * MY_HEADS + h, :] = block[:, h * HEAD_DIM:(h + 1) * HEAD_DIM]

    def write_tokens(first, last):
        @pl.loop(first, last)
        def _(b):
            pos = len_ref[me * MY_ROWS + b]
            base = pl.multiple_of((pos // 16) * 16, 16)
            here = lax.broadcasted_iota(jnp.int32, (16, HEAD_DIM), 0) == pos - base
            for i, buf in enumerate((k_buf, v_buf)):
                tile = buf[b, pl.ds(base, 16), :].astype(F32)
                row = jnp.broadcast_to(new_buf[i, pl.ds(b, 1), :], (16, HEAD_DIM))
                buf[b, pl.ds(base, 16), :] = jnp.where(here, row, tile).astype(BF16)

            @pl.when(b > first)
            def _():
                save(0, b - 1).start()
                save(1, b - 1).start()

        save(0, last - 1).start()
        save(1, last - 1).start()

    len_load.wait()
    write_tokens(0, MY_ROWS - late_rows)

    scale = HEAD_DIM ** -0.5

    def attend(rows, n):
        t = lax.broadcasted_iota(jnp.int32, (NUM_HEADS, n), 1)
        s = [lax.dot_general(q_buf[b].astype(BF16), k_buf[b, 0:n, :], (((1,), (1,)), ((), ())),
                             preferred_element_type=F32) for b in rows]
        s = [jnp.where(t <= len_ref[me * MY_ROWS + b], v * scale, -jnp.inf) for v, b in zip(s, rows)]
        peak = [jnp.max(v, axis=1, keepdims=True) for v in s]
        e = [jnp.exp(v - u) for v, u in zip(s, peak)]
        share = [1.0 / jnp.sum(v, axis=1, keepdims=True) for v in e]
        p = [(v * u).astype(BF16) for v, u in zip(e, share)]
        c = [dot(v, v_buf[b, 0:n, :]) for v, b in zip(p, rows)]
        for v, b in zip(c, rows):
            ctx_ref[:, b] = v.reshape(DEVICES, MY_HEADS, HEAD_DIM).astype(BF16)

    attend(list(range(TOGETHER)), SPANS[0])
    if late_rows:
        await_all(kv_buf.at[:, late], late_sem)
        write_tokens(MY_ROWS - late_rows, MY_ROWS)
    attend(list(range(TOGETHER, MY_ROWS)), SPANS[0])

    @pl.loop(0, MY_ROWS)
    def _(b):
        pos = len_ref[me * MY_ROWS + b]
        for low, n in zip(SPANS, SPANS[1:]):
            @pl.when(jnp.logical_and(pos >= low, pos < n))
            def _(n=n):
                attend([b], n)

    for which, hbm in enumerate((k_out, v_out)):
        await_all(hbm.at[layer], out_sems[which])


def attend_call(layer, late_rows, cache_len, q, kv_new, kv_pre, k_cache, v_cache, prev):
    any_spec = pl.BlockSpec(memory_space=pl.ANY)
    vmem_spec = pl.BlockSpec(memory_space=pltpu.VMEM)
    k_all, v_all, ctx, _ = pl.pallas_call(
        functools.partial(attend_kernel, layer, late_rows),
        name="attend",
        out_shape=(
            jax.ShapeDtypeStruct(k_cache.shape, BF16),
            jax.ShapeDtypeStruct(v_cache.shape, BF16),
            pltpu.VMEM((DEVICES, MY_ROWS, MY_HEADS, HEAD_DIM), BF16),
            pltpu.VMEM(kv_pre.shape, BF16),
        ),
        in_specs=[any_spec] + [vmem_spec] * 3 + [any_spec] * (2 + len(prev)),
        out_specs=(any_spec, any_spec, vmem_spec, vmem_spec),
        scratch_shapes=[
            pltpu.SMEM((ROWS,), jnp.int32),
            pltpu.VMEM((MY_ROWS, NUM_HEADS, HEAD_DIM), F32),
            pltpu.VMEM((2, MY_ROWS, HEAD_DIM), F32),
            pltpu.SemaphoreType.DMA((4,)),
        ],
        input_output_aliases={3: 3} | ({6: 0, 7: 1} if prev else {}),
        compiler_params=pltpu.CompilerParams(vmem_limit_bytes=16 * MIB),
    )(*in_hbm(cache_len), *in_vmem(q, kv_new, kv_pre), *in_hbm(k_cache, v_cache), *prev)
    return ctx, k_all, v_all


SELF, XN, YN, DIAG = range(4)
PASS_ON_AFTER = XN
LEFT, RIGHT = pl.ds(0, MY_COLS // 2), pl.ds(MY_COLS // 2, MY_COLS // 2)
CONTEXT, CORE, SUMS, WHOLE, HALVES, QUERY, NEW_ROWS = range(7)


def combine_kernel(layer, last, *refs):
    if last:
        (ctx_in, res_buf, wo_hbm, out_ref,
         ctx_buf, lhs, w_buf, send_d2d, recv_d2d, acc, rx_diag, ry_diag, top_in, bottom_in, h_buf,
         load_sems, send_sems, recv_sems) = refs
    else:
        (ctx_in, res_hbm, wo_hbm, wq_hbm, wk_hbm, wv_hbm, k_hbm, v_hbm, own_out, q_out, kv_out, kv_pre,
         ctx_buf, lhs, res_buf, w_buf, send_d2d, recv_d2d, acc, rx_diag, ry_diag, top_in, bottom_in, h_buf,
         wkv_buf, q_acc, q_send, kv_send,
         load_sems, send_sems, recv_sems) = refs
    me, flip, xn, yn, diag = places()
    partner, core = me + flip, lax.rem(me, 2)
    chip_mate = {SELF: me, XN: xn, YN: yn, DIAG: diag}
    columns = lambda r, c: pl.ds(pl.multiple_of((chip_mate[r] + c * flip) * MY_COLS, MY_COLS), MY_COLS)
    copies = Copies(send_sems, recv_sems)
    wo_order = [(r, c) for r in (DIAG, XN, YN, SELF) for c in (1, 0)]
    wq_order = [(r, c) for r in (SELF, XN, YN, DIAG) for c in (0, 1)]
    top, bottom = pl.ds(0, HALF), pl.ds(HALF, HALF)
    seven = pl.ds(0, DEVICES - 1)
    seqs = [pl.ds(g * GROUP_SEQS, GROUP_SEQS) for g in range(GROUPS)]

    for slot, (r, c) in enumerate(wo_order):
        pltpu.make_async_copy(wo_hbm.at[layer, :, columns(r, c)], w_buf.at[slot], load_sems.at[slot // 2]).start()
    if not last:
        wq_sem, res_sem, wkv_sem, cache_sem = [load_sems.at[4 + i] for i in range(4)]
        res_load = pltpu.make_async_copy(res_hbm.at[:, :, :, columns(SELF, 0)], res_buf, res_sem)
        res_load.start()
        load_kv_weights(layer + 1, core, wk_hbm, wv_hbm, wkv_buf, wkv_sem)

    meet_all(me)

    ctx_sems = [copies.new_receive() for _ in range(GROUPS)]

    def send_context(g):
        for to in others():
            copies.start(ctx_in.at[to, seqs[g]], ctx_buf.at[g, me], to, CONTEXT, ctx_sems[g])
        ctx_buf[g, me] = ctx_in[me, seqs[g]]

    send_context(0)

    d2d, first, in_sems = {}, {}, {}

    def receive_context(g):
        await_all(ctx_buf.at[g, seven], ctx_sems[g])
        if g + 1 < GROUPS:
            send_context(g + 1)
        rows = ctx_buf[g].astype(F32).reshape(GROUP_ROWS, MY_HEADS, HEAD_DIM)
        lhs[g] = rows.reshape(GROUP_ROWS, MY_COLS).astype(BF16)

    def settle(g, r):
        await_all(recv_d2d.at[g, r], d2d[g, r])
        acc[g, r] += recv_d2d[g, r]
        if r == DIAG:
            first[g, 0] = copies.start(acc.at[g, r, top], rx_diag.at[g], xn, SUMS)
            first[g, 1] = copies.start(acc.at[g, r, bottom], ry_diag.at[g], yn, SUMS)
        if r == YN:
            in_sems[g] = copies.new_receive(), copies.new_receive()
            copies.start(acc.at[g, XN, top], top_in.at[g, 0], xn, SUMS, in_sems[g][0])
            copies.start(acc.at[g, YN, bottom], bottom_in.at[g, 0], yn, SUMS, in_sems[g][1])

    def pass_on(g):
        first[g, 0].wait_recv()
        acc[g, YN, top] += rx_diag[g]
        copies.start(acc.at[g, YN, top], top_in.at[g, 1], yn, SUMS, in_sems[g][0])
        first[g, 1].wait_recv()
        acc[g, XN, bottom] += ry_diag[g]
        copies.start(acc.at[g, XN, bottom], bottom_in.at[g, 1], xn, SUMS, in_sems[g][1])

    pending = None
    for g in range(GROUPS):
        receive_context(g)
        for slot, (r, c) in enumerate(wo_order):
            if g == 0 and c == 1:
                await_all(w_buf.at[pl.ds(slot, 2)], load_sems.at[slot // 2])
            if c == 1:
                d2d[g, r] = copies.new_receive()
                for cols in (LEFT, RIGHT) if r == DIAG else (pl.ds(0, MY_COLS),):
                    send_d2d[g, r, :, cols] = dot(lhs[g], w_buf[slot, :, cols])
                    copies.start(send_d2d.at[g, r, :, cols], recv_d2d.at[g, r, :, cols], partner, CORE, d2d[g, r])
            else:
                acc[g, r] = dot(lhs[g], w_buf[slot])
            if not last and g == GROUPS - 1:
                pltpu.make_async_copy(wq_hbm.at[layer + 1, columns(*wq_order[slot]), :], w_buf.at[slot], wq_sem).start()
            if c == 1 and pending is not None:
                settle(*pending)
                if g > 0 and pending == (g, PASS_ON_AFTER):
                    pass_on(g - 1)
            pending = (g, r)
    settle(*pending)
    if not last:
        load_cache(layer + 1, pl.ds(0, MY_ROWS), k_hbm, v_hbm, kv_pre, cache_sem)
    pass_on(GROUPS - 1)

    gather, diag_sems = {}, {}
    if not last:
        res_load.wait()

    def finish_group(g):
        if last:
            residual = res_buf[g].astype(F32)
        else:
            residual = res_buf[:, g].astype(F32).reshape(GROUP_ROWS, MY_COLS)
        await_all(top_in.at[g], in_sems[g][0])
        total = acc[g, SELF, top] + top_in[g, 0] + top_in[g, 1]
        h_buf[SELF, 0, g, top] = (residual[:HALF] + total).astype(BF16)
        await_all(bottom_in.at[g], in_sems[g][1])
        total = acc[g, SELF, bottom] + bottom_in[g, 0] + bottom_in[g, 1]
        h_buf[SELF, 0, g, bottom] = (residual[HALF:] + total).astype(BF16)
        mine = h_buf.at[SELF, 0, g]
        for r, device, halves in ((XN, xn, (top, bottom)), (YN, yn, (bottom, top))):
            gather[r, 0, g] = [copies.start(h_buf.at[SELF, 0, g, half], h_buf.at[r, 0, g, half], device, HALVES)
                               for half in halves]
        gather[SELF, 1, g] = copies.start(mine, h_buf.at[SELF, 1, g], partner, WHOLE)
        if not last:
            own_out[g] = h_buf[SELF, 0, g]

    def arrive(r, c, g):
        gather[r, c, g].wait_recv()

    if last:
        def use(g, *pieces):
            for r, c in pieces:
                rows = h_buf[r, c, g].astype(F32).reshape(DEVICES, GROUP_SEQS, MY_COLS).astype(BF16)
                out_ref[:, g, :, columns(r, c)] = rows
    else:
        wq_slot = {piece: slot for slot, piece in enumerate(wq_order)}

        def use(g, *pieces):
            q_acc[g] += sum(dot(h_buf[r, c, g], w_buf[wq_slot[r, c]]) for r, c in pieces)

    def relay_first(g):
        diag_sems[g] = copies.new_receive()
        for r, device, half in ((XN, yn, top), (YN, xn, bottom)):
            gather[r, 0, g][0].wait_recv()
            copies.start(h_buf.at[r, 0, g, half], h_buf.at[DIAG, 0, g, half], device, HALVES, diag_sems[g])

    def relay_second(g):
        for r in (XN, YN):
            gather[r, 0, g][1].wait_recv()
            gather[r, 1, g] = copies.start(h_buf.at[r, 0, g], h_buf.at[r, 1, g], partner, WHOLE)

    def relay_diag(g):
        await_all(h_buf.at[DIAG, 0, g], diag_sems[g])
        gather[DIAG, 1, g] = copies.start(h_buf.at[DIAG, 0, g], h_buf.at[DIAG, 1, g], partner, WHOLE)

    def send_query(g):
        q_send[g] = q_acc[g].astype(BF16).reshape(DEVICES, GROUP_SEQS, MY_COLS)
        for to in others():
            copies.start(q_send.at[g, to], q_out.at[me, seqs[g], :], to, QUERY, q_sem)

    if not last:
        q_sem = copies.new_receive()
        await_all(w_buf, wq_sem)
        q_acc[...] = jnp.zeros_like(q_acc)
    finish_group(0)
    finish_group(1)
    relay_first(0)
    for g in range(GROUPS):
        arrive(SELF, 1, g)
        use(g, (SELF, 0), (SELF, 1))
    relay_second(0)
    use(0, (XN, 0), (YN, 0))
    relay_first(1)
    arrive(XN, 1, 0)
    arrive(YN, 1, 0)
    use(0, (XN, 1), (YN, 1))
    relay_second(1)
    use(1, (XN, 0), (YN, 0))
    relay_diag(0)
    use(0, (DIAG, 0))
    arrive(XN, 1, 1)
    arrive(YN, 1, 1)
    use(1, (XN, 1), (YN, 1))
    relay_diag(1)
    arrive(DIAG, 1, 0)
    use(0, (DIAG, 1))
    if not last:
        send_query(0)
    use(1, (DIAG, 0))
    arrive(DIAG, 1, 1)
    use(1, (DIAG, 1))

    if not last:
        send_query(GROUPS - 1)
        for g in range(GROUPS):
            q_out[me, seqs[g], :] = q_send[g, me]
        await_all(wkv_buf, wkv_sem)
        chip_rows = pl.ds(pl.multiple_of((me - core) * GROUP_SEQS, 2 * GROUP_SEQS), 2 * GROUP_SEQS)
        made = jnp.zeros((GROUPS * 2 * GROUP_SEQS, HEAD_DIM), F32)
        for r, c in wq_order:
            rows = jnp.concatenate([h_buf[r, c, g, chip_rows, :] for g in range(GROUPS)], axis=0)
            made += dot(rows, wkv_buf[columns(r, c), :])
        made = made.reshape(GROUPS, 2, GROUP_SEQS, HEAD_DIM)
        made = jnp.concatenate([made[g, k] for k in range(2) for g in range(GROUPS)], axis=0)
        shared = share_new_rows(copies, core, partner, made, kv_send, kv_out, NEW_ROWS)
        await_all(q_out.at[seven], q_sem)
        shared.wait()
        await_all(q_send.at[:, seven], send_sems.at[QUERY])
        await_all(kv_pre, cache_sem)
    await_all(ctx_in.at[seven], send_sems.at[CONTEXT])
    await_all(send_d2d, send_sems.at[CORE])
    await_all(acc.at[:, pl.ds(0, 3)], send_sems.at[SUMS])
    await_all(h_buf.at[pl.ds(0, 2)], send_sems.at[WHOLE])
    await_all(h_buf.at[pl.ds(0, 3), 0], send_sems.at[HALVES])


def combine_call(layer, last, ctx, residual, w_out, more):
    any_spec = pl.BlockSpec(memory_space=pl.ANY)
    vmem_spec = pl.BlockSpec(memory_space=pltpu.VMEM)
    receives = (2 if last else 4) + GROUPS * (4 + 4 + 9)
    scratch = [
        pltpu.VMEM((GROUPS, DEVICES, GROUP_SEQS, MY_HEADS, HEAD_DIM), BF16),
        pltpu.VMEM((GROUPS, GROUP_ROWS, MY_COLS), BF16),
        pltpu.VMEM((DEVICES, MY_COLS, MY_COLS), BF16),
        pltpu.VMEM((GROUPS, 4, GROUP_ROWS, MY_COLS), F32),
        pltpu.VMEM((GROUPS, 4, GROUP_ROWS, MY_COLS), F32),
        pltpu.VMEM((GROUPS, 4, GROUP_ROWS, MY_COLS), F32),
        pltpu.VMEM((GROUPS, HALF, MY_COLS), F32),
        pltpu.VMEM((GROUPS, HALF, MY_COLS), F32),
        pltpu.VMEM((GROUPS, 2, HALF, MY_COLS), F32),
        pltpu.VMEM((GROUPS, 2, HALF, MY_COLS), F32),
        pltpu.VMEM((4, 2, GROUPS, GROUP_ROWS, MY_COLS), BF16),
    ]
    if last:
        out_shape = pltpu.VMEM((DEVICES, GROUPS, GROUP_SEQS, D_MODEL), BF16)
        out_specs = vmem_spec
    else:
        out_shape = (pltpu.VMEM((GROUPS, GROUP_ROWS, MY_COLS), BF16),) + QUERY_SHAPES
        out_specs = (vmem_spec,) * len(out_shape)
        scratch.insert(2, pltpu.VMEM((DEVICES, GROUPS, GROUP_SEQS, MY_COLS), BF16))
        scratch += [
            pltpu.VMEM((D_MODEL, HEAD_DIM), BF16),
            pltpu.VMEM((GROUPS, GROUP_ROWS, MY_COLS), F32),
            pltpu.VMEM((GROUPS, DEVICES, GROUP_SEQS, MY_COLS), BF16),
            pltpu.VMEM((2, MY_ROWS, HEAD_DIM), BF16),
        ]
    scratch += [
        pltpu.SemaphoreType.DMA((4 if last else 8,)),
        pltpu.SemaphoreType.DMA((5 if last else 7,)),
        pltpu.SemaphoreType.DMA((receives,)),
    ]
    return pl.pallas_call(
        functools.partial(combine_kernel, layer, last),
        name="combine_last" if last else "combine",
        out_shape=out_shape,
        in_specs=[vmem_spec, vmem_spec if last else any_spec] + [any_spec] * (1 + len(more)),
        out_specs=out_specs,
        scratch_shapes=scratch,
        compiler_params=pltpu.CompilerParams(
            collective_id=2 if last else 1, has_side_effects=True, vmem_limit_bytes=40 * MIB
        ),
    )(*in_vmem(ctx), *(in_vmem if last else in_hbm)(residual), *in_hbm(w_out, *more))


def solution(mesh):
    cache_spec = P(None, ("replica", "model"), None, None)

    def device_step(x, cache_len, w_query, w_key, w_value, w_out, k_cache, v_cache):
        caches = (k_cache, v_cache)
        q, kv_new, kv_pre = query_call(x, w_query, w_key, w_value, *caches)
        ctx, k_all, v_all = attend_call(0, LATE_ROWS, cache_len, q, kv_new, kv_pre, *caches, ())
        own, q, kv_new, kv_pre = combine_call(0, False, ctx, x.reshape(DEVICES, GROUPS, GROUP_SEQS, D_MODEL), w_out, (w_query, w_key, w_value, *caches))
        ctx, k_all, v_all = attend_call(1, 0, cache_len, q, kv_new, kv_pre, *caches, (k_all, v_all))
        out = combine_call(1, True, ctx, own, w_out, ())
        return out.reshape(x.shape), k_all, v_all

    return jax.shard_map(
        device_step,
        mesh=mesh,
        in_specs=(P("replica", None), P("replica"), P(None, None, "model"), P(), P(), P(None, "model", None), cache_spec, cache_spec),
        out_specs=(P("replica", None), cache_spec, cache_spec),
        check_vma=False,
    )
```

```python
import functools

import jax
import jax.numpy as jnp
from jax import lax
from jax.experimental import pallas as pl
from jax.experimental.pallas import tpu as pltpu
from jax.sharding import PartitionSpec as P

MESH = pl.DeviceIdType.MESH
BF16 = jnp.bfloat16
F32 = jnp.float32
MIB = 1024 * 1024

DEVICES = 8
ROWS = 128
MY_ROWS = 16
D_MODEL = 8192
HEAD_DIM = 128
MY_HEADS = 8
NUM_HEADS = 64
MY_COLS = 1024
SEQ = 2048
QUERY_TILE = 512
QUERY_DEPTH = 2048

GROUPS = 2
GROUP_SEQS = MY_ROWS // GROUPS
GROUP_ROWS = ROWS // GROUPS
HALF = GROUP_ROWS // 2
LATE_ROWS = 4
TOGETHER = 6
SPANS = (256, 512, 1024, 2048)


def dot(a, b):
    return jnp.dot(a, b, preferred_element_type=F32)


def places():
    me = lax.axis_index("model")
    core = lax.rem(me, 2)
    x = lax.rem(lax.div(me, 2), 2)
    y = lax.div(me, 4)
    flip = 1 - 2 * core
    xn = me + 2 - 4 * x
    yn = me + 4 - 8 * y
    diag = xn + 4 - 8 * y
    return me, flip, xn, yn, diag


def await_all(ref, sem):
    pltpu.make_async_copy(ref, ref, sem).wait()


class Copies:
    def __init__(self, send_sems, recv_sems):
        self.send_sems, self.recv_sems, self.receives = send_sems, recv_sems, 0

    def new_receive(self):
        self.receives += 1
        return self.recv_sems.at[self.receives - 1]

    def start(self, src, dst, device, kind, recv_sem=None):
        copy = pltpu.make_async_remote_copy(
            src_ref=src,
            dst_ref=dst,
            send_sem=self.send_sems.at[kind],
            recv_sem=self.new_receive() if recv_sem is None else recv_sem,
            device_id={"model": device},
            device_id_type=MESH,
        )
        copy.start()
        return copy


def meet_all(me):
    barrier = pltpu.get_barrier_semaphore()
    for k in range(1, DEVICES):
        pl.semaphore_signal(barrier, inc=1, device_id={"model": lax.rem(me + k, DEVICES)}, device_id_type=MESH)
    pl.semaphore_wait(barrier, DEVICES - 1)


def others():
    me, flip, xn, yn, diag = places()
    return [diag, diag + flip, xn, yn, xn + flip, yn + flip, me + flip]


def load_cache(layer, rows, k_hbm, v_hbm, kv, sem):
    for i, hbm in enumerate((k_hbm, v_hbm)):
        pltpu.make_async_copy(hbm.at[layer, rows], kv.at[i, rows], sem).start()


def load_kv_weights(layer, core, wk_hbm, wv_hbm, wkv_buf, sem):
    for i, hbm in enumerate((wk_hbm, wv_hbm)):
        @pl.when(core == i)
        def _():
            pltpu.make_async_copy(hbm.at[layer], wkv_buf, sem).start()


def share_new_rows(copies, core, partner, made, kv_send, kv_out, kind):
    kv_send[...] = made.reshape(2, MY_ROWS, HEAD_DIM).astype(BF16)
    copy = copies.start(kv_send.at[1 - core], kv_out.at[core], partner, kind)
    kv_out[core] = kv_send[core]
    return copy


def in_vmem(*arrays):
    return [pltpu.with_memory_space_constraint(a, pltpu.VMEM) for a in arrays]


def in_hbm(*arrays):
    return [pltpu.with_memory_space_constraint(a, pltpu.HBM) for a in arrays]


QUERY_SHAPES = (
    pltpu.VMEM((DEVICES, MY_ROWS, MY_COLS), BF16),
    pltpu.VMEM((2, MY_ROWS, HEAD_DIM), BF16),
    pltpu.VMEM((2, MY_ROWS, SEQ, HEAD_DIM), BF16),
)


def query_kernel(x_hbm, wq_hbm, wk_hbm, wv_hbm, k_hbm, v_hbm, q_out, kv_out, kv_pre,
                 x_buf, wq_buf, wkv_buf, q_send, kv_send, load_sems, send_sems, recv_sems):
    me, flip, _, _, _ = places()
    core = lax.rem(me, 2)
    columns = [pl.ds(j * QUERY_TILE, QUERY_TILE) for j in range(MY_COLS // QUERY_TILE)]
    depths = [pl.ds(k * QUERY_DEPTH, QUERY_DEPTH) for k in range(D_MODEL // QUERY_DEPTH)]
    x_sem, wkv_sem, cache_sem = [load_sems.at[i] for i in range(3)]
    x_load = pltpu.make_async_copy(x_hbm, x_buf, x_sem)
    x_load.start()
    wq_loads = []
    for cols in columns:
        for depth in depths:
            sem = load_sems.at[3 + len(wq_loads)]
            wq_loads.append(pltpu.make_async_copy(wq_hbm.at[0, depth, cols], wq_buf.at[depth, cols], sem))
            wq_loads[-1].start()
    load_kv_weights(0, core, wk_hbm, wv_hbm, wkv_buf, wkv_sem)
    early = pl.ds(0, MY_ROWS - LATE_ROWS)
    load_cache(0, early, k_hbm, v_hbm, kv_pre, cache_sem)
    meet_all(me)
    copies = Copies(send_sems, recv_sems)
    q_sem = copies.new_receive()
    x_load.wait()
    for j, cols in enumerate(columns):
        q = None
        for k, depth in enumerate(depths):
            wq_loads[j * len(depths) + k].wait()
            part = dot(x_buf[:, depth], wq_buf[depth, cols])
            q = part if q is None else q + part
        q_send[:, :, cols] = q.astype(BF16).reshape(DEVICES, MY_ROWS, QUERY_TILE)
        for to in others():
            copies.start(q_send.at[to, :, cols], q_out.at[me, :, cols], to, 0, q_sem)
    q_out[me] = q_send[me]
    chip_rows = pl.ds(pl.multiple_of((me - core) * MY_ROWS, 2 * MY_ROWS), 2 * MY_ROWS)
    await_all(wkv_buf, wkv_sem)
    shared = share_new_rows(copies, core, me + flip, dot(x_buf[chip_rows, :], wkv_buf[...]), kv_send, kv_out, 1)
    seven = pl.ds(0, DEVICES - 1)
    await_all(q_out.at[seven], q_sem)
    shared.wait()
    await_all(q_send.at[seven], send_sems.at[0])
    await_all(kv_pre.at[:, early], cache_sem)


def query_call(x, w_query, w_key, w_value, k_cache, v_cache):
    any_spec = pl.BlockSpec(memory_space=pl.ANY)
    vmem_spec = pl.BlockSpec(memory_space=pltpu.VMEM)
    return pl.pallas_call(
        query_kernel,
        name="query",
        out_shape=QUERY_SHAPES,
        in_specs=[any_spec] * 6,
        out_specs=(vmem_spec,) * len(QUERY_SHAPES),
        scratch_shapes=[
            pltpu.VMEM((ROWS, D_MODEL), BF16),
            pltpu.VMEM((D_MODEL, MY_COLS), BF16),
            pltpu.VMEM((D_MODEL, HEAD_DIM), BF16),
            pltpu.VMEM((DEVICES, MY_ROWS, MY_COLS), BF16),
            pltpu.VMEM((2, MY_ROWS, HEAD_DIM), BF16),
            pltpu.SemaphoreType.DMA((3 + (MY_COLS // QUERY_TILE) * (D_MODEL // QUERY_DEPTH),)),
            pltpu.SemaphoreType.DMA((2,)),
            pltpu.SemaphoreType.DMA((2,)),
        ],
        compiler_params=pltpu.CompilerParams(
            collective_id=0, has_side_effects=True, vmem_limit_bytes=26 * MIB
        ),
    )(*in_hbm(x, w_query, w_key, w_value, k_cache, v_cache))


def attend_kernel(layer, late_rows, len_hbm, q_ref, new_ref, *refs):
    k_hbm, v_hbm = refs[1:3]
    k_out, v_out, ctx_ref, kv_buf, len_ref, long_ref, q_buf, new_buf, sems = refs[-9:]
    k_buf, v_buf = kv_buf.at[0], kv_buf.at[1]
    me = lax.axis_index("model")
    out_sems, len_sem, late_sem = (sems.at[0], sems.at[1]), sems.at[2], sems.at[3]
    len_load = pltpu.make_async_copy(len_hbm, len_ref, len_sem)
    len_load.start()
    late = pl.ds(MY_ROWS - late_rows, late_rows)
    if late_rows:
        load_cache(layer, late, k_hbm, v_hbm, kv_buf, late_sem)

    def save(which, b):
        hbm, buf = ((k_out, k_buf), (v_out, v_buf))[which]
        return pltpu.make_async_copy(buf.at[b], hbm.at[layer, b], out_sems[which])

    new_buf[...] = new_ref[...].astype(F32)
    for src in range(DEVICES):
        block = q_ref[src].astype(F32)
        for h in range(MY_HEADS):
            q_buf[:, src * MY_HEADS + h, :] = block[:, h * HEAD_DIM:(h + 1) * HEAD_DIM]

    def write_tokens(first, last):
        @pl.loop(first, last)
        def _(b):
            pos = len_ref[me * MY_ROWS + b]
            base = pl.multiple_of((pos // 16) * 16, 16)
            here = lax.broadcasted_iota(jnp.int32, (16, HEAD_DIM), 0) == pos - base
            for i, buf in enumerate((k_buf, v_buf)):
                tile = buf[b, pl.ds(base, 16), :].astype(F32)
                row = jnp.broadcast_to(new_buf[i, pl.ds(b, 1), :], (16, HEAD_DIM))
                buf[b, pl.ds(base, 16), :] = jnp.where(here, row, tile).astype(BF16)

            @pl.when(b > first)
            def _():
                save(0, b - 1).start()
                save(1, b - 1).start()

        save(0, last - 1).start()
        save(1, last - 1).start()

    len_load.wait()
    write_tokens(0, MY_ROWS - late_rows)

    scale = HEAD_DIM ** -0.5

    def attend(rows, n):
        t = lax.broadcasted_iota(jnp.int32, (NUM_HEADS, n), 1)
        s = [lax.dot_general(q_buf[b].astype(BF16), k_buf[b, 0:n, :], (((1,), (1,)), ((), ())),
                             preferred_element_type=F32) for b in rows]
        s = [jnp.where(t <= len_ref[me * MY_ROWS + b], v * scale, -jnp.inf) for v, b in zip(s, rows)]
        peak = [jnp.max(v, axis=1, keepdims=True) for v in s]
        e = [jnp.exp(v - u) for v, u in zip(s, peak)]
        share = [1.0 / jnp.sum(v, axis=1, keepdims=True) for v in e]
        p = [(v * u).astype(BF16) for v, u in zip(e, share)]
        c = [dot(v, v_buf[b, 0:n, :]) for v, b in zip(p, rows)]
        for v, b in zip(c, rows):
            ctx_ref[:, b] = v.reshape(DEVICES, MY_HEADS, HEAD_DIM).astype(BF16)

    def attend_all(first, last):
        for at in range(first, last, TOGETHER):
            attend(list(range(at, min(at + TOGETHER, last))), SPANS[0])

        def note_long(b, count):
            is_long = len_ref[me * MY_ROWS + b] >= SPANS[0]

            @pl.when(is_long)
            def _():
                long_ref[count] = b

            return count + is_long.astype(jnp.int32)

        count = lax.fori_loop(first, last, note_long, jnp.int32(0))

        @pl.loop(0, (count + 1) // 2)
        def _(i):
            pair = [long_ref[2 * i], long_ref[jnp.minimum(2 * i + 1, count - 1)]]
            longest = jnp.maximum(*[len_ref[me * MY_ROWS + b] for b in pair])
            for low, n in zip(SPANS, SPANS[1:]):
                @pl.when(jnp.logical_and(longest >= low, longest < n))
                def _(n=n):
                    attend(pair, n)

    attend_all(0, MY_ROWS - late_rows)
    if late_rows:
        await_all(kv_buf.at[:, late], late_sem)
        write_tokens(MY_ROWS - late_rows, MY_ROWS)
        attend_all(MY_ROWS - late_rows, MY_ROWS)

    for which, hbm in enumerate((k_out, v_out)):
        await_all(hbm.at[layer], out_sems[which])


def attend_call(layer, late_rows, cache_len, q, kv_new, kv_pre, k_cache, v_cache, prev):
    any_spec = pl.BlockSpec(memory_space=pl.ANY)
    vmem_spec = pl.BlockSpec(memory_space=pltpu.VMEM)
    k_all, v_all, ctx, _ = pl.pallas_call(
        functools.partial(attend_kernel, layer, late_rows),
        name="attend",
        out_shape=(
            jax.ShapeDtypeStruct(k_cache.shape, BF16),
            jax.ShapeDtypeStruct(v_cache.shape, BF16),
            pltpu.VMEM((DEVICES, MY_ROWS, MY_HEADS, HEAD_DIM), BF16),
            pltpu.VMEM(kv_pre.shape, BF16),
        ),
        in_specs=[vmem_spec] * 4 + [any_spec] * (2 + len(prev)),
        out_specs=(any_spec, any_spec, vmem_spec, vmem_spec),
        scratch_shapes=[
            pltpu.SMEM((ROWS,), jnp.int32),
            pltpu.SMEM((MY_ROWS,), jnp.int32),
            pltpu.VMEM((MY_ROWS, NUM_HEADS, HEAD_DIM), F32),
            pltpu.VMEM((2, MY_ROWS, HEAD_DIM), F32),
            pltpu.SemaphoreType.DMA((4,)),
        ],
        input_output_aliases={3: 3} | ({6: 0, 7: 1} if prev else {}),
        compiler_params=pltpu.CompilerParams(vmem_limit_bytes=16 * MIB),
    )(*in_vmem(cache_len, q, kv_new, kv_pre), *in_hbm(k_cache, v_cache), *prev)
    return ctx, k_all, v_all


SELF, XN, YN, DIAG = range(4)
PASS_ON_AFTER = XN
LEFT, RIGHT = pl.ds(0, MY_COLS // 2), pl.ds(MY_COLS // 2, MY_COLS // 2)
CONTEXT, CORE, SUMS, WHOLE, HALVES, QUERY, NEW_ROWS = range(7)


def combine_kernel(layer, last, *refs):
    if last:
        (ctx_in, res_buf, wo_hbm, out_ref,
         ctx_buf, lhs, w_buf, send_d2d, recv_d2d, acc, rx_diag, ry_diag, top_in, bottom_in, h_buf,
         load_sems, send_sems, recv_sems) = refs
    else:
        (ctx_in, res_hbm, wo_hbm, wq_hbm, wk_hbm, wv_hbm, k_hbm, v_hbm, own_out, q_out, kv_out, kv_pre,
         ctx_buf, lhs, res_buf, w_buf, send_d2d, recv_d2d, acc, rx_diag, ry_diag, top_in, bottom_in, h_buf,
         wkv_buf, q_acc, q_send, kv_send,
         load_sems, send_sems, recv_sems) = refs
    me, flip, xn, yn, diag = places()
    partner, core = me + flip, lax.rem(me, 2)
    chip_mate = {SELF: me, XN: xn, YN: yn, DIAG: diag}
    columns = lambda r, c: pl.ds(pl.multiple_of((chip_mate[r] + c * flip) * MY_COLS, MY_COLS), MY_COLS)
    copies = Copies(send_sems, recv_sems)
    wo_order = [(r, c) for r in (DIAG, XN, YN, SELF) for c in (1, 0)]
    wq_order = [(r, c) for r in (SELF, XN, YN, DIAG) for c in (0, 1)]
    top, bottom = pl.ds(0, HALF), pl.ds(HALF, HALF)
    seven = pl.ds(0, DEVICES - 1)
    seqs = [pl.ds(g * GROUP_SEQS, GROUP_SEQS) for g in range(GROUPS)]

    for slot, (r, c) in enumerate(wo_order):
        pltpu.make_async_copy(wo_hbm.at[layer, :, columns(r, c)], w_buf.at[slot], load_sems.at[slot // 2]).start()
    if not last:
        wq_sem, res_sem, wkv_sem, cache_sem = [load_sems.at[4 + i] for i in range(4)]
        res_load = pltpu.make_async_copy(res_hbm.at[:, :, :, columns(SELF, 0)], res_buf, res_sem)
        res_load.start()
        load_kv_weights(layer + 1, core, wk_hbm, wv_hbm, wkv_buf, wkv_sem)

    meet_all(me)

    ctx_sems = [copies.new_receive() for _ in range(GROUPS)]

    def send_context(g):
        for to in others():
            copies.start(ctx_in.at[to, seqs[g]], ctx_buf.at[g, me], to, CONTEXT, ctx_sems[g])
        ctx_buf[g, me] = ctx_in[me, seqs[g]]

    send_context(0)

    d2d, first, in_sems = {}, {}, {}

    def receive_context(g):
        await_all(ctx_buf.at[g, seven], ctx_sems[g])
        if g + 1 < GROUPS:
            send_context(g + 1)
        rows = ctx_buf[g].astype(F32).reshape(GROUP_ROWS, MY_HEADS, HEAD_DIM)
        lhs[g] = rows.reshape(GROUP_ROWS, MY_COLS).astype(BF16)

    def settle(g, r):
        await_all(recv_d2d.at[g, r], d2d[g, r])
        acc[g, r] += recv_d2d[g, r]
        if r == DIAG:
            first[g, 0] = copies.start(acc.at[g, r, top], rx_diag.at[g], xn, SUMS)
            first[g, 1] = copies.start(acc.at[g, r, bottom], ry_diag.at[g], yn, SUMS)
        if r == YN:
            in_sems[g] = copies.new_receive(), copies.new_receive()
            copies.start(acc.at[g, XN, top], top_in.at[g, 0], xn, SUMS, in_sems[g][0])
            copies.start(acc.at[g, YN, bottom], bottom_in.at[g, 0], yn, SUMS, in_sems[g][1])

    def pass_on(g):
        first[g, 0].wait_recv()
        acc[g, YN, top] += rx_diag[g]
        copies.start(acc.at[g, YN, top], top_in.at[g, 1], yn, SUMS, in_sems[g][0])
        first[g, 1].wait_recv()
        acc[g, XN, bottom] += ry_diag[g]
        copies.start(acc.at[g, XN, bottom], bottom_in.at[g, 1], xn, SUMS, in_sems[g][1])

    pending = None
    for g in range(GROUPS):
        receive_context(g)
        for slot, (r, c) in enumerate(wo_order):
            if g == 0 and c == 1:
                await_all(w_buf.at[pl.ds(slot, 2)], load_sems.at[slot // 2])
            if c == 1:
                d2d[g, r] = copies.new_receive()
                for cols in (LEFT, RIGHT) if r == DIAG else (pl.ds(0, MY_COLS),):
                    send_d2d[g, r, :, cols] = dot(lhs[g], w_buf[slot, :, cols])
                    copies.start(send_d2d.at[g, r, :, cols], recv_d2d.at[g, r, :, cols], partner, CORE, d2d[g, r])
            else:
                acc[g, r] = dot(lhs[g], w_buf[slot])
            if not last and g == GROUPS - 1:
                pltpu.make_async_copy(wq_hbm.at[layer + 1, columns(*wq_order[slot]), :], w_buf.at[slot], wq_sem).start()
            if c == 1 and pending is not None:
                settle(*pending)
                if g > 0 and pending == (g, PASS_ON_AFTER):
                    pass_on(g - 1)
            pending = (g, r)
    settle(*pending)
    if not last:
        load_cache(layer + 1, pl.ds(0, MY_ROWS), k_hbm, v_hbm, kv_pre, cache_sem)
    pass_on(GROUPS - 1)

    gather, diag_sems = {}, {}
    if not last:
        res_load.wait()

    def finish_group(g):
        if last:
            residual = res_buf[g].astype(F32)
        else:
            residual = res_buf[:, g].astype(F32).reshape(GROUP_ROWS, MY_COLS)
        await_all(top_in.at[g], in_sems[g][0])
        total = acc[g, SELF, top] + top_in[g, 0] + top_in[g, 1]
        h_buf[SELF, 0, g, top] = (residual[:HALF] + total).astype(BF16)
        await_all(bottom_in.at[g], in_sems[g][1])
        total = acc[g, SELF, bottom] + bottom_in[g, 0] + bottom_in[g, 1]
        h_buf[SELF, 0, g, bottom] = (residual[HALF:] + total).astype(BF16)
        mine = h_buf.at[SELF, 0, g]
        for r, device, halves in ((XN, xn, (top, bottom)), (YN, yn, (bottom, top))):
            gather[r, 0, g] = [copies.start(h_buf.at[SELF, 0, g, half], h_buf.at[r, 0, g, half], device, HALVES)
                               for half in halves]
        gather[SELF, 1, g] = copies.start(mine, h_buf.at[SELF, 1, g], partner, WHOLE)
        if not last:
            own_out[g] = h_buf[SELF, 0, g]

    def arrive(r, c, g):
        gather[r, c, g].wait_recv()

    if last:
        def use(g, *pieces):
            for r, c in pieces:
                rows = h_buf[r, c, g].astype(F32).reshape(DEVICES, GROUP_SEQS, MY_COLS).astype(BF16)
                out_ref[:, g, :, columns(r, c)] = rows
    else:
        wq_slot = {piece: slot for slot, piece in enumerate(wq_order)}

        def use(g, *pieces):
            q_acc[g] += sum(dot(h_buf[r, c, g], w_buf[wq_slot[r, c]]) for r, c in pieces)

    def relay_first(g):
        diag_sems[g] = copies.new_receive()
        for r, device, half in ((XN, yn, top), (YN, xn, bottom)):
            gather[r, 0, g][0].wait_recv()
            copies.start(h_buf.at[r, 0, g, half], h_buf.at[DIAG, 0, g, half], device, HALVES, diag_sems[g])

    def relay_second(g):
        for r in (XN, YN):
            gather[r, 0, g][1].wait_recv()
            gather[r, 1, g] = copies.start(h_buf.at[r, 0, g], h_buf.at[r, 1, g], partner, WHOLE)

    def relay_diag(g):
        await_all(h_buf.at[DIAG, 0, g], diag_sems[g])
        gather[DIAG, 1, g] = copies.start(h_buf.at[DIAG, 0, g], h_buf.at[DIAG, 1, g], partner, WHOLE)

    def send_query(g):
        q_send[g] = q_acc[g].astype(BF16).reshape(DEVICES, GROUP_SEQS, MY_COLS)
        for to in others():
            copies.start(q_send.at[g, to], q_out.at[me, seqs[g], :], to, QUERY, q_sem)

    if not last:
        q_sem = copies.new_receive()
        await_all(w_buf, wq_sem)
        q_acc[...] = jnp.zeros_like(q_acc)
    finish_group(0)
    finish_group(1)
    relay_first(0)
    for g in range(GROUPS):
        arrive(SELF, 1, g)
        use(g, (SELF, 0), (SELF, 1))
    relay_second(0)
    use(0, (XN, 0), (YN, 0))
    relay_first(1)
    arrive(XN, 1, 0)
    arrive(YN, 1, 0)
    use(0, (XN, 1), (YN, 1))
    relay_second(1)
    use(1, (XN, 0), (YN, 0))
    relay_diag(0)
    use(0, (DIAG, 0))
    arrive(XN, 1, 1)
    arrive(YN, 1, 1)
    use(1, (XN, 1), (YN, 1))
    relay_diag(1)
    arrive(DIAG, 1, 0)
    use(0, (DIAG, 1))
    if not last:
        send_query(0)
    use(1, (DIAG, 0))
    arrive(DIAG, 1, 1)
    use(1, (DIAG, 1))

    if not last:
        send_query(GROUPS - 1)
        for g in range(GROUPS):
            q_out[me, seqs[g], :] = q_send[g, me]
        await_all(wkv_buf, wkv_sem)
        chip_rows = pl.ds(pl.multiple_of((me - core) * GROUP_SEQS, 2 * GROUP_SEQS), 2 * GROUP_SEQS)
        made = jnp.zeros((GROUPS * 2 * GROUP_SEQS, HEAD_DIM), F32)
        for r, c in wq_order:
            rows = jnp.concatenate([h_buf[r, c, g, chip_rows, :] for g in range(GROUPS)], axis=0)
            made += dot(rows, wkv_buf[columns(r, c), :])
        made = made.reshape(GROUPS, 2, GROUP_SEQS, HEAD_DIM)
        made = jnp.concatenate([made[g, k] for k in range(2) for g in range(GROUPS)], axis=0)
        shared = share_new_rows(copies, core, partner, made, kv_send, kv_out, NEW_ROWS)
        await_all(q_out.at[seven], q_sem)
        shared.wait()
        await_all(q_send.at[:, seven], send_sems.at[QUERY])
        await_all(kv_pre, cache_sem)
    await_all(ctx_in.at[seven], send_sems.at[CONTEXT])
    await_all(send_d2d, send_sems.at[CORE])
    await_all(acc.at[:, pl.ds(0, 3)], send_sems.at[SUMS])
    await_all(h_buf.at[pl.ds(0, 2)], send_sems.at[WHOLE])
    await_all(h_buf.at[pl.ds(0, 3), 0], send_sems.at[HALVES])


def combine_call(layer, last, ctx, residual, w_out, more):
    any_spec = pl.BlockSpec(memory_space=pl.ANY)
    vmem_spec = pl.BlockSpec(memory_space=pltpu.VMEM)
    receives = (2 if last else 4) + GROUPS * (4 + 4 + 9)
    scratch = [
        pltpu.VMEM((GROUPS, DEVICES, GROUP_SEQS, MY_HEADS, HEAD_DIM), BF16),
        pltpu.VMEM((GROUPS, GROUP_ROWS, MY_COLS), BF16),
        pltpu.VMEM((DEVICES, MY_COLS, MY_COLS), BF16),
        pltpu.VMEM((GROUPS, 4, GROUP_ROWS, MY_COLS), F32),
        pltpu.VMEM((GROUPS, 4, GROUP_ROWS, MY_COLS), F32),
        pltpu.VMEM((GROUPS, 4, GROUP_ROWS, MY_COLS), F32),
        pltpu.VMEM((GROUPS, HALF, MY_COLS), F32),
        pltpu.VMEM((GROUPS, HALF, MY_COLS), F32),
        pltpu.VMEM((GROUPS, 2, HALF, MY_COLS), F32),
        pltpu.VMEM((GROUPS, 2, HALF, MY_COLS), F32),
        pltpu.VMEM((4, 2, GROUPS, GROUP_ROWS, MY_COLS), BF16),
    ]
    if last:
        out_shape = pltpu.VMEM((DEVICES, GROUPS, GROUP_SEQS, D_MODEL), BF16)
        out_specs = vmem_spec
    else:
        out_shape = (pltpu.VMEM((GROUPS, GROUP_ROWS, MY_COLS), BF16),) + QUERY_SHAPES
        out_specs = (vmem_spec,) * len(out_shape)
        scratch.insert(2, pltpu.VMEM((DEVICES, GROUPS, GROUP_SEQS, MY_COLS), BF16))
        scratch += [
            pltpu.VMEM((D_MODEL, HEAD_DIM), BF16),
            pltpu.VMEM((GROUPS, GROUP_ROWS, MY_COLS), F32),
            pltpu.VMEM((GROUPS, DEVICES, GROUP_SEQS, MY_COLS), BF16),
            pltpu.VMEM((2, MY_ROWS, HEAD_DIM), BF16),
        ]
    scratch += [
        pltpu.SemaphoreType.DMA((4 if last else 8,)),
        pltpu.SemaphoreType.DMA((5 if last else 7,)),
        pltpu.SemaphoreType.DMA((receives,)),
    ]
    return pl.pallas_call(
        functools.partial(combine_kernel, layer, last),
        name="combine_last" if last else "combine",
        out_shape=out_shape,
        in_specs=[vmem_spec, vmem_spec if last else any_spec] + [any_spec] * (1 + len(more)),
        out_specs=out_specs,
        scratch_shapes=scratch,
        compiler_params=pltpu.CompilerParams(
            collective_id=2 if last else 1, has_side_effects=True, vmem_limit_bytes=40 * MIB
        ),
    )(*in_vmem(ctx), *(in_vmem if last else in_hbm)(residual), *in_hbm(w_out, *more))


def solution(mesh):
    cache_spec = P(None, ("replica", "model"), None, None)

    def device_step(x, cache_len, w_query, w_key, w_value, w_out, k_cache, v_cache):
        caches = (k_cache, v_cache)
        q, kv_new, kv_pre = query_call(x, w_query, w_key, w_value, *caches)
        ctx, k_all, v_all = attend_call(0, LATE_ROWS, cache_len, q, kv_new, kv_pre, *caches, ())
        own, q, kv_new, kv_pre = combine_call(0, False, ctx, x.reshape(DEVICES, GROUPS, GROUP_SEQS, D_MODEL), w_out, (w_query, w_key, w_value, *caches))
        ctx, k_all, v_all = attend_call(1, 0, cache_len, q, kv_new, kv_pre, *caches, (k_all, v_all))
        out = combine_call(1, True, ctx, own, w_out, ())
        return out.reshape(x.shape), k_all, v_all

    return jax.shard_map(
        device_step,
        mesh=mesh,
        in_specs=(P("replica", None), P("replica"), P(None, None, "model"), P(), P(), P(None, "model", None), cache_spec, cache_spec),
        out_specs=(P("replica", None), cache_spec, cache_spec),
        check_vma=False,
    )
```

```python
import functools

import jax
import jax.numpy as jnp
from jax import lax
from jax.experimental import pallas as pl
from jax.experimental.pallas import tpu as pltpu
from jax.sharding import PartitionSpec as P

MESH = pl.DeviceIdType.MESH
BF16 = jnp.bfloat16
F32 = jnp.float32
MIB = 1024 * 1024

DEVICES = 8
ROWS = 128
MY_ROWS = 16
D_MODEL = 8192
HEAD_DIM = 128
MY_HEADS = 8
NUM_HEADS = 64
MY_COLS = 1024
SEQ = 2048
QUERY_TILE = 512
QUERY_DEPTH = 2048

GROUPS = 2
GROUP_SEQS = MY_ROWS // GROUPS
GROUP_ROWS = ROWS // GROUPS
HALF = GROUP_ROWS // 2
LATE_ROWS = 4
READY_ROWS = 2
TOGETHER = 6
SPANS = (256, 512, 1024, 2048)


def dot(a, b):
    return jnp.dot(a, b, preferred_element_type=F32)


def places():
    me = lax.axis_index("model")
    core = lax.rem(me, 2)
    x = lax.rem(lax.div(me, 2), 2)
    y = lax.div(me, 4)
    flip = 1 - 2 * core
    xn = me + 2 - 4 * x
    yn = me + 4 - 8 * y
    diag = xn + 4 - 8 * y
    return me, flip, xn, yn, diag


def await_all(ref, sem):
    pltpu.make_async_copy(ref, ref, sem).wait()


class Copies:
    def __init__(self, send_sems, recv_sems):
        self.send_sems, self.recv_sems, self.receives = send_sems, recv_sems, 0

    def new_receive(self):
        self.receives += 1
        return self.recv_sems.at[self.receives - 1]

    def start(self, src, dst, device, kind, recv_sem=None):
        copy = pltpu.make_async_remote_copy(
            src_ref=src,
            dst_ref=dst,
            send_sem=self.send_sems.at[kind],
            recv_sem=self.new_receive() if recv_sem is None else recv_sem,
            device_id={"model": device},
            device_id_type=MESH,
        )
        copy.start()
        return copy


def meet_all(me):
    barrier = pltpu.get_barrier_semaphore()
    for k in range(1, DEVICES):
        pl.semaphore_signal(barrier, inc=1, device_id={"model": lax.rem(me + k, DEVICES)}, device_id_type=MESH)
    pl.semaphore_wait(barrier, DEVICES - 1)


def others():
    me, flip, xn, yn, diag = places()
    return [diag, diag + flip, xn, yn, xn + flip, yn + flip, me + flip]


def load_cache(layer, rows, k_hbm, v_hbm, kv, sem):
    for i, hbm in enumerate((k_hbm, v_hbm)):
        pltpu.make_async_copy(hbm.at[layer, rows], kv.at[i, rows], sem).start()


def load_kv_weights(layer, core, wk_hbm, wv_hbm, wkv_buf, sem):
    for i, hbm in enumerate((wk_hbm, wv_hbm)):
        @pl.when(core == i)
        def _():
            pltpu.make_async_copy(hbm.at[layer], wkv_buf, sem).start()


def share_new_rows(copies, core, partner, made, kv_send, kv_out, kind):
    kv_send[...] = made.reshape(2, MY_ROWS, HEAD_DIM).astype(BF16)
    copy = copies.start(kv_send.at[1 - core], kv_out.at[core], partner, kind)
    kv_out[core] = kv_send[core]
    return copy


def in_vmem(*arrays):
    return [pltpu.with_memory_space_constraint(a, pltpu.VMEM) for a in arrays]


def in_hbm(*arrays):
    return [pltpu.with_memory_space_constraint(a, pltpu.HBM) for a in arrays]


QUERY_SHAPES = (
    pltpu.VMEM((DEVICES, MY_ROWS, MY_COLS), BF16),
    pltpu.VMEM((2, MY_ROWS, HEAD_DIM), BF16),
    pltpu.VMEM((2, MY_ROWS, SEQ, HEAD_DIM), BF16),
)


def query_kernel(x_hbm, wq_hbm, wk_hbm, wv_hbm, k_hbm, v_hbm, q_out, kv_out, kv_pre,
                 x_buf, wq_buf, wkv_buf, q_send, kv_send, load_sems, send_sems, recv_sems):
    me, flip, _, _, _ = places()
    core = lax.rem(me, 2)
    columns = [pl.ds(j * QUERY_TILE, QUERY_TILE) for j in range(MY_COLS // QUERY_TILE)]
    depths = [pl.ds(k * QUERY_DEPTH, QUERY_DEPTH) for k in range(D_MODEL // QUERY_DEPTH)]
    x_sem, wkv_sem, cache_sem = [load_sems.at[i] for i in range(3)]
    x_load = pltpu.make_async_copy(x_hbm, x_buf, x_sem)
    x_load.start()
    wq_loads = []
    for cols in columns:
        for depth in depths:
            sem = load_sems.at[3 + len(wq_loads)]
            wq_loads.append(pltpu.make_async_copy(wq_hbm.at[0, depth, cols], wq_buf.at[depth, cols], sem))
            wq_loads[-1].start()
    load_kv_weights(0, core, wk_hbm, wv_hbm, wkv_buf, wkv_sem)
    early = pl.ds(0, MY_ROWS - LATE_ROWS)
    load_cache(0, early, k_hbm, v_hbm, kv_pre, cache_sem)
    meet_all(me)
    copies = Copies(send_sems, recv_sems)
    q_sem = copies.new_receive()
    x_load.wait()
    for j, cols in enumerate(columns):
        q = None
        for k, depth in enumerate(depths):
            wq_loads[j * len(depths) + k].wait()
            part = dot(x_buf[:, depth], wq_buf[depth, cols])
            q = part if q is None else q + part
        q_send[:, :, cols] = q.astype(BF16).reshape(DEVICES, MY_ROWS, QUERY_TILE)
        for to in others():
            copies.start(q_send.at[to, :, cols], q_out.at[me, :, cols], to, 0, q_sem)
    q_out[me] = q_send[me]
    chip_rows = pl.ds(pl.multiple_of((me - core) * MY_ROWS, 2 * MY_ROWS), 2 * MY_ROWS)
    await_all(wkv_buf, wkv_sem)
    shared = share_new_rows(copies, core, me + flip, dot(x_buf[chip_rows, :], wkv_buf[...]), kv_send, kv_out, 1)
    seven = pl.ds(0, DEVICES - 1)
    await_all(q_out.at[seven], q_sem)
    shared.wait()
    await_all(q_send.at[seven], send_sems.at[0])
    await_all(kv_pre.at[:, early], cache_sem)


def query_call(x, w_query, w_key, w_value, k_cache, v_cache):
    any_spec = pl.BlockSpec(memory_space=pl.ANY)
    vmem_spec = pl.BlockSpec(memory_space=pltpu.VMEM)
    return pl.pallas_call(
        query_kernel,
        name="query",
        out_shape=QUERY_SHAPES,
        in_specs=[any_spec] * 6,
        out_specs=(vmem_spec,) * len(QUERY_SHAPES),
        scratch_shapes=[
            pltpu.VMEM((ROWS, D_MODEL), BF16),
            pltpu.VMEM((D_MODEL, MY_COLS), BF16),
            pltpu.VMEM((D_MODEL, HEAD_DIM), BF16),
            pltpu.VMEM((DEVICES, MY_ROWS, MY_COLS), BF16),
            pltpu.VMEM((2, MY_ROWS, HEAD_DIM), BF16),
            pltpu.SemaphoreType.DMA((3 + (MY_COLS // QUERY_TILE) * (D_MODEL // QUERY_DEPTH),)),
            pltpu.SemaphoreType.DMA((2,)),
            pltpu.SemaphoreType.DMA((2,)),
        ],
        compiler_params=pltpu.CompilerParams(
            collective_id=0, has_side_effects=True, vmem_limit_bytes=26 * MIB
        ),
    )(*in_hbm(x, w_query, w_key, w_value, k_cache, v_cache))


def attend_kernel(layer, late_rows, ready_rows, len_hbm, q_ref, new_ref, *refs):
    k_hbm, v_hbm = refs[1:3]
    k_out, v_out, ctx_ref, kv_buf, len_ref, long_ref, q_buf, new_buf, sems = refs[-9:]
    k_buf, v_buf = kv_buf.at[0], kv_buf.at[1]
    me = lax.axis_index("model")
    out_sems, len_sem, late_sem = (sems.at[0], sems.at[1]), sems.at[2], sems.at[3]
    len_load = pltpu.make_async_copy(len_hbm, len_ref, len_sem)
    len_load.start()
    late = pl.ds(MY_ROWS - late_rows, late_rows)
    if late_rows:
        load_cache(layer, late, k_hbm, v_hbm, kv_buf, late_sem)

    def save(which, b):
        hbm, buf = ((k_out, k_buf), (v_out, v_buf))[which]
        return pltpu.make_async_copy(buf.at[b], hbm.at[layer, b], out_sems[which])

    for b in range(ready_rows):
        save(0, b).start()
        save(1, b).start()

    new_buf[...] = new_ref[...].astype(F32)
    for src in range(DEVICES):
        block = q_ref[src].astype(F32)
        for h in range(MY_HEADS):
            q_buf[:, src * MY_HEADS + h, :] = block[:, h * HEAD_DIM:(h + 1) * HEAD_DIM]

    def write_tokens(first, last):
        @pl.loop(first, last)
        def _(b):
            pos = len_ref[me * MY_ROWS + b]
            base = pl.multiple_of((pos // 16) * 16, 16)
            here = lax.broadcasted_iota(jnp.int32, (16, HEAD_DIM), 0) == pos - base
            for i, buf in enumerate((k_buf, v_buf)):
                tile = buf[b, pl.ds(base, 16), :].astype(F32)
                row = jnp.broadcast_to(new_buf[i, pl.ds(b, 1), :], (16, HEAD_DIM))
                buf[b, pl.ds(base, 16), :] = jnp.where(here, row, tile).astype(BF16)

            @pl.when(b > first)
            def _():
                save(0, b - 1).start()
                save(1, b - 1).start()

        save(0, last - 1).start()
        save(1, last - 1).start()

    len_load.wait()
    write_tokens(ready_rows, MY_ROWS - late_rows)

    scale = HEAD_DIM ** -0.5

    def attend(rows, n):
        t = lax.broadcasted_iota(jnp.int32, (NUM_HEADS, n), 1)
        s = [lax.dot_general(q_buf[b].astype(BF16), k_buf[b, 0:n, :], (((1,), (1,)), ((), ())),
                             preferred_element_type=F32) for b in rows]
        s = [jnp.where(t <= len_ref[me * MY_ROWS + b], v * scale, -jnp.inf) for v, b in zip(s, rows)]
        peak = [jnp.max(v, axis=1, keepdims=True) for v in s]
        e = [jnp.exp(v - u) for v, u in zip(s, peak)]
        share = [1.0 / jnp.sum(v, axis=1, keepdims=True) for v in e]
        p = [(v * u).astype(BF16) for v, u in zip(e, share)]
        c = [dot(v, v_buf[b, 0:n, :]) for v, b in zip(p, rows)]
        for v, b in zip(c, rows):
            ctx_ref[:, b] = v.reshape(DEVICES, MY_HEADS, HEAD_DIM).astype(BF16)

    def attend_all(first, last):
        for at in range(first, last, TOGETHER):
            attend(list(range(at, min(at + TOGETHER, last))), SPANS[0])

        def note_long(b, count):
            is_long = len_ref[me * MY_ROWS + b] >= SPANS[0]

            @pl.when(is_long)
            def _():
                long_ref[count] = b

            return count + is_long.astype(jnp.int32)

        count = lax.fori_loop(first, last, note_long, jnp.int32(0))

        @pl.loop(0, (count + 1) // 2)
        def _(i):
            pair = [long_ref[2 * i], long_ref[jnp.minimum(2 * i + 1, count - 1)]]
            longest = jnp.maximum(*[len_ref[me * MY_ROWS + b] for b in pair])
            for low, n in zip(SPANS, SPANS[1:]):
                @pl.when(jnp.logical_and(longest >= low, longest < n))
                def _(n=n):
                    attend(pair, n)

    attend_all(0, MY_ROWS - late_rows)
    if late_rows:
        await_all(kv_buf.at[:, late], late_sem)
        write_tokens(MY_ROWS - late_rows, MY_ROWS)
        attend_all(MY_ROWS - late_rows, MY_ROWS)

    for which, hbm in enumerate((k_out, v_out)):
        await_all(hbm.at[layer], out_sems[which])


def attend_call(layer, late_rows, ready_rows, cache_len, q, kv_new, kv_pre, k_cache, v_cache, prev):
    any_spec = pl.BlockSpec(memory_space=pl.ANY)
    vmem_spec = pl.BlockSpec(memory_space=pltpu.VMEM)
    k_all, v_all, ctx, _ = pl.pallas_call(
        functools.partial(attend_kernel, layer, late_rows, ready_rows),
        name="attend",
        out_shape=(
            jax.ShapeDtypeStruct(k_cache.shape, BF16),
            jax.ShapeDtypeStruct(v_cache.shape, BF16),
            pltpu.VMEM((DEVICES, MY_ROWS, MY_HEADS, HEAD_DIM), BF16),
            pltpu.VMEM(kv_pre.shape, BF16),
        ),
        in_specs=[vmem_spec] * 4 + [any_spec] * (2 + len(prev)),
        out_specs=(any_spec, any_spec, vmem_spec, vmem_spec),
        scratch_shapes=[
            pltpu.SMEM((ROWS,), jnp.int32),
            pltpu.SMEM((MY_ROWS,), jnp.int32),
            pltpu.VMEM((MY_ROWS, NUM_HEADS, HEAD_DIM), F32),
            pltpu.VMEM((2, MY_ROWS, HEAD_DIM), F32),
            pltpu.SemaphoreType.DMA((4,)),
        ],
        input_output_aliases={3: 3} | ({6: 0, 7: 1} if prev else {}),
        compiler_params=pltpu.CompilerParams(vmem_limit_bytes=16 * MIB),
    )(*in_vmem(cache_len, q, kv_new, kv_pre), *in_hbm(k_cache, v_cache), *prev)
    return ctx, k_all, v_all


SELF, XN, YN, DIAG = range(4)
PASS_ON_AFTER = XN
LEFT, RIGHT, WHOLE_WIDTH = pl.ds(0, MY_COLS // 2), pl.ds(MY_COLS // 2, MY_COLS // 2), pl.ds(0, MY_COLS)
CONTEXT, CORE, SUMS, WHOLE, HALVES, QUERY, NEW_ROWS = range(7)


def combine_kernel(layer, last, *refs):
    if last:
        (ctx_in, res_buf, wo_hbm, out_ref,
         ctx_buf, lhs, w_buf, send_d2d, recv_d2d, acc, diag_in, top_in, bottom_in, h_buf,
         load_sems, send_sems, recv_sems) = refs
    else:
        (ctx_in, res_hbm, wo_hbm, wq_hbm, wk_hbm, wv_hbm, k_hbm, v_hbm, len_hbm, own_out, q_out, kv_out, kv_pre,
         ctx_buf, lhs, res_buf, w_buf, send_d2d, recv_d2d, acc, diag_in, top_in, bottom_in, h_buf,
         wkv_buf, q_acc, q_send, kv_send, len_ref,
         load_sems, send_sems, recv_sems) = refs
    me, flip, xn, yn, diag = places()
    partner, core = me + flip, lax.rem(me, 2)
    chip_mate = {SELF: me, XN: xn, YN: yn, DIAG: diag}
    columns = lambda r, c: pl.ds(pl.multiple_of((chip_mate[r] + c * flip) * MY_COLS, MY_COLS), MY_COLS)
    copies = Copies(send_sems, recv_sems)
    wo_order = [(r, c) for r in (DIAG, XN, YN, SELF) for c in (1, 0)]
    wq_order = [(r, c) for r in (SELF, XN, YN, DIAG) for c in (0, 1)]
    top, bottom = pl.ds(0, HALF), pl.ds(HALF, HALF)
    seven = pl.ds(0, DEVICES - 1)
    seqs = [pl.ds(g * GROUP_SEQS, GROUP_SEQS) for g in range(GROUPS)]

    for slot, (r, c) in enumerate(wo_order):
        pltpu.make_async_copy(wo_hbm.at[layer, :, columns(r, c)], w_buf.at[slot], load_sems.at[slot // 2]).start()
    if not last:
        wq_sem, res_sem, wkv_sem, cache_sem, len_sem = [load_sems.at[4 + i] for i in range(5)]
        res_load = pltpu.make_async_copy(res_hbm.at[:, :, :, columns(SELF, 0)], res_buf, res_sem)
        res_load.start()
        load_kv_weights(layer + 1, core, wk_hbm, wv_hbm, wkv_buf, wkv_sem)
        len_load = pltpu.make_async_copy(len_hbm, len_ref, len_sem)
        len_load.start()

    meet_all(me)

    ctx_sems = [copies.new_receive() for _ in range(GROUPS)]

    def send_context(g):
        for to in others():
            copies.start(ctx_in.at[to, seqs[g]], ctx_buf.at[g, me], to, CONTEXT, ctx_sems[g])
        ctx_buf[g, me] = ctx_in[me, seqs[g]]

    send_context(0)

    d2d, first, in_sems = {}, {}, {}

    def receive_context(g):
        await_all(ctx_buf.at[g, seven], ctx_sems[g])
        if g + 1 < GROUPS:
            send_context(g + 1)
        rows = ctx_buf[g].astype(F32).reshape(GROUP_ROWS, MY_HEADS, HEAD_DIM)
        lhs[g] = rows.reshape(GROUP_ROWS, MY_COLS).astype(BF16)

    def add_partner(g, r, cols):
        await_all(recv_d2d.at[g, r, :, cols], d2d[g, r, cols.start])
        acc[g, r, :, cols] += recv_d2d[g, r, :, cols]

    def start_diagonal(g, cols):
        if g not in first:
            first[g] = copies.new_receive()
        add_partner(g, DIAG, cols)
        copies.start(acc.at[g, DIAG, top, cols], diag_in.at[g, 0, :, cols], xn, SUMS, first[g])
        copies.start(acc.at[g, DIAG, bottom, cols], diag_in.at[g, 1, :, cols], yn, SUMS, first[g])

    def settle(g, r):
        if r == DIAG:
            start_diagonal(g, pieces_of(g, r)[-1])
            return
        add_partner(g, r, WHOLE_WIDTH)
        if r == YN:
            in_sems[g] = copies.new_receive(), copies.new_receive()
            copies.start(acc.at[g, XN, top], top_in.at[g, 0], xn, SUMS, in_sems[g][0])
            copies.start(acc.at[g, YN, bottom], bottom_in.at[g, 0], yn, SUMS, in_sems[g][1])

    def pieces_of(g, r):
        return (LEFT, RIGHT) if (g, r) == (0, DIAG) else (WHOLE_WIDTH,)

    def pass_on(g):
        await_all(diag_in.at[g], first[g])
        acc[g, YN, top] += diag_in[g, 0]
        copies.start(acc.at[g, YN, top], top_in.at[g, 1], yn, SUMS, in_sems[g][0])
        acc[g, XN, bottom] += diag_in[g, 1]
        copies.start(acc.at[g, XN, bottom], bottom_in.at[g, 1], xn, SUMS, in_sems[g][1])

    pending = None
    for g in range(GROUPS):
        receive_context(g)
        for slot, (r, c) in enumerate(wo_order):
            if g == 0 and c == 1:
                await_all(w_buf.at[pl.ds(slot, 2)], load_sems.at[slot // 2])
            if c == 1:
                for cols in pieces_of(g, r):
                    d2d[g, r, cols.start] = copies.new_receive()
                    send_d2d[g, r, :, cols] = dot(lhs[g], w_buf[slot, :, cols])
                    copies.start(send_d2d.at[g, r, :, cols], recv_d2d.at[g, r, :, cols], partner, CORE, d2d[g, r, cols.start])
            else:
                acc[g, r] = dot(lhs[g], w_buf[slot])
                if len(pieces_of(g, r)) > 1:
                    start_diagonal(g, LEFT)
            if not last and g == GROUPS - 1:
                pltpu.make_async_copy(wq_hbm.at[layer + 1, columns(*wq_order[slot]), :], w_buf.at[slot], wq_sem).start()
            if c == 1 and pending is not None:
                settle(*pending)
                if g > 0 and pending == (g, PASS_ON_AFTER):
                    pass_on(g - 1)
            pending = (g, r)
    settle(*pending)
    if not last:
        load_cache(layer + 1, pl.ds(0, MY_ROWS), k_hbm, v_hbm, kv_pre, cache_sem)
    pass_on(GROUPS - 1)

    gather, diag_sems, relay_sems = {}, {}, {}
    if not last:
        res_load.wait()

    def finish_group(g):
        if last:
            residual = res_buf[g].astype(F32)
        else:
            residual = res_buf[:, g].astype(F32).reshape(GROUP_ROWS, MY_COLS)
        await_all(top_in.at[g], in_sems[g][0])
        total = acc[g, SELF, top] + top_in[g, 0] + top_in[g, 1]
        h_buf[SELF, 0, g, top] = (residual[:HALF] + total).astype(BF16)
        await_all(bottom_in.at[g], in_sems[g][1])
        total = acc[g, SELF, bottom] + bottom_in[g, 0] + bottom_in[g, 1]
        h_buf[SELF, 0, g, bottom] = (residual[HALF:] + total).astype(BF16)
        mine = h_buf.at[SELF, 0, g]
        for r, device, halves in ((XN, xn, (top, bottom)), (YN, yn, (bottom, top))):
            gather[r, 0, g] = [copies.start(h_buf.at[SELF, 0, g, half], h_buf.at[r, 0, g, half], device, HALVES)
                               for half in halves]
        gather[SELF, 1, g] = copies.start(mine, h_buf.at[SELF, 1, g], partner, WHOLE)
        if not last:
            own_out[g] = h_buf[SELF, 0, g]

    def arrive(r, c, g):
        gather[r, c, g].wait_recv()

    if last:
        def use(g, *pieces):
            for r, c in pieces:
                rows = h_buf[r, c, g].astype(F32).reshape(DEVICES, GROUP_SEQS, MY_COLS).astype(BF16)
                out_ref[:, g, :, columns(r, c)] = rows
    else:
        wq_slot = {piece: slot for slot, piece in enumerate(wq_order)}

        def use(g, *pieces):
            q_acc[g] += sum(dot(h_buf[r, c, g], w_buf[wq_slot[r, c]]) for r, c in pieces)

    def relay_first(g):
        diag_sems[g] = copies.new_receive()
        for r, device, half in ((XN, yn, top), (YN, xn, bottom)):
            gather[r, 0, g][0].wait_recv()
            copies.start(h_buf.at[r, 0, g, half], h_buf.at[DIAG, 0, g, half], device, HALVES, diag_sems[g])

    def relay_second(g):
        relay_sems[g] = copies.new_receive()
        for r in (XN, YN):
            gather[r, 0, g][1].wait_recv()
            copies.start(h_buf.at[r, 0, g], h_buf.at[r, 1, g], partner, WHOLE, relay_sems[g])

    def relay_diag(g):
        await_all(h_buf.at[DIAG, 0, g], diag_sems[g])
        gather[DIAG, 1, g] = copies.start(h_buf.at[DIAG, 0, g], h_buf.at[DIAG, 1, g], partner, WHOLE)

    def send_query(g):
        q_send[g] = q_acc[g].astype(BF16).reshape(DEVICES, GROUP_SEQS, MY_COLS)
        for to in others():
            copies.start(q_send.at[g, to], q_out.at[me, seqs[g], :], to, QUERY, q_sem)

    if not last:
        q_sem = copies.new_receive()
        await_all(w_buf, wq_sem)
        q_acc[...] = jnp.zeros_like(q_acc)
    finish_group(0)
    finish_group(1)
    relay_first(0)
    for g in range(GROUPS):
        arrive(SELF, 1, g)
        use(g, (SELF, 0), (SELF, 1))
    relay_second(0)
    use(0, (XN, 0), (YN, 0))
    relay_first(1)
    await_all(h_buf.at[pl.ds(XN, 2), 1, 0], relay_sems[0])
    use(0, (XN, 1), (YN, 1))
    relay_second(1)
    use(1, (XN, 0), (YN, 0))
    relay_diag(0)
    use(0, (DIAG, 0))
    await_all(h_buf.at[pl.ds(XN, 2), 1, 1], relay_sems[1])
    use(1, (XN, 1), (YN, 1))
    relay_diag(1)
    arrive(DIAG, 1, 0)
    use(0, (DIAG, 1))
    if not last:
        send_query(0)
    use(1, (DIAG, 0))
    arrive(DIAG, 1, 1)
    use(1, (DIAG, 1))

    if not last:
        send_query(GROUPS - 1)
        for g in range(GROUPS):
            q_out[me, seqs[g], :] = q_send[g, me]
        await_all(wkv_buf, wkv_sem)
        chip_rows = pl.ds(pl.multiple_of((me - core) * GROUP_SEQS, 2 * GROUP_SEQS), 2 * GROUP_SEQS)
        made = jnp.zeros((GROUPS * 2 * GROUP_SEQS, HEAD_DIM), F32)
        for r, c in wq_order:
            rows = jnp.concatenate([h_buf[r, c, g, chip_rows, :] for g in range(GROUPS)], axis=0)
            made += dot(rows, wkv_buf[columns(r, c), :])
        made = made.reshape(GROUPS, 2, GROUP_SEQS, HEAD_DIM)
        made = jnp.concatenate([made[g, k] for k in range(2) for g in range(GROUPS)], axis=0)
        shared = share_new_rows(copies, core, partner, made, kv_send, kv_out, NEW_ROWS)
        len_load.wait()
        await_all(kv_pre, cache_sem)
        shared.wait()
        for b in range(READY_ROWS):
            here = lax.broadcasted_iota(jnp.int32, (SEQ, HEAD_DIM), 0) == len_ref[me * MY_ROWS + b]
            for i in range(2):
                row = jnp.broadcast_to(kv_out[i, b:b + 1, :].astype(F32), (SEQ, HEAD_DIM))
                kv_pre[i, b] = jnp.where(here, row, kv_pre[i, b].astype(F32)).astype(BF16)
        await_all(q_out.at[seven], q_sem)
        await_all(q_send.at[:, seven], send_sems.at[QUERY])
    await_all(ctx_in.at[seven], send_sems.at[CONTEXT])
    await_all(send_d2d, send_sems.at[CORE])
    await_all(acc.at[:, pl.ds(0, 3)], send_sems.at[SUMS])
    await_all(h_buf.at[pl.ds(0, 2)], send_sems.at[WHOLE])
    await_all(h_buf.at[pl.ds(0, 3), 0], send_sems.at[HALVES])


def combine_call(layer, last, ctx, residual, w_out, more):
    any_spec = pl.BlockSpec(memory_space=pl.ANY)
    vmem_spec = pl.BlockSpec(memory_space=pltpu.VMEM)
    receives = (2 if last else 4) + 1 + GROUPS * (4 + 3 + 8)
    scratch = [
        pltpu.VMEM((GROUPS, DEVICES, GROUP_SEQS, MY_HEADS, HEAD_DIM), BF16),
        pltpu.VMEM((GROUPS, GROUP_ROWS, MY_COLS), BF16),
        pltpu.VMEM((DEVICES, MY_COLS, MY_COLS), BF16),
        pltpu.VMEM((GROUPS, 4, GROUP_ROWS, MY_COLS), F32),
        pltpu.VMEM((GROUPS, 4, GROUP_ROWS, MY_COLS), F32),
        pltpu.VMEM((GROUPS, 4, GROUP_ROWS, MY_COLS), F32),
        pltpu.VMEM((GROUPS, 2, HALF, MY_COLS), F32),
        pltpu.VMEM((GROUPS, 2, HALF, MY_COLS), F32),
        pltpu.VMEM((GROUPS, 2, HALF, MY_COLS), F32),
        pltpu.VMEM((4, 2, GROUPS, GROUP_ROWS, MY_COLS), BF16),
    ]
    if last:
        out_shape = pltpu.VMEM((DEVICES, GROUPS, GROUP_SEQS, D_MODEL), BF16)
        out_specs = vmem_spec
    else:
        out_shape = (pltpu.VMEM((GROUPS, GROUP_ROWS, MY_COLS), BF16),) + QUERY_SHAPES
        out_specs = (vmem_spec,) * len(out_shape)
        scratch.insert(2, pltpu.VMEM((DEVICES, GROUPS, GROUP_SEQS, MY_COLS), BF16))
        scratch += [
            pltpu.VMEM((D_MODEL, HEAD_DIM), BF16),
            pltpu.VMEM((GROUPS, GROUP_ROWS, MY_COLS), F32),
            pltpu.VMEM((GROUPS, DEVICES, GROUP_SEQS, MY_COLS), BF16),
            pltpu.VMEM((2, MY_ROWS, HEAD_DIM), BF16),
            pltpu.SMEM((ROWS,), jnp.int32),
        ]
    scratch += [
        pltpu.SemaphoreType.DMA((4 if last else 9,)),
        pltpu.SemaphoreType.DMA((5 if last else 7,)),
        pltpu.SemaphoreType.DMA((receives,)),
    ]
    return pl.pallas_call(
        functools.partial(combine_kernel, layer, last),
        name="combine_last" if last else "combine",
        out_shape=out_shape,
        in_specs=[vmem_spec, vmem_spec if last else any_spec] + [any_spec] * (1 + len(more)),
        out_specs=out_specs,
        scratch_shapes=scratch,
        compiler_params=pltpu.CompilerParams(
            collective_id=2 if last else 1, has_side_effects=True, vmem_limit_bytes=40 * MIB
        ),
    )(*in_vmem(ctx), *(in_vmem if last else in_hbm)(residual), *in_hbm(w_out, *more))


def solution(mesh):
    cache_spec = P(None, ("replica", "model"), None, None)

    def device_step(x, cache_len, w_query, w_key, w_value, w_out, k_cache, v_cache):
        caches = (k_cache, v_cache)
        q, kv_new, kv_pre = query_call(x, w_query, w_key, w_value, *caches)
        ctx, k_all, v_all = attend_call(0, LATE_ROWS, 0, cache_len, q, kv_new, kv_pre, *caches, ())
        own, q, kv_new, kv_pre = combine_call(0, False, ctx, x.reshape(DEVICES, GROUPS, GROUP_SEQS, D_MODEL), w_out, (w_query, w_key, w_value, *caches, cache_len))
        ctx, k_all, v_all = attend_call(1, 0, READY_ROWS, cache_len, q, kv_new, kv_pre, *caches, (k_all, v_all))
        out = combine_call(1, True, ctx, own, w_out, ())
        return out.reshape(x.shape), k_all, v_all

    return jax.shard_map(
        device_step,
        mesh=mesh,
        in_specs=(P("replica", None), P("replica"), P(None, None, "model"), P(), P(), P(None, "model", None), cache_spec, cache_spec),
        out_specs=(P("replica", None), cache_spec, cache_spec),
        check_vma=False,
    )
```

```python
import functools

import jax
import jax.numpy as jnp
from jax import lax
from jax.experimental import pallas as pl
from jax.experimental.pallas import tpu as pltpu
from jax.sharding import PartitionSpec as P

MESH = pl.DeviceIdType.MESH
BF16 = jnp.bfloat16
F32 = jnp.float32
MIB = 1024 * 1024

DEVICES = 8
ROWS = 128
MY_ROWS = 16
D_MODEL = 8192
HEAD_DIM = 128
MY_HEADS = 8
NUM_HEADS = 64
MY_COLS = 1024
SEQ = 2048
QUERY_TILE = 512
QUERY_DEPTH = 2048

GROUPS = 2
GROUP_SEQS = MY_ROWS // GROUPS
GROUP_ROWS = ROWS // GROUPS
HALF = GROUP_ROWS // 2
LATE_ROWS = 4
READY_ROWS = 2
TOGETHER = 6
SPANS = (256, 512, 1024, 2048)


def dot(a, b):
    return jnp.dot(a, b, preferred_element_type=F32)


def places():
    me = lax.axis_index("model")
    core = lax.rem(me, 2)
    x = lax.rem(lax.div(me, 2), 2)
    y = lax.div(me, 4)
    flip = 1 - 2 * core
    xn = me + 2 - 4 * x
    yn = me + 4 - 8 * y
    diag = xn + 4 - 8 * y
    return me, flip, xn, yn, diag


def await_all(ref, sem):
    pltpu.make_async_copy(ref, ref, sem).wait()


class Copies:
    def __init__(self, send_sems, recv_sems):
        self.send_sems, self.recv_sems, self.receives = send_sems, recv_sems, 0

    def new_receive(self):
        self.receives += 1
        return self.recv_sems.at[self.receives - 1]

    def start(self, src, dst, device, kind, recv_sem=None):
        copy = pltpu.make_async_remote_copy(
            src_ref=src,
            dst_ref=dst,
            send_sem=self.send_sems.at[kind],
            recv_sem=self.new_receive() if recv_sem is None else recv_sem,
            device_id={"model": device},
            device_id_type=MESH,
        )
        copy.start()
        return copy


def greet_all(me):
    for k in range(1, DEVICES):
        pl.semaphore_signal(pltpu.get_barrier_semaphore(), inc=1, device_id={"model": lax.rem(me + k, DEVICES)}, device_id_type=MESH)


def await_greetings():
    pl.semaphore_wait(pltpu.get_barrier_semaphore(), DEVICES - 1)


def others():
    me, flip, xn, yn, diag = places()
    return [diag, diag + flip, xn, yn, xn + flip, yn + flip, me + flip]


def load_cache(layer, rows, k_hbm, v_hbm, kv, sem):
    for i, hbm in enumerate((k_hbm, v_hbm)):
        pltpu.make_async_copy(hbm.at[layer, rows], kv.at[i, rows], sem).start()


def load_kv_weights(layer, core, wk_hbm, wv_hbm, wkv_buf, sem):
    for i, hbm in enumerate((wk_hbm, wv_hbm)):
        @pl.when(core == i)
        def _():
            pltpu.make_async_copy(hbm.at[layer], wkv_buf, sem).start()


def share_new_rows(copies, core, partner, made, kv_send, kv_out, kind):
    kv_send[...] = made.reshape(2, MY_ROWS, HEAD_DIM).astype(BF16)
    copy = copies.start(kv_send.at[1 - core], kv_out.at[core], partner, kind)
    kv_out[core] = kv_send[core]
    return copy


def in_vmem(*arrays):
    return [pltpu.with_memory_space_constraint(a, pltpu.VMEM) for a in arrays]


def in_hbm(*arrays):
    return [pltpu.with_memory_space_constraint(a, pltpu.HBM) for a in arrays]


QUERY_SHAPES = (
    pltpu.VMEM((DEVICES, MY_ROWS, MY_COLS), BF16),
    pltpu.VMEM((2, MY_ROWS, HEAD_DIM), BF16),
    pltpu.VMEM((2, MY_ROWS, SEQ, HEAD_DIM), BF16),
)


def query_kernel(x_hbm, wq_hbm, wk_hbm, wv_hbm, k_hbm, v_hbm, q_out, kv_out, kv_pre,
                 x_buf, wq_buf, wkv_buf, q_send, kv_send, load_sems, send_sems, recv_sems):
    me, flip, _, _, _ = places()
    core = lax.rem(me, 2)
    columns = [pl.ds(j * QUERY_TILE, QUERY_TILE) for j in range(MY_COLS // QUERY_TILE)]
    depths = [pl.ds(k * QUERY_DEPTH, QUERY_DEPTH) for k in range(D_MODEL // QUERY_DEPTH)]
    x_sem, wkv_sem, cache_sem = [load_sems.at[i] for i in range(3)]
    x_load = pltpu.make_async_copy(x_hbm, x_buf, x_sem)
    x_load.start()
    wq_loads = []
    for cols in columns:
        for depth in depths:
            sem = load_sems.at[3 + len(wq_loads)]
            wq_loads.append(pltpu.make_async_copy(wq_hbm.at[0, depth, cols], wq_buf.at[depth, cols], sem))
            wq_loads[-1].start()
    load_kv_weights(0, core, wk_hbm, wv_hbm, wkv_buf, wkv_sem)
    early = pl.ds(0, MY_ROWS - LATE_ROWS)
    load_cache(0, early, k_hbm, v_hbm, kv_pre, cache_sem)
    greet_all(me)
    await_greetings()
    copies = Copies(send_sems, recv_sems)
    q_sem = copies.new_receive()
    x_load.wait()
    for j, cols in enumerate(columns):
        q = None
        for k, depth in enumerate(depths):
            wq_loads[j * len(depths) + k].wait()
            part = dot(x_buf[:, depth], wq_buf[depth, cols])
            q = part if q is None else q + part
        q_send[:, :, cols] = q.astype(BF16).reshape(DEVICES, MY_ROWS, QUERY_TILE)
        for to in others():
            copies.start(q_send.at[to, :, cols], q_out.at[me, :, cols], to, 0, q_sem)
    q_out[me] = q_send[me]
    chip_rows = pl.ds(pl.multiple_of((me - core) * MY_ROWS, 2 * MY_ROWS), 2 * MY_ROWS)
    await_all(wkv_buf, wkv_sem)
    shared = share_new_rows(copies, core, me + flip, dot(x_buf[chip_rows, :], wkv_buf[...]), kv_send, kv_out, 1)
    seven = pl.ds(0, DEVICES - 1)
    await_all(q_out.at[seven], q_sem)
    shared.wait()
    await_all(q_send.at[seven], send_sems.at[0])
    await_all(kv_pre.at[:, early], cache_sem)


def query_call(x, w_query, w_key, w_value, k_cache, v_cache):
    any_spec = pl.BlockSpec(memory_space=pl.ANY)
    vmem_spec = pl.BlockSpec(memory_space=pltpu.VMEM)
    return pl.pallas_call(
        query_kernel,
        name="query",
        out_shape=QUERY_SHAPES,
        in_specs=[any_spec] * 6,
        out_specs=(vmem_spec,) * len(QUERY_SHAPES),
        scratch_shapes=[
            pltpu.VMEM((ROWS, D_MODEL), BF16),
            pltpu.VMEM((D_MODEL, MY_COLS), BF16),
            pltpu.VMEM((D_MODEL, HEAD_DIM), BF16),
            pltpu.VMEM((DEVICES, MY_ROWS, MY_COLS), BF16),
            pltpu.VMEM((2, MY_ROWS, HEAD_DIM), BF16),
            pltpu.SemaphoreType.DMA((3 + (MY_COLS // QUERY_TILE) * (D_MODEL // QUERY_DEPTH),)),
            pltpu.SemaphoreType.DMA((2,)),
            pltpu.SemaphoreType.DMA((2,)),
        ],
        compiler_params=pltpu.CompilerParams(
            collective_id=0, has_side_effects=True, vmem_limit_bytes=26 * MIB
        ),
    )(*in_hbm(x, w_query, w_key, w_value, k_cache, v_cache))


def attend_kernel(layer, late_rows, ready_rows, len_hbm, q_ref, new_ref, *refs):
    k_hbm, v_hbm = refs[1:3]
    k_out, v_out, ctx_ref, kv_buf, len_ref, long_ref, q_buf, new_buf, sems = refs[-9:]
    k_buf, v_buf = kv_buf.at[0], kv_buf.at[1]
    me = lax.axis_index("model")
    out_sems, len_sem, late_sem = (sems.at[0], sems.at[1]), sems.at[2], sems.at[3]
    len_load = pltpu.make_async_copy(len_hbm, len_ref, len_sem)
    len_load.start()
    late = pl.ds(MY_ROWS - late_rows, late_rows)
    if late_rows:
        load_cache(layer, late, k_hbm, v_hbm, kv_buf, late_sem)

    def save(which, b):
        hbm, buf = ((k_out, k_buf), (v_out, v_buf))[which]
        return pltpu.make_async_copy(buf.at[b], hbm.at[layer, b], out_sems[which])

    for b in range(ready_rows):
        save(0, b).start()
        save(1, b).start()

    new_buf[...] = new_ref[...].astype(F32)
    for src in range(DEVICES):
        block = q_ref[src].astype(F32)
        for h in range(MY_HEADS):
            q_buf[:, src * MY_HEADS + h, :] = block[:, h * HEAD_DIM:(h + 1) * HEAD_DIM]

    def write_tokens(first, last):
        @pl.loop(first, last)
        def _(b):
            pos = len_ref[me * MY_ROWS + b]
            base = pl.multiple_of((pos // 16) * 16, 16)
            here = lax.broadcasted_iota(jnp.int32, (16, HEAD_DIM), 0) == pos - base
            for i, buf in enumerate((k_buf, v_buf)):
                tile = buf[b, pl.ds(base, 16), :].astype(F32)
                row = jnp.broadcast_to(new_buf[i, pl.ds(b, 1), :], (16, HEAD_DIM))
                buf[b, pl.ds(base, 16), :] = jnp.where(here, row, tile).astype(BF16)

            @pl.when(b > first)
            def _():
                save(0, b - 1).start()
                save(1, b - 1).start()

        save(0, last - 1).start()
        save(1, last - 1).start()

    len_load.wait()
    write_tokens(ready_rows, MY_ROWS - late_rows)

    scale = HEAD_DIM ** -0.5

    def attend(rows, n):
        t = lax.broadcasted_iota(jnp.int32, (NUM_HEADS, n), 1)
        s = [lax.dot_general(q_buf[b].astype(BF16), k_buf[b, 0:n, :], (((1,), (1,)), ((), ())),
                             preferred_element_type=F32) for b in rows]
        s = [jnp.where(t <= len_ref[me * MY_ROWS + b], v * scale, -jnp.inf) for v, b in zip(s, rows)]
        peak = [jnp.max(v, axis=1, keepdims=True) for v in s]
        e = [jnp.exp(v - u) for v, u in zip(s, peak)]
        share = [1.0 / jnp.sum(v, axis=1, keepdims=True) for v in e]
        p = [(v * u).astype(BF16) for v, u in zip(e, share)]
        c = [dot(v, v_buf[b, 0:n, :]) for v, b in zip(p, rows)]
        for v, b in zip(c, rows):
            ctx_ref[:, b] = v.reshape(DEVICES, MY_HEADS, HEAD_DIM).astype(BF16)

    def attend_all(first, last):
        for at in range(first, last, TOGETHER):
            attend(list(range(at, min(at + TOGETHER, last))), SPANS[0])

        def note_long(b, count):
            is_long = len_ref[me * MY_ROWS + b] >= SPANS[0]

            @pl.when(is_long)
            def _():
                long_ref[count] = b

            return count + is_long.astype(jnp.int32)

        count = lax.fori_loop(first, last, note_long, jnp.int32(0))

        @pl.loop(0, (count + 1) // 2)
        def _(i):
            pair = [long_ref[2 * i], long_ref[jnp.minimum(2 * i + 1, count - 1)]]
            longest = jnp.maximum(*[len_ref[me * MY_ROWS + b] for b in pair])
            for low, n in zip(SPANS, SPANS[1:]):
                @pl.when(jnp.logical_and(longest >= low, longest < n))
                def _(n=n):
                    attend(pair, n)

    attend_all(0, MY_ROWS - late_rows)
    if late_rows:
        await_all(kv_buf.at[:, late], late_sem)
        write_tokens(MY_ROWS - late_rows, MY_ROWS)
        attend_all(MY_ROWS - late_rows, MY_ROWS)

    for which, hbm in enumerate((k_out, v_out)):
        await_all(hbm.at[layer], out_sems[which])


def attend_call(layer, late_rows, ready_rows, cache_len, q, kv_new, kv_pre, k_cache, v_cache, prev):
    any_spec = pl.BlockSpec(memory_space=pl.ANY)
    vmem_spec = pl.BlockSpec(memory_space=pltpu.VMEM)
    k_all, v_all, ctx, _ = pl.pallas_call(
        functools.partial(attend_kernel, layer, late_rows, ready_rows),
        name="attend",
        out_shape=(
            jax.ShapeDtypeStruct(k_cache.shape, BF16),
            jax.ShapeDtypeStruct(v_cache.shape, BF16),
            pltpu.VMEM((DEVICES, MY_ROWS, MY_HEADS, HEAD_DIM), BF16),
            pltpu.VMEM(kv_pre.shape, BF16),
        ),
        in_specs=[vmem_spec] * 4 + [any_spec] * (2 + len(prev)),
        out_specs=(any_spec, any_spec, vmem_spec, vmem_spec),
        scratch_shapes=[
            pltpu.SMEM((ROWS,), jnp.int32),
            pltpu.SMEM((MY_ROWS,), jnp.int32),
            pltpu.VMEM((MY_ROWS, NUM_HEADS, HEAD_DIM), F32),
            pltpu.VMEM((2, MY_ROWS, HEAD_DIM), F32),
            pltpu.SemaphoreType.DMA((4,)),
        ],
        input_output_aliases={3: 3} | ({6: 0, 7: 1} if prev else {}),
        compiler_params=pltpu.CompilerParams(vmem_limit_bytes=16 * MIB),
    )(*in_vmem(cache_len, q, kv_new, kv_pre), *in_hbm(k_cache, v_cache), *prev)
    return ctx, k_all, v_all


SELF, XN, YN, DIAG = range(4)
PASS_ON_AFTER = XN
LEFT, RIGHT, WHOLE_WIDTH = pl.ds(0, MY_COLS // 2), pl.ds(MY_COLS // 2, MY_COLS // 2), pl.ds(0, MY_COLS)
CONTEXT, CORE, SUMS, WHOLE, HALVES, QUERY, NEW_ROWS = range(7)


def combine_kernel(layer, last, *refs):
    if last:
        (ctx_in, res_buf, wo_hbm, out_ref,
         ctx_buf, lhs, w_buf, send_d2d, recv_d2d, acc, diag_in, top_in, bottom_in, h_buf,
         load_sems, send_sems, recv_sems) = refs
    else:
        (ctx_in, res_hbm, wo_hbm, wq_hbm, wk_hbm, wv_hbm, k_hbm, v_hbm, len_hbm, own_out, q_out, kv_out, kv_pre,
         ctx_buf, lhs, res_buf, w_buf, send_d2d, recv_d2d, acc, diag_in, top_in, bottom_in, h_buf,
         wkv_buf, q_acc, q_send, kv_send, len_ref,
         load_sems, send_sems, recv_sems) = refs
    me, flip, xn, yn, diag = places()
    partner, core = me + flip, lax.rem(me, 2)
    greet_all(me)
    chip_mate = {SELF: me, XN: xn, YN: yn, DIAG: diag}
    columns = lambda r, c: pl.ds(pl.multiple_of((chip_mate[r] + c * flip) * MY_COLS, MY_COLS), MY_COLS)
    copies = Copies(send_sems, recv_sems)
    wo_order = [(r, c) for r in (DIAG, XN, YN, SELF) for c in (1, 0)]
    wq_order = [(r, c) for r in (SELF, XN, YN, DIAG) for c in (0, 1)]
    top, bottom = pl.ds(0, HALF), pl.ds(HALF, HALF)
    seven = pl.ds(0, DEVICES - 1)
    seqs = [pl.ds(g * GROUP_SEQS, GROUP_SEQS) for g in range(GROUPS)]

    for slot, (r, c) in enumerate(wo_order):
        pltpu.make_async_copy(wo_hbm.at[layer, :, columns(r, c)], w_buf.at[slot], load_sems.at[slot // 2]).start()
    if not last:
        wq_sem, res_sem, wkv_sem, cache_sem, len_sem = [load_sems.at[4 + i] for i in range(5)]
        res_load = pltpu.make_async_copy(res_hbm.at[:, :, :, columns(SELF, 0)], res_buf, res_sem)
        res_load.start()
        load_kv_weights(layer + 1, core, wk_hbm, wv_hbm, wkv_buf, wkv_sem)
        len_load = pltpu.make_async_copy(len_hbm, len_ref, len_sem)
        len_load.start()

    await_greetings()

    ctx_sems = [copies.new_receive() for _ in range(GROUPS)]

    def send_context(g):
        for to in others():
            copies.start(ctx_in.at[to, seqs[g]], ctx_buf.at[g, me], to, CONTEXT, ctx_sems[g])
        ctx_buf[g, me] = ctx_in[me, seqs[g]]

    send_context(0)

    d2d, first, in_sems = {}, {}, {}

    def receive_context(g):
        await_all(ctx_buf.at[g, seven], ctx_sems[g])
        if g + 1 < GROUPS:
            send_context(g + 1)
        rows = ctx_buf[g].astype(F32).reshape(GROUP_ROWS, MY_HEADS, HEAD_DIM)
        lhs[g] = rows.reshape(GROUP_ROWS, MY_COLS).astype(BF16)

    def add_partner(g, r, cols):
        await_all(recv_d2d.at[g, r, :, cols], d2d[g, r, cols.start])
        acc[g, r, :, cols] += recv_d2d[g, r, :, cols]

    def start_diagonal(g, cols):
        if g not in first:
            first[g] = copies.new_receive()
        add_partner(g, DIAG, cols)
        copies.start(acc.at[g, DIAG, top, cols], diag_in.at[g, 0, :, cols], xn, SUMS, first[g])
        copies.start(acc.at[g, DIAG, bottom, cols], diag_in.at[g, 1, :, cols], yn, SUMS, first[g])

    def settle(g, r):
        if r == DIAG:
            start_diagonal(g, pieces_of(g, r)[-1])
            return
        add_partner(g, r, WHOLE_WIDTH)
        if r == YN:
            in_sems[g] = copies.new_receive(), copies.new_receive()
            copies.start(acc.at[g, XN, top], top_in.at[g, 0], xn, SUMS, in_sems[g][0])
            copies.start(acc.at[g, YN, bottom], bottom_in.at[g, 0], yn, SUMS, in_sems[g][1])

    def pieces_of(g, r):
        return (LEFT, RIGHT) if (g, r) == (0, DIAG) else (WHOLE_WIDTH,)

    def pass_on(g):
        await_all(diag_in.at[g], first[g])
        acc[g, YN, top] += diag_in[g, 0]
        copies.start(acc.at[g, YN, top], top_in.at[g, 1], yn, SUMS, in_sems[g][0])
        acc[g, XN, bottom] += diag_in[g, 1]
        copies.start(acc.at[g, XN, bottom], bottom_in.at[g, 1], xn, SUMS, in_sems[g][1])

    pending = None
    for g in range(GROUPS):
        receive_context(g)
        for slot, (r, c) in enumerate(wo_order):
            if g == 0 and c == 1:
                await_all(w_buf.at[pl.ds(slot, 2)], load_sems.at[slot // 2])
            if c == 1:
                for cols in pieces_of(g, r):
                    d2d[g, r, cols.start] = copies.new_receive()
                    send_d2d[g, r, :, cols] = dot(lhs[g], w_buf[slot, :, cols])
                    copies.start(send_d2d.at[g, r, :, cols], recv_d2d.at[g, r, :, cols], partner, CORE, d2d[g, r, cols.start])
            else:
                acc[g, r] = dot(lhs[g], w_buf[slot])
                if len(pieces_of(g, r)) > 1:
                    start_diagonal(g, LEFT)
            if not last and g == GROUPS - 1:
                pltpu.make_async_copy(wq_hbm.at[layer + 1, columns(*wq_order[slot]), :], w_buf.at[slot], wq_sem).start()
            if c == 1 and pending is not None:
                settle(*pending)
                if g > 0 and pending == (g, PASS_ON_AFTER):
                    pass_on(g - 1)
            pending = (g, r)
    settle(*pending)
    if not last:
        load_cache(layer + 1, pl.ds(0, MY_ROWS), k_hbm, v_hbm, kv_pre, cache_sem)
    pass_on(GROUPS - 1)

    gather, diag_sems, relay_sems = {}, {}, {}
    if not last:
        res_load.wait()

    def finish_group(g):
        if last:
            residual = res_buf[g].astype(F32)
        else:
            residual = res_buf[:, g].astype(F32).reshape(GROUP_ROWS, MY_COLS)
        await_all(top_in.at[g], in_sems[g][0])
        total = acc[g, SELF, top] + top_in[g, 0] + top_in[g, 1]
        h_buf[SELF, 0, g, top] = (residual[:HALF] + total).astype(BF16)
        await_all(bottom_in.at[g], in_sems[g][1])
        total = acc[g, SELF, bottom] + bottom_in[g, 0] + bottom_in[g, 1]
        h_buf[SELF, 0, g, bottom] = (residual[HALF:] + total).astype(BF16)
        mine = h_buf.at[SELF, 0, g]
        for r, device, halves in ((XN, xn, (top, bottom)), (YN, yn, (bottom, top))):
            gather[r, 0, g] = [copies.start(h_buf.at[SELF, 0, g, half], h_buf.at[r, 0, g, half], device, HALVES)
                               for half in halves]
        gather[SELF, 1, g] = copies.start(mine, h_buf.at[SELF, 1, g], partner, WHOLE)
        if not last:
            own_out[g] = h_buf[SELF, 0, g]

    def arrive(r, c, g):
        gather[r, c, g].wait_recv()

    if last:
        def use(g, *pieces):
            for r, c in pieces:
                rows = h_buf[r, c, g].astype(F32).reshape(DEVICES, GROUP_SEQS, MY_COLS).astype(BF16)
                out_ref[:, g, :, columns(r, c)] = rows
    else:
        wq_slot = {piece: slot for slot, piece in enumerate(wq_order)}

        def use(g, *pieces):
            q_acc[g] += sum(dot(h_buf[r, c, g], w_buf[wq_slot[r, c]]) for r, c in pieces)

    def relay_first(g):
        diag_sems[g] = copies.new_receive()
        for r, device, half in ((XN, yn, top), (YN, xn, bottom)):
            gather[r, 0, g][0].wait_recv()
            copies.start(h_buf.at[r, 0, g, half], h_buf.at[DIAG, 0, g, half], device, HALVES, diag_sems[g])

    def relay_second(g):
        relay_sems[g] = copies.new_receive()
        for r in (XN, YN):
            gather[r, 0, g][1].wait_recv()
            copies.start(h_buf.at[r, 0, g], h_buf.at[r, 1, g], partner, WHOLE, relay_sems[g])

    def relay_diag(g):
        await_all(h_buf.at[DIAG, 0, g], diag_sems[g])
        gather[DIAG, 1, g] = copies.start(h_buf.at[DIAG, 0, g], h_buf.at[DIAG, 1, g], partner, WHOLE)

    def send_query(g):
        q_send[g] = q_acc[g].astype(BF16).reshape(DEVICES, GROUP_SEQS, MY_COLS)
        for to in others():
            copies.start(q_send.at[g, to], q_out.at[me, seqs[g], :], to, QUERY, q_sem)

    if not last:
        q_sem = copies.new_receive()
        await_all(w_buf, wq_sem)
        q_acc[...] = jnp.zeros_like(q_acc)
    finish_group(0)
    finish_group(1)
    relay_first(0)
    for g in range(GROUPS):
        arrive(SELF, 1, g)
        use(g, (SELF, 0), (SELF, 1))
    relay_second(0)
    use(0, (XN, 0), (YN, 0))
    relay_first(1)
    await_all(h_buf.at[pl.ds(XN, 2), 1, 0], relay_sems[0])
    use(0, (XN, 1), (YN, 1))
    relay_second(1)
    use(1, (XN, 0), (YN, 0))
    relay_diag(0)
    use(0, (DIAG, 0))
    await_all(h_buf.at[pl.ds(XN, 2), 1, 1], relay_sems[1])
    use(1, (XN, 1), (YN, 1))
    relay_diag(1)
    arrive(DIAG, 1, 0)
    use(0, (DIAG, 1))
    if not last:
        send_query(0)
    use(1, (DIAG, 0))
    arrive(DIAG, 1, 1)
    use(1, (DIAG, 1))

    if not last:
        send_query(GROUPS - 1)
        for g in range(GROUPS):
            q_out[me, seqs[g], :] = q_send[g, me]
        await_all(wkv_buf, wkv_sem)
        chip_rows = pl.ds(pl.multiple_of((me - core) * GROUP_SEQS, 2 * GROUP_SEQS), 2 * GROUP_SEQS)
        made = jnp.zeros((GROUPS * 2 * GROUP_SEQS, HEAD_DIM), F32)
        for r, c in wq_order:
            rows = jnp.concatenate([h_buf[r, c, g, chip_rows, :] for g in range(GROUPS)], axis=0)
            made += dot(rows, wkv_buf[columns(r, c), :])
        made = made.reshape(GROUPS, 2, GROUP_SEQS, HEAD_DIM)
        made = jnp.concatenate([made[g, k] for k in range(2) for g in range(GROUPS)], axis=0)
        shared = share_new_rows(copies, core, partner, made, kv_send, kv_out, NEW_ROWS)
        len_load.wait()
        await_all(kv_pre, cache_sem)
        shared.wait()
        for b in range(READY_ROWS):
            here = lax.broadcasted_iota(jnp.int32, (SEQ, HEAD_DIM), 0) == len_ref[me * MY_ROWS + b]
            for i in range(2):
                row = jnp.broadcast_to(kv_out[i, b:b + 1, :].astype(F32), (SEQ, HEAD_DIM))
                kv_pre[i, b] = jnp.where(here, row, kv_pre[i, b].astype(F32)).astype(BF16)
        await_all(q_out.at[seven], q_sem)
        await_all(q_send.at[:, seven], send_sems.at[QUERY])
    await_all(ctx_in.at[seven], send_sems.at[CONTEXT])
    await_all(send_d2d, send_sems.at[CORE])
    await_all(acc.at[:, pl.ds(0, 3)], send_sems.at[SUMS])
    await_all(h_buf.at[pl.ds(0, 2)], send_sems.at[WHOLE])
    await_all(h_buf.at[pl.ds(0, 3), 0], send_sems.at[HALVES])


def combine_call(layer, last, ctx, residual, w_out, more):
    any_spec = pl.BlockSpec(memory_space=pl.ANY)
    vmem_spec = pl.BlockSpec(memory_space=pltpu.VMEM)
    receives = (2 if last else 4) + 1 + GROUPS * (4 + 3 + 8)
    scratch = [
        pltpu.VMEM((GROUPS, DEVICES, GROUP_SEQS, MY_HEADS, HEAD_DIM), BF16),
        pltpu.VMEM((GROUPS, GROUP_ROWS, MY_COLS), BF16),
        pltpu.VMEM((DEVICES, MY_COLS, MY_COLS), BF16),
        pltpu.VMEM((GROUPS, 4, GROUP_ROWS, MY_COLS), F32),
        pltpu.VMEM((GROUPS, 4, GROUP_ROWS, MY_COLS), F32),
        pltpu.VMEM((GROUPS, 4, GROUP_ROWS, MY_COLS), F32),
        pltpu.VMEM((GROUPS, 2, HALF, MY_COLS), F32),
        pltpu.VMEM((GROUPS, 2, HALF, MY_COLS), F32),
        pltpu.VMEM((GROUPS, 2, HALF, MY_COLS), F32),
        pltpu.VMEM((4, 2, GROUPS, GROUP_ROWS, MY_COLS), BF16),
    ]
    if last:
        out_shape = pltpu.VMEM((DEVICES, GROUPS, GROUP_SEQS, D_MODEL), BF16)
        out_specs = vmem_spec
    else:
        out_shape = (pltpu.VMEM((GROUPS, GROUP_ROWS, MY_COLS), BF16),) + QUERY_SHAPES
        out_specs = (vmem_spec,) * len(out_shape)
        scratch.insert(2, pltpu.VMEM((DEVICES, GROUPS, GROUP_SEQS, MY_COLS), BF16))
        scratch += [
            pltpu.VMEM((D_MODEL, HEAD_DIM), BF16),
            pltpu.VMEM((GROUPS, GROUP_ROWS, MY_COLS), F32),
            pltpu.VMEM((GROUPS, DEVICES, GROUP_SEQS, MY_COLS), BF16),
            pltpu.VMEM((2, MY_ROWS, HEAD_DIM), BF16),
            pltpu.SMEM((ROWS,), jnp.int32),
        ]
    scratch += [
        pltpu.SemaphoreType.DMA((4 if last else 9,)),
        pltpu.SemaphoreType.DMA((5 if last else 7,)),
        pltpu.SemaphoreType.DMA((receives,)),
    ]
    return pl.pallas_call(
        functools.partial(combine_kernel, layer, last),
        name="combine_last" if last else "combine",
        out_shape=out_shape,
        in_specs=[vmem_spec, vmem_spec if last else any_spec] + [any_spec] * (1 + len(more)),
        out_specs=out_specs,
        scratch_shapes=scratch,
        compiler_params=pltpu.CompilerParams(
            collective_id=2 if last else 1, has_side_effects=True, vmem_limit_bytes=40 * MIB
        ),
    )(*in_vmem(ctx), *(in_vmem if last else in_hbm)(residual), *in_hbm(w_out, *more))


def solution(mesh):
    cache_spec = P(None, ("replica", "model"), None, None)

    def device_step(x, cache_len, w_query, w_key, w_value, w_out, k_cache, v_cache):
        caches = (k_cache, v_cache)
        q, kv_new, kv_pre = query_call(x, w_query, w_key, w_value, *caches)
        ctx, k_all, v_all = attend_call(0, LATE_ROWS, 0, cache_len, q, kv_new, kv_pre, *caches, ())
        own, q, kv_new, kv_pre = combine_call(0, False, ctx, x.reshape(DEVICES, GROUPS, GROUP_SEQS, D_MODEL), w_out, (w_query, w_key, w_value, *caches, cache_len))
        ctx, k_all, v_all = attend_call(1, 0, READY_ROWS, cache_len, q, kv_new, kv_pre, *caches, (k_all, v_all))
        out = combine_call(1, True, ctx, own, w_out, ())
        return out.reshape(x.shape), k_all, v_all

    return jax.shard_map(
        device_step,
        mesh=mesh,
        in_specs=(P("replica", None), P("replica"), P(None, None, "model"), P(), P(), P(None, "model", None), cache_spec, cache_spec),
        out_specs=(P("replica", None), cache_spec, cache_spec),
        check_vma=False,
    )
```
